128 devices in a mesh: row: 8 (over y, x_lo), col: 16 (over x_hi, z, core).
Axes of the slice: x: 4 (x_hi: 2, x_lo: 2; x = x_hi * 2 + x_lo), y: 4, z: 4, core: 2. Of those that a mesh axis runs over, the one named last changes fastest.
Arguments:
- features: bfloat16 [131072, 128], P(('row', 'col')), may hold values from -24 to 24
- tile_rows: int32 [8, 16, 1024], P('row', 'col'), may hold values from 0 to 127
- tile_cols: int32 [8, 16, 1024], P('row', 'col'), may hold values from 0 to 63
- edge_lists: int32 [2, 8, 16, 1024, 128], P(None, 'row', 'col'), may hold values from -16 to 127
- tile_counts: int32 [8, 16], P('row', 'col'), may hold values from 128 to 1024, as said below
Outputs:
- hop_one: bfloat16 [131072, 128], P(('row', 'col'))
- hop_two: bfloat16 [131072, 128], P(('row', 'col'))
The draws below stay inside these ranges and needn't reach their ends.
Inputs may be any that keep to these rules, and one draw needn't show every extreme that they name: `tile_counts`: live tile slots of a block; some block has exactly 1024. `edge_lists`: a negative entry marks an empty edge slot; slots at or past a block's count hold arbitrary entries. `tile_rows`: a tile may occur in several slots; slots at or past a block's count hold arbitrary entries. `tile_cols`: slots at or past a block's count hold arbitrary entries.
All inputs are finite; a program needn't handle non-finite values.
Results may differ from the reference program's by a relative error of at most 0.0058.
Values may be sent and summed in bfloat16 or wider, within the bound.
A program may use at most 192 MiB of HBM per device.

```python
import jax
import jax.numpy as jnp
from jax import lax

F = 128
TILE = 128
EDGE_TILE = 128
NODE_DEV = 1024
TILE_MOST = 1024
NODES = 131072
TILE_ROWS = 128
TILE_COLS = 64
N_ROW = 8
N_COL = 16


def draw_tile_counts(key, part):
    base = jax.random.randint(jax.random.fold_in(key, 11), (N_ROW * N_COL,), TILE_MOST // 8, TILE_MOST // 2 + 1)
    busiest = jax.random.randint(jax.random.fold_in(key, 12), (), 0, N_ROW * N_COL)
    placed = jnp.where(jnp.arange(N_ROW * N_COL) == busiest, TILE_MOST, base)
    return placed.reshape(N_ROW, N_COL).astype(jnp.int32)


def set_ends(result, key, smallest, high):
    shape = result.shape
    place = [jax.random.randint(jax.random.fold_in(key, axis), (), 0, shape[axis]) for axis in range(len(shape))]
    result = result.at[tuple(place)].set(smallest)
    longest = shape.index(max(shape))
    place[longest] = (place[longest] + 1) % shape[longest]
    return result.at[tuple(place)].set(high)


def level_of(key, dims, shards, low, largest):
    factor_of, own = 1.0, jax.random.fold_in(key, 6)
    for dim, shards_of in shards:
        steps = jnp.exp(jax.random.uniform(jax.random.fold_in(own, dim), (shards_of,), jnp.float32, low / len(shards), largest / len(shards)))
        factor_of = factor_of * jnp.repeat(steps, dims[dim] // shards_of).reshape([-1 if axis == dim else 1 for axis in range(len(dims))])
    return factor_of


def scatter_about(rng, shape, scale, bound, shards=(), dtype=jnp.bfloat16):
    values = scale * jax.random.normal(rng, shape, jnp.float32)
    if shards:
        values = values * level_of(rng, shape, shards, -0.22, 0.18)
    return jnp.clip(values, -bound, bound).astype(dtype)


def setup_inputs(seed: int = 0) -> dict:
    keys = jax.random.split(jax.random.key(seed), 6)
    features = scatter_about(keys[0], (NODES, F), 4.0, 24.0, ((0, 128),))
    tile_rows = set_ends(jax.random.randint(keys[1], (N_ROW, N_COL, TILE_MOST), 0, TILE_ROWS), jax.random.fold_in(keys[1], 1), 0, TILE_ROWS - 1).astype(jnp.int32)
    tile_cols = set_ends(jax.random.randint(keys[2], (N_ROW, N_COL, TILE_MOST), 0, TILE_COLS), jax.random.fold_in(keys[2], 1), 0, TILE_COLS - 1).astype(jnp.int32)
    edge_lists = set_ends(jax.random.randint(keys[3], (2, N_ROW, N_COL, TILE_MOST, EDGE_TILE), -16, TILE), jax.random.fold_in(keys[3], 1), -16, TILE - 1).astype(jnp.int32)
    tile_counts = draw_tile_counts(jax.random.fold_in(keys[5], 71), 0)
    return dict(features=features, tile_rows=tile_rows, tile_cols=tile_cols, edge_lists=edge_lists, tile_counts=tile_counts)


def reference(features, tile_rows, tile_cols, edge_lists, tile_counts):
    node_total = NODE_DEV * N_ROW * N_COL
    block_nodes = NODE_DEV * N_COL
    slot_ids = lax.iota(jnp.int32, TILE_MOST)

    def edges_of(device_idx):
        row_idx = device_idx // N_COL
        col_idx = device_idx % N_COL
        dst_ids = edge_lists[0, row_idx, col_idx]
        src_ids = edge_lists[1, row_idx, col_idx]
        alive = (slot_ids < tile_counts[row_idx, col_idx])[:, None] & (dst_ids >= 0) & (src_ids >= 0)
        target = row_idx * block_nodes + tile_rows[row_idx, col_idx][:, None] * TILE + dst_ids
        column = tile_cols[row_idx, col_idx][:, None] * TILE + src_ids
        source = (column // NODE_DEV * N_COL + col_idx) * NODE_DEV + column % NODE_DEV
        target = jnp.where(alive, target, 0).reshape(-1)
        source = jnp.where(alive, source, 0).reshape(-1)
        return (target, source, alive.astype(jnp.float32).reshape(-1))

    def count_edges(device_idx, degree):
        target, source, weight = edges_of(device_idx)
        return degree.at[target].add(weight)
    degree = lax.fori_loop(0, N_ROW * N_COL, count_edges, jnp.zeros((node_total,), jnp.float32))
    inv_root = lax.rsqrt(1.0 + degree)

    def propagate(scaled):

        def add_edges(device_idx, summed):
            target, source, weight = edges_of(device_idx)
            return summed.at[target].add(scaled[source].astype(jnp.float32) * weight[:, None])
        return lax.fori_loop(0, N_ROW * N_COL, add_edges, jnp.zeros((node_total, F), jnp.float32))
    scaled_zero = (features.astype(jnp.float32) * inv_root[:, None]).astype(jnp.bfloat16)
    first_sum = propagate(scaled_zero)
    hop_one = (first_sum * inv_root[:, None]).astype(jnp.bfloat16)
    scaled_one = (first_sum * (inv_root * inv_root)[:, None]).astype(jnp.bfloat16)
    second_sum = propagate(scaled_one)
    hop_two = (second_sum * inv_root[:, None]).astype(jnp.bfloat16)
    return (hop_one, hop_two)
```

```python
import functools

import jax
import jax.numpy as jnp
from jax import lax
from jax.experimental import pallas as pl
from jax.experimental.pallas import tpu as pltpu
from jax.sharding import PartitionSpec as P

TILE = 128
GROUP = 64
BATCH = 8


def last_group(count_ref):
    return (count_ref[0] - 1) // GROUP


def build_kernel(count_ref, rows_ref, dst_ref, src_ref, tiles_ref, degree_ref):
    group = pl.program_id(0)
    count = count_ref[0]

    @pl.when(group == 0)
    def _():
        degree_ref[...] = jnp.zeros_like(degree_ref)

    @pl.when(group * GROUP < count)
    def _():
        slot = group * GROUP + lax.broadcasted_iota(jnp.int32, (GROUP, TILE), 0)
        dst = jnp.where(slot < count, dst_ref[...], -1).astype(jnp.float32).astype(jnp.bfloat16)
        src = src_ref[...].astype(jnp.float32).astype(jnp.bfloat16)
        cell = lax.broadcasted_iota(jnp.int32, (TILE, TILE), 0).astype(jnp.float32).astype(jnp.bfloat16)
        one, zero = jnp.bfloat16(1), jnp.bfloat16(0)
        totals = []
        for i in range(GROUP):
            dst_hot = jnp.where(jnp.broadcast_to(dst[i : i + 1, :], (TILE, TILE)) == cell, one, zero)
            src_hot = jnp.where(jnp.broadcast_to(src[i : i + 1, :], (TILE, TILE)) == cell, one, zero)
            counts = lax.dot_general(
                src_hot, dst_hot, (((1,), (1,)), ((), ())), preferred_element_type=jnp.float32
            )
            tiles_ref[i] = counts.astype(jnp.bfloat16)
            totals.append(jnp.sum(counts, axis=0, keepdims=True))
        for i in range(GROUP):
            degree_ref[pl.ds(rows_ref[group * GROUP + i], 1), :] += totals[i]


def build_tiles(count, rows, dst, src):
    slots = dst.shape[0]
    lists = pl.BlockSpec((GROUP, TILE), lambda g, n, r: (jnp.minimum(g, last_group(n)), 0))
    return pl.pallas_call(
        build_kernel,
        grid_spec=pltpu.PrefetchScalarGridSpec(
            num_scalar_prefetch=2,
            grid=(slots // GROUP,),
            in_specs=[lists, lists],
            out_specs=[
                pl.BlockSpec((GROUP, TILE, TILE), lambda g, n, r: (jnp.minimum(g, last_group(n)), 0, 0)),
                pl.BlockSpec((TILE, TILE), lambda g, n, r: (0, 0)),
            ],
        ),
        out_shape=[
            jax.ShapeDtypeStruct((slots, TILE, TILE), jnp.bfloat16),
            jax.ShapeDtypeStruct((TILE, TILE), jnp.float32),
        ],
        name="build_tiles",
    )(count, rows, dst, src)


def apply_kernel(count_ref, rows_ref, cols_ref, tiles_ref, x_ref, out_ref, total):
    group = pl.program_id(0)

    @pl.when(group == 0)
    def _():
        total[...] = jnp.zeros_like(total)

    @pl.when(group * GROUP < count_ref[0])
    def _():
        base = group * GROUP
        for start in range(0, GROUP, BATCH):
            products = [
                jnp.dot(x_ref[cols_ref[base + i]], tiles_ref[i], preferred_element_type=jnp.float32)
                for i in range(start, start + BATCH)
            ]
            for j, product in enumerate(products):
                total[rows_ref[base + start + j]] += product

    @pl.when(group == pl.num_programs(0) - 1)
    def _():
        out_ref[...] = total[...].astype(jnp.bfloat16)


def apply_tiles(count, rows, cols, tiles, x):
    slots = tiles.shape[0]
    blocks = x.shape[0]
    return pl.pallas_call(
        apply_kernel,
        grid_spec=pltpu.PrefetchScalarGridSpec(
            num_scalar_prefetch=3,
            grid=(slots // GROUP,),
            in_specs=[
                pl.BlockSpec((GROUP, TILE, TILE), lambda g, n, r, c: (jnp.minimum(g, last_group(n)), 0, 0)),
                pl.BlockSpec((blocks, TILE, TILE), lambda g, n, r, c: (0, 0, 0)),
            ],
            out_specs=pl.BlockSpec((TILE, TILE, TILE), lambda g, n, r, c: (0, 0, 0)),
            scratch_shapes=[pltpu.VMEM((TILE, TILE, TILE), jnp.float32)],
        ),
        out_shape=jax.ShapeDtypeStruct((TILE, TILE, TILE), jnp.bfloat16),
        compiler_params=pltpu.CompilerParams(vmem_limit_bytes=40 * 2**20),
        name="apply_tiles",
    )(count, rows, cols, tiles, x)


def share_sum(partial, axis):
    size = lax.axis_size(axis)
    pieces = partial.reshape(size, partial.shape[0] // size, *partial.shape[1:])
    return lax.all_to_all(pieces, axis, 0, 0, tiled=True).astype(jnp.float32).sum(0)


def gathered(x, axis):
    size = lax.axis_size(axis)
    pieces = lax.all_to_all(jnp.broadcast_to(x[None], (size, *x.shape)), axis, 0, 0, tiled=True)
    return pieces.reshape(size * x.shape[0], *x.shape[1:])


def tile_transpose(x):
    return jnp.swapaxes(x, 1, 2)


def local(features, tile_rows, tile_cols, edge_lists, tile_counts):
    nodes, width = features.shape
    rows, cols = tile_rows[0, 0], tile_cols[0, 0]
    count = tile_counts[0]
    tiles, degree = build_tiles(count, rows, edge_lists[0, 0, 0], edge_lists[1, 0, 0])
    own_degree = share_sum(degree, "col")
    inv_root = lax.rsqrt(1.0 + own_degree)[:, None, :]

    def propagate(scaled):
        partial = apply_tiles(count, rows, cols, tiles, gathered(scaled, "row"))
        return share_sum(partial, "col")

    def output(x):
        return tile_transpose(x).reshape(nodes, width)

    own = tile_transpose(features.reshape(nodes // TILE, TILE, width))
    scaled_zero = (own.astype(jnp.float32) * inv_root).astype(jnp.bfloat16)
    first_sum = propagate(scaled_zero)
    hop_one = (first_sum * inv_root).astype(jnp.bfloat16)
    scaled_one = (first_sum * (inv_root * inv_root)).astype(jnp.bfloat16)
    second_sum = propagate(scaled_one)
    hop_two = (second_sum * inv_root).astype(jnp.bfloat16)
    return (output(hop_one), output(hop_two))


def solution(mesh):
    placed = (
        P(("row", "col"), None),
        P("row", "col", None),
        P("row", "col", None),
        P(None, "row", "col", None, None),
        P("row", "col"),
    )
    return jax.shard_map(
        local,
        mesh=mesh,
        in_specs=placed,
        out_specs=(P(("row", "col"), None), P(("row", "col"), None)),
        check_vma=False,
    )
```

```python
import functools

import jax
import jax.numpy as jnp
from jax import lax
from jax.experimental import pallas as pl
from jax.experimental.pallas import tpu as pltpu
from jax.sharding import PartitionSpec as P

TILE = 128
GROUP = 64
BATCH = 8


def last_group(count_ref):
    return (count_ref[0] - 1) // GROUP


def build_kernel(count_ref, rows_ref, edges_ref, tiles_ref, degree_ref):
    group = pl.program_id(0)
    count = count_ref[0]

    @pl.when(group == 0)
    def _():
        degree_ref[...] = jnp.zeros_like(degree_ref)

    @pl.when(group * GROUP < count)
    def _():
        slot = group * GROUP + lax.broadcasted_iota(jnp.int32, (GROUP, TILE), 0)
        dst = jnp.where(slot < count, edges_ref[0], -1).astype(jnp.float32).astype(jnp.bfloat16)
        src = edges_ref[1].astype(jnp.float32).astype(jnp.bfloat16)
        cell = lax.broadcasted_iota(jnp.int32, (TILE, TILE), 0).astype(jnp.float32).astype(jnp.bfloat16)
        one, zero = jnp.bfloat16(1), jnp.bfloat16(0)
        totals = []
        for i in range(GROUP):
            dst_hot = jnp.where(jnp.broadcast_to(dst[i : i + 1, :], (TILE, TILE)) == cell, one, zero)
            src_hot = jnp.where(jnp.broadcast_to(src[i : i + 1, :], (TILE, TILE)) == cell, one, zero)
            counts = lax.dot_general(
                src_hot, dst_hot, (((1,), (1,)), ((), ())), preferred_element_type=jnp.float32
            )
            tiles_ref[i] = counts.astype(jnp.bfloat16)
            totals.append(jnp.sum(counts, axis=0, keepdims=True))
        for i in range(GROUP):
            degree_ref[pl.ds(rows_ref[group * GROUP + i], 1), :] += totals[i]


def build_tiles(count, rows, edges):
    slots = edges.shape[1]
    lists = pl.BlockSpec((2, GROUP, TILE), lambda g, n, r: (0, jnp.minimum(g, last_group(n)), 0))
    return pl.pallas_call(
        build_kernel,
        grid_spec=pltpu.PrefetchScalarGridSpec(
            num_scalar_prefetch=2,
            grid=(slots // GROUP,),
            in_specs=[lists],
            out_specs=[
                pl.BlockSpec((GROUP, TILE, TILE), lambda g, n, r: (jnp.minimum(g, last_group(n)), 0, 0)),
                pl.BlockSpec((TILE, TILE), lambda g, n, r: (0, 0)),
            ],
        ),
        out_shape=[
            jax.ShapeDtypeStruct((slots, TILE, TILE), jnp.bfloat16),
            jax.ShapeDtypeStruct((TILE, TILE), jnp.float32),
        ],
        name="build_tiles",
    )(count, rows, edges)


def apply_kernel(count_ref, rows_ref, cols_ref, tiles_ref, x_ref, out_ref, total):
    group = pl.program_id(0)

    @pl.when(group == 0)
    def _():
        total[...] = jnp.zeros_like(total)

    @pl.when(group * GROUP < count_ref[0])
    def _():
        base = group * GROUP
        for start in range(0, GROUP, BATCH):
            products = [
                jnp.dot(x_ref[cols_ref[base + i]], tiles_ref[i], preferred_element_type=jnp.float32)
                for i in range(start, start + BATCH)
            ]
            for j, product in enumerate(products):
                total[rows_ref[base + start + j]] += product

    @pl.when(group == pl.num_programs(0) - 1)
    def _():
        out_ref[...] = total[...].astype(jnp.bfloat16)


def apply_tiles(count, rows, cols, tiles, x):
    slots = tiles.shape[0]
    blocks = x.shape[0]
    return pl.pallas_call(
        apply_kernel,
        grid_spec=pltpu.PrefetchScalarGridSpec(
            num_scalar_prefetch=3,
            grid=(slots // GROUP,),
            in_specs=[
                pl.BlockSpec((GROUP, TILE, TILE), lambda g, n, r, c: (jnp.minimum(g, last_group(n)), 0, 0)),
                pl.BlockSpec((blocks, TILE, TILE), lambda g, n, r, c: (0, 0, 0)),
            ],
            out_specs=pl.BlockSpec((TILE, TILE, TILE), lambda g, n, r, c: (0, 0, 0)),
            scratch_shapes=[pltpu.VMEM((TILE, TILE, TILE), jnp.float32)],
        ),
        out_shape=jax.ShapeDtypeStruct((TILE, TILE, TILE), jnp.bfloat16),
        compiler_params=pltpu.CompilerParams(vmem_limit_bytes=40 * 2**20),
        name="apply_tiles",
    )(count, rows, cols, tiles, x)


N_CHUNK = 4
MESH = pl.DeviceIdType.MESH


class Place:
    def __init__(self):
        self.row, self.col = lax.axis_index("row"), lax.axis_index("col")
        self.y, self.x_lo = self.row // 2, self.row % 2
        self.x_hi, self.z, self.core = self.col // 8, (self.col // 2) % 4, self.col % 2

    def at(self, y=None, x_lo=None, x_hi=None, z=None, core=None):
        pick = lambda new, old: old if new is None else new
        row = pick(y, self.y) * 2 + pick(x_lo, self.x_lo)
        col = (pick(x_hi, self.x_hi) * 4 + pick(z, self.z)) * 2 + pick(core, self.core)
        return (row, col)


def greet(devices):
    barrier = pltpu.get_barrier_semaphore()
    for device in devices:
        pl.semaphore_signal(barrier, inc=1, device_id=device, device_id_type=MESH)
    pl.semaphore_wait(barrier, len(devices))


def sum_devices(me):
    return [
        me.at(core=1 - me.core),
        me.at(z=(me.z + 1) % 4),
        me.at(z=(me.z + 3) % 4),
        me.at(x_hi=1 - me.x_hi),
    ]


def spread_devices(me):
    return [me.at(x_lo=1 - me.x_lo), me.at(y=(me.y + 1) % 4), me.at(y=(me.y + 3) % 4)]


def run_stages(stages, chunks):
    for tick in range(len(stages) + chunks - 1):
        for q in range(chunks):
            if 0 <= tick - q < len(stages):
                stages[tick - q](q)


def each_tile(q, body):
    def step(i, carry):
        body(q * PER_CHUNK + i)
        return carry

    lax.fori_loop(0, PER_CHUNK, step, 0)


PER_CHUNK = 8 // N_CHUNK


def span(q):
    return pl.ds(q * PER_CHUNK, PER_CHUNK)


def wide(x):
    return x.astype(jnp.float32)


def sum_stages(me, part, bufs, sems, finish):
    own, given, running, arrived, kept, across, crossed = bufs
    own_sem, pair_send, pair_recv, ring_send, ring_recv, far_send, far_recv = sems
    sent = []

    def own_copy(q):
        return pltpu.make_async_copy(part.at[:, :, me.core, span(q)], own.at[:, :, span(q)], own_sem.at[q])

    def pair_copy(q):
        return pltpu.make_async_remote_copy(
            part.at[:, :, 1 - me.core, span(q)], given.at[:, :, span(q)], pair_send.at[q], pair_recv.at[q],
            device_id=me.at(core=1 - me.core), device_id_type=MESH,
        )

    def ring_copy(way, step, q):
        return pltpu.make_async_remote_copy(
            running.at[way, step, span(q)], arrived.at[way, step, span(q)],
            ring_send.at[way, step, q], ring_recv.at[way, step, q],
            device_id=me.at(z=(me.z + (1 if way == 0 else 3)) % 4), device_id_type=MESH,
        )

    def far_copy(q):
        return pltpu.make_async_remote_copy(
            across.at[span(q)], crossed.at[span(q)], far_send.at[q], far_recv.at[q],
            device_id=me.at(x_hi=1 - me.x_hi), device_id_type=MESH,
        )

    def begin():
        for q in range(N_CHUNK):
            own_copy(q).start()
            pair_copy(q).start()

    def local_sum(way, step, k):
        x_hi = me.x_hi if way == 0 else 1 - me.x_hi
        z = (me.z + (3 - step if way == 0 else 1 + step)) % 4
        return wide(own[x_hi, z, k]) + wide(given[x_hi, z, k])

    def first(q):
        own_copy(q).wait()
        pair_copy(q).wait_recv()
        for way in (1, 0):
            def body(k, way=way):
                running[way, 0, k] = local_sum(way, 0, k).astype(jnp.bfloat16)

            each_tile(q, body)
            ring_copy(way, 0, q).start()

    def middle(step):
        def stage(q):
            for way in (1, 0):
                ring_copy(way, step - 1, q).wait_recv()

                def body(k, way=way):
                    total = local_sum(way, step, k) + wide(arrived[way, step - 1, k])
                    running[way, step, k] = total.astype(jnp.bfloat16)

                each_tile(q, body)
                ring_copy(way, step, q).start()

        return stage

    def last(q):
        ring_copy(1, 2, q).wait_recv()

        def other(k):
            across[k] = (local_sum(1, 3, k) + wide(arrived[1, 2, k])).astype(jnp.bfloat16)

        each_tile(q, other)
        far_copy(q).start()
        ring_copy(0, 2, q).wait_recv()

        def mine(k):
            kept[k] = local_sum(0, 3, k) + wide(arrived[0, 2, k])

        each_tile(q, mine)

    def done(q):
        far_copy(q).wait_recv()
        each_tile(q, lambda k: finish(k, kept[k] + wide(crossed[k])))

    def drain():
        for q in range(N_CHUNK):
            pair_copy(q).wait_send()
            far_copy(q).wait_send()
            for way in (0, 1):
                for step in range(3):
                    ring_copy(way, step, q).wait_send()

    return begin, [first, middle(1), middle(2), last, done], drain


def sum_scratch():
    block = lambda *lead, dtype=jnp.bfloat16: pltpu.VMEM((*lead, 8, TILE, TILE), dtype)
    dma = pltpu.SemaphoreType.DMA
    bufs = [block(2, 4), block(2, 4), block(2, 3), block(2, 3), block(dtype=jnp.float32), block(), block()]
    sems = [dma((N_CHUNK,))] * 3 + [dma((2, 3, N_CHUNK))] * 2 + [dma((N_CHUNK,))] * 2
    return bufs + sems


N_SUM = 14


def spread_stages(me, gathered, sems):
    side_send, side_recv, near_send, near_recv, relay_send, relay_recv = sems

    def side_copy(q):
        block = gathered.at[me.y, me.x_lo, span(q)]
        return pltpu.make_async_remote_copy(
            block, block, side_send.at[q], side_recv.at[q],
            device_id=me.at(x_lo=1 - me.x_lo), device_id_type=MESH,
        )

    def near_copy(kind, way, q):
        block = gathered.at[me.y, me.x_lo if kind == 0 else 1 - me.x_lo, span(q)]
        return pltpu.make_async_remote_copy(
            block, block, near_send.at[kind, way, q], near_recv.at[kind, way, q],
            device_id=me.at(y=(me.y + (1 if way == 0 else 3)) % 4), device_id_type=MESH,
        )

    def relay_copy(way, q):
        y = (me.y + (3 if way == 0 else 1)) % 4
        block = gathered.at[y, me.x_lo if way == 0 else 1 - me.x_lo, span(q)]
        return pltpu.make_async_remote_copy(
            block, block, relay_send.at[way, q], relay_recv.at[way, q],
            device_id=me.at(y=(me.y + (1 if way == 0 else 3)) % 4), device_id_type=MESH,
        )

    def own(q):
        side_copy(q).start()
        near_copy(0, 0, q).start()
        near_copy(0, 1, q).start()

    def beside(q):
        side_copy(q).wait_recv()
        near_copy(1, 0, q).start()
        near_copy(1, 1, q).start()

    def relay_own(q):
        near_copy(0, 0, q).wait_recv()
        relay_copy(0, q).start()

    def relay_beside(q):
        near_copy(1, 1, q).wait_recv()
        relay_copy(1, q).start()

    def drain():
        for q in range(N_CHUNK):
            near_copy(0, 1, q).wait_recv()
            near_copy(1, 0, q).wait_recv()
            relay_copy(0, q).wait_recv()
            relay_copy(1, q).wait_recv()
        for q in range(N_CHUNK):
            side_copy(q).wait_send()
            for way in (0, 1):
                near_copy(0, way, q).wait_send()
                near_copy(1, way, q).wait_send()
                relay_copy(way, q).wait_send()

    return [own, beside, relay_own, relay_beside], drain


def spread_scratch():
    dma = pltpu.SemaphoreType.DMA
    return [dma((N_CHUNK,))] * 2 + [dma((2, 2, N_CHUNK))] * 2 + [dma((2, N_CHUNK))] * 2


def start_kernel(degree_ref, features_ref, root_ref, gathered_ref, shares, share_send, share_recv, *sems):
    me = Place()
    peers = [lax.rem(me.col + i, 16) for i in range(1, 16)]
    greet([(me.row, peer) for peer in peers] + spread_devices(me))

    def share_copy(i):
        return pltpu.make_async_remote_copy(
            degree_ref.at[peers[i]], shares.at[i], share_send.at[i], share_recv.at[i],
            device_id=(me.row, peers[i]), device_id_type=MESH,
        )

    for i in range(15):
        share_copy(i).start()
    total = degree_ref[me.col]
    for i in range(15):
        share_copy(i).wait_recv()
        total = total + shares[i]
    root_ref[...] = lax.rsqrt(1.0 + total)

    def scale(q):
        def body(k):
            x = wide(features_ref[k]).T * root_ref[pl.ds(k, 1), :]
            gathered_ref[me.y, me.x_lo, k] = x.astype(jnp.bfloat16)

        each_tile(q, body)

    stages, drain = spread_stages(me, gathered_ref, sems)
    run_stages([scale] + stages, N_CHUNK)
    drain()
    for i in range(15):
        share_copy(i).wait_send()


def sum_kernel(spreads, part_ref, root_ref, hop_ref, *refs):
    me = Place()
    gathered_ref = refs[0] if spreads else None
    scratch = refs[1:] if spreads else refs
    greet(sum_devices(me) + (spread_devices(me) if spreads else []))

    def finish(k, total):
        root = root_ref[pl.ds(k, 1), :]
        hop_ref[k] = (total * root).T.astype(jnp.bfloat16)
        if spreads:
            gathered_ref[me.y, me.x_lo, k] = (total * (root * root)).astype(jnp.bfloat16)

    begin, stages, drain = sum_stages(me, part_ref, scratch[:7], scratch[7:N_SUM], finish)
    begin()
    if spreads:
        more, drain_spread = spread_stages(me, gathered_ref, scratch[N_SUM:])
        run_stages(stages + more, N_CHUNK)
        drain_spread()
    else:
        run_stages(stages, N_CHUNK)
    drain()


VMEM = pl.BlockSpec(memory_space=pltpu.VMEM)
GATHERED = jax.ShapeDtypeStruct((4, 2, 8, TILE, TILE), jnp.bfloat16)


def comm_params(number):
    return pltpu.CompilerParams(collective_id=number, has_side_effects=True, vmem_limit_bytes=32 * 2**20)


def start(degree, features):
    dma = pltpu.SemaphoreType.DMA
    return pl.pallas_call(
        start_kernel,
        out_shape=[jax.ShapeDtypeStruct((8, TILE), jnp.float32), GATHERED],
        in_specs=[VMEM, VMEM],
        out_specs=[VMEM, VMEM],
        scratch_shapes=[pltpu.VMEM((15, 8, TILE), jnp.float32), dma((15,)), dma((15,))] + spread_scratch(),
        compiler_params=comm_params(0),
        name="start_spread",
    )(degree.reshape(16, 8, TILE), features.reshape(8, TILE, TILE))


def sum_parts(part, root, spreads):
    hop = jax.ShapeDtypeStruct((8, TILE, TILE), jnp.bfloat16)
    return pl.pallas_call(
        functools.partial(sum_kernel, spreads),
        out_shape=[hop, GATHERED] if spreads else [hop],
        in_specs=[pl.BlockSpec(memory_space=pl.ANY), VMEM],
        out_specs=[VMEM, VMEM] if spreads else [VMEM],
        scratch_shapes=sum_scratch() + (spread_scratch() if spreads else []),
        compiler_params=comm_params(1 if spreads else 2),
        name="sum_spread" if spreads else "sum_last",
    )(part.reshape(2, 4, 2, 8, TILE, TILE), root)


def local(features, tile_rows, tile_cols, edge_lists, tile_counts):
    rows, cols = tile_rows[0, 0], tile_cols[0, 0]
    count = tile_counts[0]
    edges = edge_lists.reshape(2, *edge_lists.shape[3:])
    tiles, degree = build_tiles(count, rows, edges)
    root, gathered = start(degree, features)
    part = apply_tiles(count, rows, cols, tiles, gathered.reshape(64, TILE, TILE))
    hop_one, gathered = sum_parts(part, root, True)
    part = apply_tiles(count, rows, cols, tiles, gathered.reshape(64, TILE, TILE))
    (hop_two,) = sum_parts(part, root, False)
    return (hop_one.reshape(features.shape), hop_two.reshape(features.shape))


def solution(mesh):
    placed = (
        P(("row", "col"), None),
        P("row", "col", None),
        P("row", "col", None),
        P(None, "row", "col", None, None),
        P("row", "col"),
    )
    return jax.shard_map(
        local,
        mesh=mesh,
        in_specs=placed,
        out_specs=(P(("row", "col"), None), P(("row", "col"), None)),
        check_vma=False,
    )
```

```python
import functools

import jax
import jax.numpy as jnp
from jax import lax
from jax.experimental import pallas as pl
from jax.experimental.pallas import tpu as pltpu
from jax.sharding import PartitionSpec as P

TILE = 128
GROUP = 64
BATCH = 8
SUM_CHUNK = 8
RAW_CHUNK = 2


MESH = pl.DeviceIdType.MESH


class Place:
    def __init__(self):
        self.row, self.col = lax.axis_index("row"), lax.axis_index("col")
        self.y, self.x_lo = self.row // 2, self.row % 2
        self.x_hi, self.z, self.core = self.col // 8, (self.col // 2) % 4, self.col % 2

    def at(self, y=None, x_lo=None, x_hi=None, z=None, core=None):
        pick = lambda new, old: old if new is None else new
        row = pick(y, self.y) * 2 + pick(x_lo, self.x_lo)
        col = (pick(x_hi, self.x_hi) * 4 + pick(z, self.z)) * 2 + pick(core, self.core)
        return (row, col)


def greet(devices):
    barrier = pltpu.get_barrier_semaphore()
    for device in devices:
        pl.semaphore_signal(barrier, inc=1, device_id=device, device_id_type=MESH)
    pl.semaphore_wait(barrier, len(devices))


def sum_devices(me):
    return [
        me.at(core=1 - me.core),
        me.at(z=(me.z + 1) % 4),
        me.at(z=(me.z + 3) % 4),
        me.at(x_hi=1 - me.x_hi),
    ]


def spread_devices(me):
    return [me.at(x_lo=1 - me.x_lo), me.at(y=(me.y + 1) % 4), me.at(y=(me.y + 3) % 4)]


def run_stages(stages, chunks):
    for tick in range(len(stages) + chunks - 1):
        for q in range(chunks):
            if 0 <= tick - q < len(stages):
                stages[tick - q](q)


def each_tile(q, chunks, body):
    size = 8 // chunks

    def step(i, carry):
        body(q * size + i)
        return carry

    lax.fori_loop(0, size, step, 0)


def span(q, chunks):
    return pl.ds(q * (8 // chunks), 8 // chunks)


def wide(x):
    return x.astype(jnp.float32)


def sum_stages(me, part, bufs, sems, finish):
    own, given, running, arrived, kept, across, crossed = bufs
    own_sem, pair_send, pair_recv, ring_send, ring_recv, far_send, far_recv = sems
    chunks = SUM_CHUNK

    def own_copy(q):
        return pltpu.make_async_copy(
            part.at[:, :, me.core, span(q, chunks)], own.at[:, :, span(q, chunks)], own_sem.at[q]
        )

    def pair_copy(q):
        return pltpu.make_async_remote_copy(
            part.at[:, :, 1 - me.core, span(q, chunks)], given.at[:, :, span(q, chunks)],
            pair_send.at[q], pair_recv.at[q],
            device_id=me.at(core=1 - me.core), device_id_type=MESH,
        )

    def ring_copy(half, step, q):
        up = (half == 0) == (step < 2)
        return pltpu.make_async_remote_copy(
            running.at[half, step, span(q, chunks)], arrived.at[half, step, span(q, chunks)],
            ring_send.at[half, step, q], ring_recv.at[half, step, q],
            device_id=me.at(z=(me.z + (1 if up else 3)) % 4), device_id_type=MESH,
        )

    def far_copy(q):
        return pltpu.make_async_remote_copy(
            across.at[span(q, chunks)], crossed.at[span(q, chunks)], far_send.at[q], far_recv.at[q],
            device_id=me.at(x_hi=1 - me.x_hi), device_id_type=MESH,
        )

    def begin():
        for q in range(chunks):
            own_copy(q).start()
            pair_copy(q).start()

    def local_sum(half, offset, k):
        x_hi = me.x_hi if half == 0 else 1 - me.x_hi
        z = (me.z + (offset if half == 0 else 4 - offset)) % 4
        return wide(own[x_hi, z, k]) + wide(given[x_hi, z, k])

    def first(q):
        own_copy(q).wait()
        pair_copy(q).wait_recv()
        for half in (1, 0):
            for step, offset in ((0, 2), (2, 3)):
                def body(k, half=half, step=step, offset=offset):
                    running[half, step, k] = local_sum(half, offset, k).astype(jnp.bfloat16)

                each_tile(q, chunks, body)
                ring_copy(half, step, q).start()

    def middle(q):
        for half in (1, 0):
            ring_copy(half, 0, q).wait_recv()

            def body(k, half=half):
                running[half, 1, k] = (local_sum(half, 1, k) + wide(arrived[half, 0, k])).astype(jnp.bfloat16)

            each_tile(q, chunks, body)
            ring_copy(half, 1, q).start()

    def last(q):
        for half in (1, 0):
            ring_copy(half, 2, q).wait_recv()
            ring_copy(half, 1, q).wait_recv()

            def body(k, half=half):
                total = local_sum(half, 0, k) + (wide(arrived[half, 1, k]) + wide(arrived[half, 2, k]))
                if half == 1:
                    across[k] = total.astype(jnp.bfloat16)
                else:
                    kept[k] = total

            each_tile(q, chunks, body)
            if half == 1:
                far_copy(q).start()

    def done(q):
        far_copy(q).wait_recv()
        each_tile(q, chunks, lambda k: finish(k, kept[k] + wide(crossed[k])))

    def drain():
        for q in range(chunks):
            pair_copy(q).wait_send()
            far_copy(q).wait_send()
            for half in (0, 1):
                for step in range(3):
                    ring_copy(half, step, q).wait_send()

    return begin, [first, middle, last, done], drain


def sum_scratch():
    block = lambda *lead, dtype=jnp.bfloat16: pltpu.VMEM((*lead, 8, TILE, TILE), dtype)
    dma = pltpu.SemaphoreType.DMA
    bufs = [block(2, 4), block(2, 4), block(2, 3), block(2, 3), block(dtype=jnp.float32), block(), block()]
    sems = [dma((SUM_CHUNK,))] * 3 + [dma((2, 3, SUM_CHUNK))] * 2 + [dma((SUM_CHUNK,))] * 2
    return bufs + sems


N_SUM = 14


def spread_stages(me, gathered, sems, chunks):
    side_send, side_recv, near_send, near_recv, relay_send, relay_recv, pass_send, pass_recv = sems

    def copy(block, send, recv, device):
        return pltpu.make_async_remote_copy(block, block, send, recv, device_id=device, device_id_type=MESH)

    def block(y, x_lo, q):
        return gathered.at[me.core, (me.y + y) % 4, me.x_lo if x_lo == 0 else 1 - me.x_lo, span(q, chunks)]

    def side_copy(q):
        return copy(block(0, 0, q), side_send.at[q], side_recv.at[q], me.at(x_lo=1 - me.x_lo))

    def near_copy(kind, way, q):
        device = me.at(y=(me.y + (1 if way == 0 else 3)) % 4)
        return copy(block(0, kind, q), near_send.at[kind, way, q], near_recv.at[kind, way, q], device)

    def relay_copy(way, q):
        device = me.at(y=(me.y + (1 if way == 0 else 3)) % 4)
        return copy(block(3 if way == 0 else 1, way, q), relay_send.at[way, q], relay_recv.at[way, q], device)

    def pass_copy(y, x_lo, q):
        return copy(block(y, x_lo, q), pass_send.at[y, x_lo, q], pass_recv.at[y, x_lo, q], me.at(core=1 - me.core))

    def own(q):
        side_copy(q).start()
        near_copy(0, 0, q).start()
        near_copy(0, 1, q).start()
        pass_copy(0, 0, q).start()

    def beside(q):
        side_copy(q).wait_recv()
        near_copy(1, 0, q).start()
        near_copy(1, 1, q).start()
        pass_copy(0, 1, q).start()

    def relay_own(q):
        near_copy(0, 0, q).wait_recv()
        relay_copy(0, q).start()
        pass_copy(3, 0, q).start()
        near_copy(0, 1, q).wait_recv()
        pass_copy(1, 0, q).start()

    def relay_beside(q):
        near_copy(1, 1, q).wait_recv()
        relay_copy(1, q).start()
        pass_copy(1, 1, q).start()
        near_copy(1, 0, q).wait_recv()
        pass_copy(3, 1, q).start()

    def opposite(q):
        for way in (0, 1):
            relay_copy(way, q).wait_recv()
            pass_copy(2, way, q).start()

    def drain():
        for q in range(chunks):
            for y in range(4):
                for x_lo in range(2):
                    pass_copy(y, x_lo, q).wait_recv()
        for q in range(chunks):
            side_copy(q).wait_send()
            for way in (0, 1):
                near_copy(0, way, q).wait_send()
                near_copy(1, way, q).wait_send()
                relay_copy(way, q).wait_send()
            for y in range(4):
                for x_lo in range(2):
                    pass_copy(y, x_lo, q).wait_send()

    return [own, beside, relay_own, relay_beside, opposite], drain


def spread_scratch(chunks):
    dma = pltpu.SemaphoreType.DMA
    return [dma((chunks,))] * 2 + [dma((2, 2, chunks))] * 2 + [dma((2, chunks))] * 2 + [dma((4, 2, chunks))] * 2


def hot(ids, cell):
    return jnp.where(jnp.broadcast_to(ids, (TILE, TILE)) == cell, jnp.bfloat16(1), jnp.bfloat16(0))


def narrow(x):
    return x.astype(jnp.float32).astype(jnp.bfloat16)


def start_kernel(
    features_ref, meta_ref, edges_ref, tiles_ref, metas_ref, root_ref, gathered_ref,
    lists, raw, staged, slot_degree, degree, shares, roots,
    list_sem, list_send, list_recv, meta_send, meta_recv, tile_sem, share_send, share_recv, root_send, root_recv, *sems,
):
    me = Place()
    peers = [lax.rem(me.col + i, 16) for i in range(1, 16)]
    across = me.col + 1 - 2 * me.core
    friends = [(lax.rem(me.row + i % 8, 8), me.col if i < 8 else across) for i in range(1, 16)]
    greet([(me.row, peer) for peer in peers] + [friend for i, friend in enumerate(friends) if i != 7])
    partner = me.at(core=1 - me.core)

    own_lists = pltpu.make_async_copy(edges_ref.at[:, :, me.core], lists.at[me.core], list_sem)
    give_lists = pltpu.make_async_remote_copy(
        edges_ref.at[:, :, 1 - me.core], lists.at[me.core], list_send, list_recv, device_id=partner, device_id_type=MESH
    )
    give_meta = pltpu.make_async_remote_copy(
        meta_ref, metas_ref.at[me.core], meta_send, meta_recv, device_id=partner, device_id_type=MESH
    )

    def tile_copy(group, side):
        return pltpu.make_async_copy(staged.at[side], tiles_ref.at[group], tile_sem.at[side])

    def share_copy(i):
        return pltpu.make_async_remote_copy(
            degree.at[peers[i]], shares.at[i], share_send.at[i], share_recv.at[i],
            device_id=(me.row, peers[i]), device_id_type=MESH,
        )

    def root_copy(i):
        block = roots.at[me.core, me.y, me.x_lo]
        return pltpu.make_async_remote_copy(
            block, block, root_send.at[i], root_recv.at[i], device_id=friends[i], device_id_type=MESH
        )

    own_lists.start()
    give_lists.start()
    give_meta.start()
    metas_ref[me.core] = meta_ref[...]

    def turn(k, carry):
        raw[me.core, me.y, me.x_lo, k] = wide(features_ref[k]).T.astype(jnp.bfloat16)
        return carry

    lax.fori_loop(0, 8, turn, 0)
    slot_degree[...] = jnp.zeros_like(slot_degree)
    stages, drain = spread_stages(me, raw, sems, RAW_CHUNK)
    ticks = len(stages) + RAW_CHUNK - 1
    groups = 2 * lists.shape[2] * 8 // GROUP
    blocks = GROUP // 8
    own_lists.wait()

    def build(group, carry):
        for tick, when in enumerate(TICK_GROUP):
            @pl.when(group == when)
            def _(tick=tick):
                for q in range(RAW_CHUNK):
                    if 0 <= tick - q < len(stages):
                        stages[tick - q](q)

        @pl.when(group == groups // 2)
        def _():
            give_lists.wait_recv()
            give_meta.wait_recv()

        half = group // (groups // 2)
        place = group % (groups // 2)
        owner = me.core + half * (1 - 2 * me.core)
        side = group % 2
        base = place * blocks

        @pl.when(group >= 2)
        def _():
            tile_copy(0, side).wait()

        shape = (blocks, 8, TILE)
        slot = (lax.broadcasted_iota(jnp.int32, shape, 0) + base) * 16 + 8 * me.core + lax.broadcasted_iota(jnp.int32, shape, 1)
        live = slot < jnp.broadcast_to(metas_ref[owner, 8:9, :].reshape(1, 1, TILE), shape)
        dst = jnp.where(live, lists[owner, 0, pl.ds(base, blocks)], -1).reshape(GROUP, TILE)
        src = lists[owner, 1, pl.ds(base, blocks)].reshape(GROUP, TILE)
        dst, src = narrow(dst), narrow(src)
        cell = narrow(lax.broadcasted_iota(jnp.int32, (TILE, TILE), 0))
        for block in range(blocks):
            totals = []
            for i in range(8 * block, 8 * block + 8):
                counts = lax.dot_general(
                    hot(src[i : i + 1, :], cell), hot(dst[i : i + 1, :], cell), (((1,), (1,)), ((), ())),
                    preferred_element_type=jnp.float32,
                )
                staged[side, i] = counts.astype(jnp.bfloat16)
                totals.append(jnp.sum(counts, axis=0, keepdims=True))
            slot_degree[owner, (base + block) * 2 + me.core] = jnp.concatenate(totals, axis=0)
        tile_copy(owner * (groups // 2) + place, side).start()
        return carry

    lax.fori_loop(0, groups, build, 0)

    cell = lax.broadcasted_iota(jnp.int32, (TILE, TILE), 0)
    counted = jnp.zeros((TILE, TILE), jnp.float32)
    for owner in range(2):
        for j in range(8):
            row_hot = (jnp.broadcast_to(metas_ref[owner, j : j + 1, :] % 256, (TILE, TILE)) == cell).astype(jnp.float32)
            slots = slot_degree[owner, 16 * j : 16 * j + 16].reshape(TILE, TILE)
            counted += jnp.dot(
                row_hot.astype(jnp.bfloat16), slots.astype(jnp.bfloat16), preferred_element_type=jnp.float32
            )
    degree[...] = counted.reshape(16, 8, TILE)
    for i in range(15):
        share_copy(i).start()
    for tick in range(len(TICK_GROUP), ticks):
        for q in range(RAW_CHUNK):
            if 0 <= tick - q < len(stages):
                stages[tick - q](q)
    total = degree[me.col]
    for i in range(15):
        share_copy(i).wait_recv()
        total = total + shares[i]
    root = lax.rsqrt(1.0 + total)
    root_ref[...] = root
    roots[me.core, me.y, me.x_lo] = root
    for i in range(15):
        root_copy(i).start()
    drain()
    for i in range(15):
        root_copy(i).wait_recv()

    def scale(i, carry):
        c, y, x, k = i // 64, (i // 16) % 4, (i // 8) % 2, i % 8
        gathered_ref[c, y, x, k] = (wide(raw[c, y, x, k]) * roots[c, y, x, pl.ds(k, 1), :]).astype(jnp.bfloat16)
        return carry

    lax.fori_loop(0, 128, scale, 0, unroll=4)
    for i in range(15):
        share_copy(i).wait_send()
        root_copy(i).wait_send()
    give_lists.wait_send()
    give_meta.wait_send()
    for side in range(2):
        tile_copy(0, side).wait()


TICK_GROUP = (0, 4, 7, 10, 13)


def sum_kernel(spreads, part_ref, root_ref, hop_ref, *refs):
    me = Place()
    gathered_ref = refs[0] if spreads else None
    scratch = refs[1:] if spreads else refs
    greet(sum_devices(me) + (spread_devices(me) if spreads else []))

    def finish(k, total):
        root = root_ref[pl.ds(k, 1), :]
        hop_ref[k] = (total * root).T.astype(jnp.bfloat16)
        if spreads:
            gathered_ref[me.core, me.y, me.x_lo, k] = (total * (root * root)).astype(jnp.bfloat16)

    begin, stages, drain = sum_stages(me, part_ref, scratch[:7], scratch[7:N_SUM], finish)
    begin()
    if spreads:
        more, drain_spread = spread_stages(me, gathered_ref, scratch[N_SUM:], SUM_CHUNK)
        run_stages(stages + more, SUM_CHUNK)
        drain_spread()
    else:
        run_stages(stages, SUM_CHUNK)
    drain()


VMEM = pl.BlockSpec(memory_space=pltpu.VMEM)
ANY = pl.BlockSpec(memory_space=pl.ANY)
GATHERED = (2, 4, 2, 8, TILE, TILE)


def comm_params(number):
    return pltpu.CompilerParams(collective_id=number, has_side_effects=True, vmem_limit_bytes=32 * 2**20)


def start(features, meta, edges):
    dma = pltpu.SemaphoreType.DMA
    slots = edges.shape[1]
    shape = jax.ShapeDtypeStruct
    f32, bf16, i32 = jnp.float32, jnp.bfloat16, jnp.int32
    return pl.pallas_call(
        start_kernel,
        out_shape=[
            shape((slots // GROUP, GROUP, TILE, TILE), bf16), shape((2, 16, TILE), i32), shape((8, TILE), f32), shape(GATHERED, bf16)
        ],
        in_specs=[VMEM, VMEM, ANY],
        out_specs=[ANY, VMEM, VMEM, VMEM],
        scratch_shapes=[
            pltpu.VMEM((2, 2, slots // 16, 8, TILE), i32),
            pltpu.VMEM(GATHERED, bf16),
            pltpu.VMEM((2, GROUP, TILE, TILE), bf16),
            pltpu.VMEM((2, slots // 8, 8, TILE), f32),
            pltpu.VMEM((16, 8, TILE), f32),
            pltpu.VMEM((15, 8, TILE), f32),
            pltpu.VMEM((2, 4, 2, 8, TILE), f32),
            *[dma] * 5, dma((2,)), *[dma((15,))] * 4,
            *spread_scratch(RAW_CHUNK),
        ],
        compiler_params=comm_params(0),
        name="start_build",
    )(features.reshape(8, TILE, TILE), meta, edges.reshape(2, slots // 16, 2, 8, TILE))


def live_count(metas_ref, core_ref, owner):
    count = metas_ref[owner, 8, 0]
    return count // 16 * 8 + jnp.clip(count % 16 - 8 * core_ref[0], 0, 8)


def shown_group(group, metas_ref, core_ref, half_groups):
    owner = group // half_groups
    last = (live_count(metas_ref, core_ref, owner) - 1) // GROUP
    return owner * half_groups + jnp.minimum(group % half_groups, last)


def apply_kernel(half_groups, metas_ref, core_ref, tiles_ref, x_ref, out_ref, total):
    group = pl.program_id(0)
    owner, place = group // half_groups, group % half_groups

    @pl.when(group == 0)
    def _():
        total[...] = jnp.zeros_like(total)

    @pl.when(place * GROUP < live_count(metas_ref, core_ref, owner))
    def _():
        base = place * GROUP * 2 + 8 * core_ref[0]
        for start in range(0, GROUP, BATCH):
            ids = []
            for i in range(start, start + BATCH):
                slot = base + i // 8 * 16 + i % 8
                ids.append(metas_ref[owner, slot // 128, slot % 128])
            products = [
                jnp.dot(x_ref[owner * 64 + ids[j] // 256], tiles_ref[0, start + j], preferred_element_type=jnp.float32)
                for j in range(BATCH)
            ]
            for j, product in enumerate(products):
                total[ids[j] % 256] += product

    @pl.when(group == pl.num_programs(0) - 1)
    def _():
        out_ref[...] = total[...].astype(jnp.bfloat16)


def apply_tiles(metas, core, tiles, x):
    groups = tiles.shape[0]
    half_groups = groups // 2
    return pl.pallas_call(
        functools.partial(apply_kernel, half_groups),
        grid_spec=pltpu.PrefetchScalarGridSpec(
            num_scalar_prefetch=2,
            grid=(groups,),
            in_specs=[
                pl.BlockSpec(
                    (1, GROUP, TILE, TILE), lambda g, m, c: (shown_group(g, m, c, half_groups), 0, 0, 0)
                ),
                pl.BlockSpec(x.shape, lambda g, m, c: (0, 0, 0)),
            ],
            out_specs=pl.BlockSpec((TILE, TILE, TILE), lambda g, m, c: (0, 0, 0)),
            scratch_shapes=[pltpu.VMEM((TILE, TILE, TILE), jnp.float32)],
        ),
        out_shape=jax.ShapeDtypeStruct((TILE, TILE, TILE), jnp.bfloat16),
        compiler_params=pltpu.CompilerParams(vmem_limit_bytes=40 * 2**20),
        name="apply_tiles",
    )(metas, core, tiles, x)


def sum_parts(part, root, spreads):
    hop = jax.ShapeDtypeStruct((8, TILE, TILE), jnp.bfloat16)
    gathered = jax.ShapeDtypeStruct(GATHERED, jnp.bfloat16)
    return pl.pallas_call(
        functools.partial(sum_kernel, spreads),
        out_shape=[hop, gathered] if spreads else [hop],
        in_specs=[ANY, VMEM],
        out_specs=[VMEM, VMEM] if spreads else [VMEM],
        scratch_shapes=sum_scratch() + (spread_scratch(SUM_CHUNK) if spreads else []),
        compiler_params=comm_params(1 if spreads else 2),
        name="sum_spread" if spreads else "sum_last",
    )(part.reshape(2, 4, 2, 8, TILE, TILE), root)


def local(features, tile_rows, tile_cols, edge_lists, tile_counts):
    edges = edge_lists.reshape(2, *edge_lists.shape[3:])
    places = (tile_rows + 256 * tile_cols).reshape(8, TILE)
    meta = jnp.concatenate([places, jnp.broadcast_to(tile_counts, (8, TILE))], axis=0)
    core = (lax.axis_index("col") % 2).astype(jnp.int32).reshape(1)
    tiles, metas, root, gathered = start(features, meta, edges)
    part = apply_tiles(metas, core, tiles, gathered.reshape(128, TILE, TILE))
    hop_one, gathered = sum_parts(part, root, True)
    part = apply_tiles(metas, core, tiles, gathered.reshape(128, TILE, TILE))
    (hop_two,) = sum_parts(part, root, False)
    return (hop_one.reshape(features.shape), hop_two.reshape(features.shape))


def solution(mesh):
    placed = (
        P(("row", "col"), None),
        P("row", "col", None),
        P("row", "col", None),
        P(None, "row", "col", None, None),
        P("row", "col"),
    )
    return jax.shard_map(
        local,
        mesh=mesh,
        in_specs=placed,
        out_specs=(P(("row", "col"), None), P(("row", "col"), None)),
        check_vma=False,
    )
```

```python
import functools

import jax
import jax.numpy as jnp
from jax import lax
from jax.experimental import pallas as pl
from jax.experimental.pallas import tpu as pltpu
from jax.sharding import PartitionSpec as P

TILE = 128
GROUP = 64
BATCH = 8
SUM_CHUNK = 8
RAW_CHUNK = 2
SUM_LAGS = (0, 2, 4, 6, 6, 8, 10, 10, 12)


MESH = pl.DeviceIdType.MESH


class Place:
    def __init__(self):
        self.row, self.col = lax.axis_index("row"), lax.axis_index("col")
        self.y, self.x_lo = self.row // 2, self.row % 2
        self.x_hi, self.z, self.core = self.col // 8, (self.col // 2) % 4, self.col % 2

    def at(self, y=None, x_lo=None, x_hi=None, z=None, core=None):
        pick = lambda new, old: old if new is None else new
        row = pick(y, self.y) * 2 + pick(x_lo, self.x_lo)
        col = (pick(x_hi, self.x_hi) * 4 + pick(z, self.z)) * 2 + pick(core, self.core)
        return (row, col)


def greet(devices):
    barrier = pltpu.get_barrier_semaphore()
    for device in devices:
        pl.semaphore_signal(barrier, inc=1, device_id=device, device_id_type=MESH)
    pl.semaphore_wait(barrier, len(devices))


def sum_devices(me):
    return [
        me.at(core=1 - me.core),
        me.at(z=(me.z + 1) % 4),
        me.at(z=(me.z + 3) % 4),
        me.at(x_hi=1 - me.x_hi),
    ]


def spread_devices(me):
    return [me.at(x_lo=1 - me.x_lo), me.at(y=(me.y + 1) % 4), me.at(y=(me.y + 3) % 4)]


def run_stages(stages, lags, chunks):
    for tick in range(max(lags) + chunks):
        for stage, lag in zip(stages, lags):
            if 0 <= tick - lag < chunks:
                stage(tick - lag)


def each_tile(q, chunks, body):
    size = 8 // chunks

    def step(i, carry):
        body(q * size + i)
        return carry

    lax.fori_loop(0, size, step, 0)


def span(q, chunks):
    return pl.ds(q * (8 // chunks), 8 // chunks)


def wide(x):
    return x.astype(jnp.float32)


def sum_stages(me, part, bufs, sems, finish):
    own, given, running, arrived, kept, across, crossed = bufs
    own_sem, pair_send, pair_recv, ring_send, ring_recv, far_send, far_recv = sems
    chunks = SUM_CHUNK

    def own_copy(q):
        return pltpu.make_async_copy(
            part.at[:, :, me.core, span(q, chunks)], own.at[:, :, span(q, chunks)], own_sem.at[q]
        )

    def pair_copy(q):
        return pltpu.make_async_remote_copy(
            part.at[:, :, 1 - me.core, span(q, chunks)], given.at[:, :, span(q, chunks)],
            pair_send.at[q], pair_recv.at[q],
            device_id=me.at(core=1 - me.core), device_id_type=MESH,
        )

    def ring_copy(half, step, q):
        up = (half == 0) == (step < 2)
        return pltpu.make_async_remote_copy(
            running.at[half, step, span(q, chunks)], arrived.at[half, step, span(q, chunks)],
            ring_send.at[half, step, q], ring_recv.at[half, step, q],
            device_id=me.at(z=(me.z + (1 if up else 3)) % 4), device_id_type=MESH,
        )

    def far_copy(q):
        return pltpu.make_async_remote_copy(
            across.at[span(q, chunks)], crossed.at[span(q, chunks)], far_send.at[q], far_recv.at[q],
            device_id=me.at(x_hi=1 - me.x_hi), device_id_type=MESH,
        )

    def begin():
        for q in range(chunks):
            own_copy(q).start()
            pair_copy(q).start()

    def local_sum(half, offset, k):
        x_hi = me.x_hi if half == 0 else 1 - me.x_hi
        z = (me.z + (offset if half == 0 else 4 - offset)) % 4
        return wide(own[x_hi, z, k]) + wide(given[x_hi, z, k])

    def first(q):
        own_copy(q).wait()
        pair_copy(q).wait_recv()
        for step, offset in ((0, 2), (2, 3)):
            for half in (1, 0):
                def body(k, half=half, step=step, offset=offset):
                    running[half, step, k] = local_sum(half, offset, k).astype(jnp.bfloat16)

                each_tile(q, chunks, body)
                ring_copy(half, step, q).start()

    def middle(q):
        for half in (1, 0):
            ring_copy(half, 0, q).wait_recv()

            def body(k, half=half):
                running[half, 1, k] = (local_sum(half, 1, k) + wide(arrived[half, 0, k])).astype(jnp.bfloat16)

            each_tile(q, chunks, body)
            ring_copy(half, 1, q).start()

    def last(q):
        for half in (1, 0):
            ring_copy(half, 2, q).wait_recv()
            ring_copy(half, 1, q).wait_recv()

            def body(k, half=half):
                total = local_sum(half, 0, k) + (wide(arrived[half, 1, k]) + wide(arrived[half, 2, k]))
                if half == 1:
                    across[k] = total.astype(jnp.bfloat16)
                else:
                    kept[k] = total

            each_tile(q, chunks, body)
            if half == 1:
                far_copy(q).start()

    def done(q):
        far_copy(q).wait_recv()
        each_tile(q, chunks, lambda k: finish(k, kept[k] + wide(crossed[k])))

    def drain():
        for q in range(chunks):
            pair_copy(q).wait_send()
            far_copy(q).wait_send()
            for half in (0, 1):
                for step in range(3):
                    ring_copy(half, step, q).wait_send()

    return begin, [first, middle, last, done], drain


def sum_scratch():
    block = lambda *lead, dtype=jnp.bfloat16: pltpu.VMEM((*lead, 8, TILE, TILE), dtype)
    dma = pltpu.SemaphoreType.DMA
    bufs = [block(2, 4), block(2, 4), block(2, 3), block(2, 3), block(dtype=jnp.float32), block(), block()]
    sems = [dma((SUM_CHUNK,))] * 3 + [dma((2, 3, SUM_CHUNK))] * 2 + [dma((SUM_CHUNK,))] * 2
    return bufs + sems


N_SUM = 14


def spread_stages(me, gathered, sems, chunks):
    side_send, side_recv, near_send, near_recv, relay_send, relay_recv, pass_send, pass_recv = sems

    def copy(block, send, recv, device):
        return pltpu.make_async_remote_copy(block, block, send, recv, device_id=device, device_id_type=MESH)

    def block(y, x_lo, q):
        return gathered.at[me.core, (me.y + y) % 4, me.x_lo if x_lo == 0 else 1 - me.x_lo, span(q, chunks)]

    def side_copy(q):
        return copy(block(0, 0, q), side_send.at[q], side_recv.at[q], me.at(x_lo=1 - me.x_lo))

    def near_copy(kind, way, q):
        device = me.at(y=(me.y + (1 if way == 0 else 3)) % 4)
        return copy(block(0, kind, q), near_send.at[kind, way, q], near_recv.at[kind, way, q], device)

    def relay_copy(way, q):
        device = me.at(y=(me.y + (1 if way == 0 else 3)) % 4)
        return copy(block(3 if way == 0 else 1, way, q), relay_send.at[way, q], relay_recv.at[way, q], device)

    def pass_copy(y, x_lo, q):
        return copy(block(y, x_lo, q), pass_send.at[y, x_lo, q], pass_recv.at[y, x_lo, q], me.at(core=1 - me.core))

    def own(q):
        side_copy(q).start()
        near_copy(0, 0, q).start()
        near_copy(0, 1, q).start()
        pass_copy(0, 0, q).start()

    def beside(q):
        side_copy(q).wait_recv()
        near_copy(1, 0, q).start()
        near_copy(1, 1, q).start()
        pass_copy(0, 1, q).start()

    def relay_own(q):
        near_copy(0, 0, q).wait_recv()
        relay_copy(0, q).start()
        pass_copy(3, 0, q).start()

    def relay_beside(q):
        near_copy(1, 1, q).wait_recv()
        relay_copy(1, q).start()
        pass_copy(1, 1, q).start()

    def opposite(q):
        near_copy(0, 1, q).wait_recv()
        pass_copy(1, 0, q).start()
        near_copy(1, 0, q).wait_recv()
        pass_copy(3, 1, q).start()
        for way in (0, 1):
            relay_copy(way, q).wait_recv()
            pass_copy(2, way, q).start()

    def drain():
        for q in range(chunks):
            for y in range(4):
                for x_lo in range(2):
                    pass_copy(y, x_lo, q).wait_recv()
        for q in range(chunks):
            side_copy(q).wait_send()
            for way in (0, 1):
                near_copy(0, way, q).wait_send()
                near_copy(1, way, q).wait_send()
                relay_copy(way, q).wait_send()
            for y in range(4):
                for x_lo in range(2):
                    pass_copy(y, x_lo, q).wait_send()

    return [own, beside, relay_own, relay_beside, opposite], drain


def spread_scratch(chunks):
    dma = pltpu.SemaphoreType.DMA
    return [dma((chunks,))] * 2 + [dma((2, 2, chunks))] * 2 + [dma((2, chunks))] * 2 + [dma((4, 2, chunks))] * 2


def hot(ids, cell):
    return jnp.where(jnp.broadcast_to(ids, (TILE, TILE)) == cell, jnp.bfloat16(1), jnp.bfloat16(0))


def narrow(x):
    return x.astype(jnp.float32).astype(jnp.bfloat16)


def start_kernel(
    features_ref, meta_ref, edges_ref, tiles_ref, metas_ref, root_ref, gathered_ref,
    lists, raw, staged, slot_degree, degree, shares, roots,
    list_sem, list_send, list_recv, meta_send, meta_recv, tile_sem, share_send, share_recv, root_send, root_recv, *sems,
):
    me = Place()
    peers = [lax.rem(me.col + i, 16) for i in range(1, 16)]
    across = me.col + 1 - 2 * me.core
    friends = [(lax.rem(me.row + i % 8, 8), me.col if i < 8 else across) for i in range(1, 16)]
    greet([(me.row, peer) for peer in peers] + [friend for i, friend in enumerate(friends) if i != 7])
    partner = me.at(core=1 - me.core)

    own_lists = pltpu.make_async_copy(edges_ref.at[:, :, me.core], lists.at[me.core], list_sem)
    give_lists = pltpu.make_async_remote_copy(
        edges_ref.at[:, :, 1 - me.core], lists.at[me.core], list_send, list_recv, device_id=partner, device_id_type=MESH
    )
    give_meta = pltpu.make_async_remote_copy(
        meta_ref, metas_ref.at[me.core], meta_send, meta_recv, device_id=partner, device_id_type=MESH
    )

    def tile_copy(group, side):
        return pltpu.make_async_copy(staged.at[side], tiles_ref.at[group], tile_sem.at[side])

    def share_copy(i):
        return pltpu.make_async_remote_copy(
            degree.at[peers[i]], shares.at[i], share_send.at[i], share_recv.at[i],
            device_id=(me.row, peers[i]), device_id_type=MESH,
        )

    def root_copy(i):
        block = roots.at[me.core, me.y, me.x_lo]
        return pltpu.make_async_remote_copy(
            block, block, root_send.at[i], root_recv.at[i], device_id=friends[i], device_id_type=MESH
        )

    own_lists.start()
    give_lists.start()
    give_meta.start()
    metas_ref[me.core] = meta_ref[...]

    def turn(k, carry):
        raw[me.core, me.y, me.x_lo, k] = wide(features_ref[k]).T.astype(jnp.bfloat16)
        return carry

    lax.fori_loop(0, 8, turn, 0)
    slot_degree[...] = jnp.zeros_like(slot_degree)
    stages, drain = spread_stages(me, raw, sems, RAW_CHUNK)
    ticks = len(stages) + RAW_CHUNK - 1
    groups = 2 * lists.shape[2] * 8 // GROUP
    blocks = GROUP // 8
    own_lists.wait()

    def build(group, carry):
        for tick, when in enumerate(TICK_GROUP):
            @pl.when(group == when)
            def _(tick=tick):
                for q in range(RAW_CHUNK):
                    if 0 <= tick - q < len(stages):
                        stages[tick - q](q)

        @pl.when(group == groups // 2)
        def _():
            give_lists.wait_recv()
            give_meta.wait_recv()

        half = group // (groups // 2)
        place = group % (groups // 2)
        owner = me.core + half * (1 - 2 * me.core)
        side = group % 2
        base = place * blocks

        @pl.when(group >= 2)
        def _():
            tile_copy(0, side).wait()

        shape = (blocks, 8, TILE)
        slot = (lax.broadcasted_iota(jnp.int32, shape, 0) + base) * 16 + 8 * me.core + lax.broadcasted_iota(jnp.int32, shape, 1)
        live = slot < jnp.broadcast_to(metas_ref[owner, 8:9, :].reshape(1, 1, TILE), shape)
        dst = jnp.where(live, lists[owner, 0, pl.ds(base, blocks)], -1).reshape(GROUP, TILE)
        src = lists[owner, 1, pl.ds(base, blocks)].reshape(GROUP, TILE)
        dst, src = narrow(dst), narrow(src)
        cell = narrow(lax.broadcasted_iota(jnp.int32, (TILE, TILE), 0))
        for block in range(blocks):
            totals = []
            for i in range(8 * block, 8 * block + 8):
                counts = lax.dot_general(
                    hot(src[i : i + 1, :], cell), hot(dst[i : i + 1, :], cell), (((1,), (1,)), ((), ())),
                    preferred_element_type=jnp.float32,
                )
                staged[side, i] = counts.astype(jnp.bfloat16)
                totals.append(jnp.sum(counts, axis=0, keepdims=True))
            slot_degree[owner, (base + block) * 2 + me.core] = jnp.concatenate(totals, axis=0)
        tile_copy(owner * (groups // 2) + place, side).start()
        return carry

    lax.fori_loop(0, groups, build, 0)

    cell = lax.broadcasted_iota(jnp.int32, (TILE, TILE), 0)
    counted = jnp.zeros((TILE, TILE), jnp.float32)
    for owner in range(2):
        for j in range(8):
            row_hot = (jnp.broadcast_to(metas_ref[owner, j : j + 1, :] % 256, (TILE, TILE)) == cell).astype(jnp.float32)
            slots = slot_degree[owner, 16 * j : 16 * j + 16].reshape(TILE, TILE)
            counted += jnp.dot(
                row_hot.astype(jnp.bfloat16), slots.astype(jnp.bfloat16), preferred_element_type=jnp.float32
            )
    degree[...] = counted.reshape(16, 8, TILE)
    for i in range(15):
        share_copy(i).start()
    for tick in range(len(TICK_GROUP), ticks):
        for q in range(RAW_CHUNK):
            if 0 <= tick - q < len(stages):
                stages[tick - q](q)
    total = degree[me.col]
    for i in range(15):
        share_copy(i).wait_recv()
        total = total + shares[i]
    root = lax.rsqrt(1.0 + total)
    root_ref[...] = root
    roots[me.core, me.y, me.x_lo] = root
    for i in range(15):
        root_copy(i).start()
    drain()
    for i in range(15):
        root_copy(i).wait_recv()

    def scale(i, carry):
        c, y, x, k = i // 64, (i // 16) % 4, (i // 8) % 2, i % 8
        gathered_ref[c, y, x, k] = (wide(raw[c, y, x, k]) * roots[c, y, x, pl.ds(k, 1), :]).astype(jnp.bfloat16)
        return carry

    lax.fori_loop(0, 128, scale, 0, unroll=4)
    for i in range(15):
        share_copy(i).wait_send()
        root_copy(i).wait_send()
    give_lists.wait_send()
    give_meta.wait_send()
    for side in range(2):
        tile_copy(0, side).wait()


TICK_GROUP = (0, 4, 7, 10, 13)


def sum_kernel(spreads, part_ref, root_ref, hop_ref, *refs):
    me = Place()
    gathered_ref = refs[0] if spreads else None
    scratch = refs[1:] if spreads else refs
    greet(sum_devices(me) + (spread_devices(me) if spreads else []))

    def finish(k, total):
        root = root_ref[pl.ds(k, 1), :]
        hop_ref[k] = (total * root).T.astype(jnp.bfloat16)
        if spreads:
            gathered_ref[me.core, me.y, me.x_lo, k] = (total * (root * root)).astype(jnp.bfloat16)

    begin, stages, drain = sum_stages(me, part_ref, scratch[:7], scratch[7:N_SUM], finish)
    begin()
    if spreads:
        more, drain_spread = spread_stages(me, gathered_ref, scratch[N_SUM:], SUM_CHUNK)
        run_stages(stages + more, SUM_LAGS, SUM_CHUNK)
        drain_spread()
    else:
        run_stages(stages, SUM_LAGS[:4], SUM_CHUNK)
    drain()


VMEM = pl.BlockSpec(memory_space=pltpu.VMEM)
ANY = pl.BlockSpec(memory_space=pl.ANY)
GATHERED = (2, 4, 2, 8, TILE, TILE)


def comm_params(number):
    return pltpu.CompilerParams(collective_id=number, has_side_effects=True, vmem_limit_bytes=32 * 2**20)


def start(features, meta, edges):
    dma = pltpu.SemaphoreType.DMA
    slots = edges.shape[1]
    shape = jax.ShapeDtypeStruct
    f32, bf16, i32 = jnp.float32, jnp.bfloat16, jnp.int32
    return pl.pallas_call(
        start_kernel,
        out_shape=[
            shape((slots // GROUP, GROUP, TILE, TILE), bf16), shape((2, 16, TILE), i32), shape((8, TILE), f32), shape(GATHERED, bf16)
        ],
        in_specs=[VMEM, VMEM, ANY],
        out_specs=[ANY, VMEM, VMEM, VMEM],
        scratch_shapes=[
            pltpu.VMEM((2, 2, slots // 16, 8, TILE), i32),
            pltpu.VMEM(GATHERED, bf16),
            pltpu.VMEM((2, GROUP, TILE, TILE), bf16),
            pltpu.VMEM((2, slots // 8, 8, TILE), f32),
            pltpu.VMEM((16, 8, TILE), f32),
            pltpu.VMEM((15, 8, TILE), f32),
            pltpu.VMEM((2, 4, 2, 8, TILE), f32),
            *[dma] * 5, dma((2,)), *[dma((15,))] * 4,
            *spread_scratch(RAW_CHUNK),
        ],
        compiler_params=comm_params(0),
        name="start_build",
    )(features.reshape(8, TILE, TILE), meta, edges.reshape(2, slots // 16, 2, 8, TILE))


def live_count(metas_ref, core_ref, owner):
    count = metas_ref[owner, 8, 0]
    return count // 16 * 8 + jnp.clip(count % 16 - 8 * core_ref[0], 0, 8)


def shown_group(group, metas_ref, core_ref, half_groups):
    owner = group // half_groups
    last = (live_count(metas_ref, core_ref, owner) - 1) // GROUP
    return owner * half_groups + jnp.minimum(group % half_groups, last)


def apply_kernel(half_groups, metas_ref, core_ref, tiles_ref, x_ref, out_ref, total):
    group = pl.program_id(0)
    owner, place = group // half_groups, group % half_groups

    @pl.when(group == 0)
    def _():
        total[...] = jnp.zeros_like(total)

    @pl.when(place * GROUP < live_count(metas_ref, core_ref, owner))
    def _():
        base = place * GROUP * 2 + 8 * core_ref[0]
        for start in range(0, GROUP, BATCH):
            ids = []
            for i in range(start, start + BATCH):
                slot = base + i // 8 * 16 + i % 8
                ids.append(metas_ref[owner, slot // 128, slot % 128])
            products = [
                jnp.dot(x_ref[owner * 64 + ids[j] // 256], tiles_ref[0, start + j], preferred_element_type=jnp.float32)
                for j in range(BATCH)
            ]
            for j, product in enumerate(products):
                total[ids[j] % 256] += product

    @pl.when(group == pl.num_programs(0) - 1)
    def _():
        out_ref[...] = total[...].astype(jnp.bfloat16)


def apply_tiles(metas, core, tiles, x):
    groups = tiles.shape[0]
    half_groups = groups // 2
    return pl.pallas_call(
        functools.partial(apply_kernel, half_groups),
        grid_spec=pltpu.PrefetchScalarGridSpec(
            num_scalar_prefetch=2,
            grid=(groups,),
            in_specs=[
                pl.BlockSpec(
                    (1, GROUP, TILE, TILE), lambda g, m, c: (shown_group(g, m, c, half_groups), 0, 0, 0)
                ),
                pl.BlockSpec(x.shape, lambda g, m, c: (0, 0, 0)),
            ],
            out_specs=pl.BlockSpec((TILE, TILE, TILE), lambda g, m, c: (0, 0, 0)),
            scratch_shapes=[pltpu.VMEM((TILE, TILE, TILE), jnp.float32)],
        ),
        out_shape=jax.ShapeDtypeStruct((TILE, TILE, TILE), jnp.bfloat16),
        compiler_params=pltpu.CompilerParams(vmem_limit_bytes=40 * 2**20),
        name="apply_tiles",
    )(metas, core, tiles, x)


def sum_parts(part, root, spreads):
    hop = jax.ShapeDtypeStruct((8, TILE, TILE), jnp.bfloat16)
    gathered = jax.ShapeDtypeStruct(GATHERED, jnp.bfloat16)
    return pl.pallas_call(
        functools.partial(sum_kernel, spreads),
        out_shape=[hop, gathered] if spreads else [hop],
        in_specs=[ANY, VMEM],
        out_specs=[VMEM, VMEM] if spreads else [VMEM],
        scratch_shapes=sum_scratch() + (spread_scratch(SUM_CHUNK) if spreads else []),
        compiler_params=comm_params(1 if spreads else 2),
        name="sum_spread" if spreads else "sum_last",
    )(part.reshape(2, 4, 2, 8, TILE, TILE), root)


def local(features, tile_rows, tile_cols, edge_lists, tile_counts):
    edges = edge_lists.reshape(2, *edge_lists.shape[3:])
    places = (tile_rows + 256 * tile_cols).reshape(8, TILE)
    meta = jnp.concatenate([places, jnp.broadcast_to(tile_counts, (8, TILE))], axis=0)
    core = (lax.axis_index("col") % 2).astype(jnp.int32).reshape(1)
    tiles, metas, root, gathered = start(features, meta, edges)
    part = apply_tiles(metas, core, tiles, gathered.reshape(128, TILE, TILE))
    hop_one, gathered = sum_parts(part, root, True)
    part = apply_tiles(metas, core, tiles, gathered.reshape(128, TILE, TILE))
    (hop_two,) = sum_parts(part, root, False)
    return (hop_one.reshape(features.shape), hop_two.reshape(features.shape))


def solution(mesh):
    placed = (
        P(("row", "col"), None),
        P("row", "col", None),
        P("row", "col", None),
        P(None, "row", "col", None, None),
        P("row", "col"),
    )
    return jax.shard_map(
        local,
        mesh=mesh,
        in_specs=placed,
        out_specs=(P(("row", "col"), None), P(("row", "col"), None)),
        check_vma=False,
    )
```

```python
import functools

import jax
import jax.numpy as jnp
from jax import lax
from jax.experimental import pallas as pl
from jax.experimental.pallas import tpu as pltpu
from jax.sharding import PartitionSpec as P

TILE = 128
GROUP = 64
BATCH = 8
SUM_CHUNK = 8
RAW_CHUNK = 2
START_LIMIT = 42 * 2**20
APPLY_LIMIT = 34 * 2**20
SUM_LIMIT = 12 * 2**20
SUM_LAGS = (0, 2, 4, 6, 6, 8, 10, 10, 12)


MESH = pl.DeviceIdType.MESH


class Place:
    def __init__(self):
        self.row, self.col = lax.axis_index("row"), lax.axis_index("col")
        self.y, self.x_lo = self.row // 2, self.row % 2
        self.x_hi, self.z, self.core = self.col // 8, (self.col // 2) % 4, self.col % 2

    def at(self, y=None, x_lo=None, x_hi=None, z=None, core=None):
        pick = lambda new, old: old if new is None else new
        row = pick(y, self.y) * 2 + pick(x_lo, self.x_lo)
        col = (pick(x_hi, self.x_hi) * 4 + pick(z, self.z)) * 2 + pick(core, self.core)
        return (row, col)


def greet(devices):
    barrier = pltpu.get_barrier_semaphore()
    for device in devices:
        pl.semaphore_signal(barrier, inc=1, device_id=device, device_id_type=MESH)
    pl.semaphore_wait(barrier, len(devices))


def sum_devices(me):
    return [
        me.at(core=1 - me.core),
        me.at(z=(me.z + 1) % 4),
        me.at(z=(me.z + 3) % 4),
        me.at(x_hi=1 - me.x_hi),
    ]


def spread_devices(me):
    return [me.at(x_lo=1 - me.x_lo), me.at(y=(me.y + 1) % 4), me.at(y=(me.y + 3) % 4)]


def run_stages(stages, lags, chunks):
    for tick in range(max(lags) + chunks):
        for stage, lag in zip(stages, lags):
            if 0 <= tick - lag < chunks:
                stage(tick - lag)


def each_tile(q, chunks, body):
    size = 8 // chunks

    def step(i, carry):
        body(q * size + i)
        return carry

    lax.fori_loop(0, size, step, 0)


def span(q, chunks):
    return pl.ds(q * (8 // chunks), 8 // chunks)


def wide(x):
    return x.astype(jnp.float32)


def sum_stages(me, part, bufs, sems, finish):
    given, running, arrived, kept, across, crossed = bufs
    pair_send, pair_recv, ring_send, ring_recv, far_send, far_recv = sems
    chunks = SUM_CHUNK

    def pair_copy(q):
        return pltpu.make_async_remote_copy(
            part.at[:, :, 1 - me.core, span(q, chunks)], given.at[:, :, span(q, chunks)],
            pair_send.at[q], pair_recv.at[q],
            device_id=me.at(core=1 - me.core), device_id_type=MESH,
        )

    def ring_copy(half, step, q):
        up = (half == 0) == (step < 2)
        return pltpu.make_async_remote_copy(
            running.at[half, step, span(q, chunks)], arrived.at[half, step, span(q, chunks)],
            ring_send.at[half, step, q], ring_recv.at[half, step, q],
            device_id=me.at(z=(me.z + (1 if up else 3)) % 4), device_id_type=MESH,
        )

    def far_copy(q):
        return pltpu.make_async_remote_copy(
            across.at[span(q, chunks)], crossed.at[span(q, chunks)], far_send.at[q], far_recv.at[q],
            device_id=me.at(x_hi=1 - me.x_hi), device_id_type=MESH,
        )

    def begin():
        for q in range(chunks):
            pair_copy(q).start()

    def local_sum(half, offset, k):
        x_hi = me.x_hi if half == 0 else 1 - me.x_hi
        z = (me.z + (offset if half == 0 else 4 - offset)) % 4
        return part[x_hi, z, me.core, k] + given[x_hi, z, k]

    def first(q):
        pair_copy(q).wait_recv()
        for step, offset in ((0, 2), (2, 3)):
            for half in (1, 0):
                def body(k, half=half, step=step, offset=offset):
                    running[half, step, k] = local_sum(half, offset, k).astype(jnp.bfloat16)

                each_tile(q, chunks, body)
                ring_copy(half, step, q).start()

    def middle(q):
        for half in (1, 0):
            ring_copy(half, 0, q).wait_recv()

            def body(k, half=half):
                running[half, 1, k] = (local_sum(half, 1, k) + wide(arrived[half, 0, k])).astype(jnp.bfloat16)

            each_tile(q, chunks, body)
            ring_copy(half, 1, q).start()

    def last(q):
        for half in (1, 0):
            ring_copy(half, 2, q).wait_recv()
            ring_copy(half, 1, q).wait_recv()

            def body(k, half=half):
                total = local_sum(half, 0, k) + (wide(arrived[half, 1, k]) + wide(arrived[half, 2, k]))
                if half == 1:
                    across[k] = total.astype(jnp.bfloat16)
                else:
                    kept[k] = total

            each_tile(q, chunks, body)
            if half == 1:
                far_copy(q).start()

    def done(q):
        far_copy(q).wait_recv()
        each_tile(q, chunks, lambda k: finish(k, kept[k] + wide(crossed[k])))

    def drain():
        for q in range(chunks):
            pair_copy(q).wait_send()
            far_copy(q).wait_send()
            for half in (0, 1):
                for step in range(3):
                    ring_copy(half, step, q).wait_send()

    return begin, [first, middle, last, done], drain


def sum_scratch():
    block = lambda *lead, dtype=jnp.bfloat16: pltpu.VMEM((*lead, 8, TILE, TILE), dtype)
    dma = pltpu.SemaphoreType.DMA
    bufs = [block(2, 4, dtype=jnp.float32), block(2, 3), block(2, 3), block(dtype=jnp.float32), block(), block()]
    sems = [dma((SUM_CHUNK,))] * 2 + [dma((2, 3, SUM_CHUNK))] * 2 + [dma((SUM_CHUNK,))] * 2
    return bufs + sems


N_SUM = 12


def spread_stages(me, gathered, sems, chunks):
    side_send, side_recv, near_send, near_recv, relay_send, relay_recv, pass_send, pass_recv = sems

    def copy(block, send, recv, device):
        return pltpu.make_async_remote_copy(block, block, send, recv, device_id=device, device_id_type=MESH)

    def block(y, x_lo, q):
        return gathered.at[me.core, (me.y + y) % 4, me.x_lo if x_lo == 0 else 1 - me.x_lo, span(q, chunks)]

    def side_copy(q):
        return copy(block(0, 0, q), side_send.at[q], side_recv.at[q], me.at(x_lo=1 - me.x_lo))

    def near_copy(kind, way, q):
        device = me.at(y=(me.y + (1 if way == 0 else 3)) % 4)
        return copy(block(0, kind, q), near_send.at[kind, way, q], near_recv.at[kind, way, q], device)

    def relay_copy(way, q):
        device = me.at(y=(me.y + (1 if way == 0 else 3)) % 4)
        return copy(block(3 if way == 0 else 1, way, q), relay_send.at[way, q], relay_recv.at[way, q], device)

    def pass_copy(y, x_lo, q):
        return copy(block(y, x_lo, q), pass_send.at[y, x_lo, q], pass_recv.at[y, x_lo, q], me.at(core=1 - me.core))

    def own(q):
        side_copy(q).start()
        near_copy(0, 0, q).start()
        near_copy(0, 1, q).start()
        pass_copy(0, 0, q).start()

    def beside(q):
        side_copy(q).wait_recv()
        near_copy(1, 0, q).start()
        near_copy(1, 1, q).start()
        pass_copy(0, 1, q).start()

    def relay_own(q):
        near_copy(0, 0, q).wait_recv()
        relay_copy(0, q).start()
        pass_copy(3, 0, q).start()

    def relay_beside(q):
        near_copy(1, 1, q).wait_recv()
        relay_copy(1, q).start()
        pass_copy(1, 1, q).start()

    def opposite(q):
        near_copy(0, 1, q).wait_recv()
        pass_copy(1, 0, q).start()
        near_copy(1, 0, q).wait_recv()
        pass_copy(3, 1, q).start()
        for way in (0, 1):
            relay_copy(way, q).wait_recv()
            pass_copy(2, way, q).start()

    def drain():
        for q in range(chunks):
            for y in range(4):
                for x_lo in range(2):
                    pass_copy(y, x_lo, q).wait_recv()
        for q in range(chunks):
            side_copy(q).wait_send()
            for way in (0, 1):
                near_copy(0, way, q).wait_send()
                near_copy(1, way, q).wait_send()
                relay_copy(way, q).wait_send()
            for y in range(4):
                for x_lo in range(2):
                    pass_copy(y, x_lo, q).wait_send()

    return [own, beside, relay_own, relay_beside, opposite], drain


def spread_scratch(chunks):
    dma = pltpu.SemaphoreType.DMA
    return [dma((chunks,))] * 2 + [dma((2, 2, chunks))] * 2 + [dma((2, chunks))] * 2 + [dma((4, 2, chunks))] * 2


def hot(ids, cell):
    return jnp.where(jnp.broadcast_to(ids, (TILE, TILE)) == cell, jnp.bfloat16(1), jnp.bfloat16(0))


def narrow(x):
    return x.astype(jnp.float32).astype(jnp.bfloat16)


def start_kernel(
    count_ref, features_hbm, rows_hbm, cols_hbm, edges_ref, tiles_hbm, metas_ref, root_ref, gathered_ref,
    tiles_ref, features_ref, meta, lists, raw, slot_degree, degree, shares, roots,
    tile_sem, load_sem, list_sem, list_send, list_recv, meta_send, meta_recv, share_send, share_recv, root_send, root_recv, *sems,
):
    me = Place()
    peers = [lax.rem(me.col + i, 16) for i in range(1, 16)]
    across = me.col + 1 - 2 * me.core
    friends = [(lax.rem(me.row + i % 8, 8), me.col if i < 8 else across) for i in range(1, 16)]
    loads = [
        pltpu.make_async_copy(rows_hbm, meta.at[pl.ds(0, 8)], load_sem.at[0]),
        pltpu.make_async_copy(cols_hbm, meta.at[pl.ds(8, 8)], load_sem.at[1]),
        pltpu.make_async_copy(features_hbm, features_ref, load_sem.at[2]),
    ]
    own_lists = pltpu.make_async_copy(edges_ref.at[:, :, me.core], lists.at[me.core], list_sem)
    for load in loads:
        load.start()
    own_lists.start()
    meta[16:24, :] = jnp.full((8, TILE), count_ref[0, 0], jnp.int32)
    greet([(me.row, peer) for peer in peers] + [friend for i, friend in enumerate(friends) if i != 7])
    partner = me.at(core=1 - me.core)

    give_lists = pltpu.make_async_remote_copy(
        edges_ref.at[:, :, 1 - me.core], lists.at[me.core], list_send, list_recv, device_id=partner, device_id_type=MESH
    )
    give_meta = pltpu.make_async_remote_copy(
        meta, metas_ref.at[me.core], meta_send, meta_recv, device_id=partner, device_id_type=MESH
    )

    def tile_copy(bank):
        return pltpu.make_async_copy(tiles_ref.at[bank], tiles_hbm.at[bank], tile_sem.at[bank])

    def share_copy(i):
        return pltpu.make_async_remote_copy(
            degree.at[peers[i]], shares.at[i], share_send.at[i], share_recv.at[i],
            device_id=(me.row, peers[i]), device_id_type=MESH,
        )

    def root_copy(i):
        block = roots.at[me.core, me.y, me.x_lo]
        return pltpu.make_async_remote_copy(
            block, block, root_send.at[i], root_recv.at[i], device_id=friends[i], device_id_type=MESH
        )

    give_lists.start()
    for load in loads:
        load.wait()
    give_meta.start()
    metas_ref[me.core] = meta[...]

    def turn(k, carry):
        raw[me.core, me.y, me.x_lo, k] = wide(features_ref[k]).T.astype(jnp.bfloat16)
        return carry

    lax.fori_loop(0, 8, turn, 0)
    slot_degree[...] = jnp.zeros_like(slot_degree)
    stages, drain = spread_stages(me, raw, sems, RAW_CHUNK)
    ticks = len(stages) + RAW_CHUNK - 1
    groups = 2 * lists.shape[2] * 8 // GROUP
    blocks = GROUP // 8
    own_lists.wait()

    def build(group, carry):
        for tick, when in enumerate(TICK_GROUP):
            @pl.when(group == when)
            def _(tick=tick):
                for q in range(RAW_CHUNK):
                    if 0 <= tick - q < len(stages):
                        stages[tick - q](q)

        @pl.when(group == groups // 2)
        def _():
            give_lists.wait_recv()
            give_meta.wait_recv()

        half = group // (groups // 2)
        place = group % (groups // 2)
        owner = me.core + half * (1 - 2 * me.core)
        bank = owner * (groups // 2) + place
        base = place * blocks

        shape = (blocks, 8, TILE)
        slot = (lax.broadcasted_iota(jnp.int32, shape, 0) + base) * 16 + 8 * me.core + lax.broadcasted_iota(jnp.int32, shape, 1)
        live = slot < jnp.broadcast_to(metas_ref[owner, 16:17, :].reshape(1, 1, TILE), shape)
        dst = jnp.where(live, lists[owner, 0, pl.ds(base, blocks)], -1).reshape(GROUP, TILE)
        src = lists[owner, 1, pl.ds(base, blocks)].reshape(GROUP, TILE)
        dst, src = narrow(dst), narrow(src)
        cell = narrow(lax.broadcasted_iota(jnp.int32, (TILE, TILE), 0))
        for block in range(blocks):
            totals = []
            for i in range(8 * block, 8 * block + 8):
                counts = lax.dot_general(
                    hot(src[i : i + 1, :], cell), hot(dst[i : i + 1, :], cell), (((1,), (1,)), ((), ())),
                    preferred_element_type=jnp.float32,
                )
                tiles_ref[bank, i] = counts.astype(jnp.bfloat16)
                totals.append(jnp.sum(counts, axis=0, keepdims=True))
            slot_degree[owner, (base + block) * 2 + me.core] = jnp.concatenate(totals, axis=0)
        tile_copy(bank).start()
        return carry

    lax.fori_loop(0, groups, build, 0)

    cell = lax.broadcasted_iota(jnp.int32, (TILE, TILE), 0)
    counted = jnp.zeros((TILE, TILE), jnp.float32)
    for owner in range(2):
        for j in range(8):
            row_hot = (jnp.broadcast_to(metas_ref[owner, j : j + 1, :], (TILE, TILE)) == cell).astype(jnp.float32)
            slots = slot_degree[owner, 16 * j : 16 * j + 16].reshape(TILE, TILE)
            counted += jnp.dot(
                row_hot.astype(jnp.bfloat16), slots.astype(jnp.bfloat16), preferred_element_type=jnp.float32
            )
    degree[...] = counted.reshape(16, 8, TILE)
    for i in range(15):
        share_copy(i).start()
    for tick in range(len(TICK_GROUP), ticks):
        for q in range(RAW_CHUNK):
            if 0 <= tick - q < len(stages):
                stages[tick - q](q)
    total = degree[me.col]
    for i in range(15):
        share_copy(i).wait_recv()
        total = total + shares[i]
    root = lax.rsqrt(1.0 + total)
    root_ref[...] = root
    roots[me.core, me.y, me.x_lo] = root
    for i in range(15):
        root_copy(i).start()
    drain()
    for i in range(15):
        root_copy(i).wait_recv()

    def scale(i, carry):
        c, y, x, k = i // 64, (i // 16) % 4, (i // 8) % 2, i % 8
        gathered_ref[c, y, x, k] = (wide(raw[c, y, x, k]) * roots[c, y, x, pl.ds(k, 1), :]).astype(jnp.bfloat16)
        return carry

    lax.fori_loop(0, 128, scale, 0, unroll=4)
    for i in range(15):
        share_copy(i).wait_send()
        root_copy(i).wait_send()
    give_lists.wait_send()
    give_meta.wait_send()
    for bank in range(groups):
        tile_copy(bank).wait()


TICK_GROUP = (0, 4, 7, 10, 13)


def sum_kernel(spreads, part_ref, root_ref, hop_ref, *refs):
    me = Place()
    gathered_ref = refs[0] if spreads else None
    scratch = refs[1:] if spreads else refs
    greet(sum_devices(me) + (spread_devices(me) if spreads else []))

    def finish(k, total):
        root = root_ref[pl.ds(k, 1), :]
        hop_ref[k] = (total * root).T.astype(jnp.bfloat16)
        if spreads:
            gathered_ref[me.core, me.y, me.x_lo, k] = (total * (root * root)).astype(jnp.bfloat16)

    begin, stages, drain = sum_stages(me, part_ref, scratch[:6], scratch[6:N_SUM], finish)
    begin()
    if spreads:
        more, drain_spread = spread_stages(me, gathered_ref, scratch[N_SUM:], SUM_CHUNK)
        run_stages(stages + more, SUM_LAGS, SUM_CHUNK)
        drain_spread()
    else:
        run_stages(stages, SUM_LAGS[:4], SUM_CHUNK)
    drain()


VMEM = pl.BlockSpec(memory_space=pltpu.VMEM)
SMEM = pl.BlockSpec(memory_space=pltpu.SMEM)
HBM = pl.BlockSpec(memory_space=pltpu.HBM)
GATHERED = (2, 4, 2, 8, TILE, TILE)


def comm_params(number, limit):
    return pltpu.CompilerParams(collective_id=number, has_side_effects=True, vmem_limit_bytes=limit)


def start(counts, features, rows, cols, edges):
    dma = pltpu.SemaphoreType.DMA
    slots = edges.shape[1]
    shape = jax.ShapeDtypeStruct
    f32, bf16, i32 = jnp.float32, jnp.bfloat16, jnp.int32
    return pl.pallas_call(
        start_kernel,
        out_shape=[
            shape((slots // GROUP, GROUP, TILE, TILE), bf16), shape((2, 24, TILE), i32), shape((8, TILE), f32), shape(GATHERED, bf16)
        ],
        in_specs=[SMEM, HBM, HBM, HBM, HBM],
        out_specs=[HBM, VMEM, VMEM, VMEM],
        scratch_shapes=[
            pltpu.VMEM((slots // GROUP, GROUP, TILE, TILE), bf16),
            pltpu.VMEM((8, TILE, TILE), bf16),
            pltpu.VMEM((24, TILE), i32),
            pltpu.VMEM((2, 2, slots // 16, 8, TILE), i32),
            pltpu.VMEM(GATHERED, bf16),
            pltpu.VMEM((2, slots // 8, 8, TILE), f32),
            pltpu.VMEM((16, 8, TILE), f32),
            pltpu.VMEM((15, 8, TILE), f32),
            pltpu.VMEM((2, 4, 2, 8, TILE), f32),
            dma((slots // GROUP,)), dma((3,)), *[dma] * 5, *[dma((15,))] * 4,
            *spread_scratch(RAW_CHUNK),
        ],
        compiler_params=comm_params(0, START_LIMIT),
        name="start_build",
    )(
        counts, features.reshape(8, TILE, TILE), rows.reshape(8, TILE), cols.reshape(8, TILE),
        edges.reshape(2, slots // 16, 2, 8, TILE),
    )


def live_count(metas_ref, core, owner):
    count = metas_ref[owner, 16, 0]
    return count // 16 * 8 + jnp.clip(count % 16 - 8 * core, 0, 8)


def apply_kernel(metas_ref, tiles_hbm, x_ref, total, tiles_ref, tile_sem):
    core = lax.axis_index("col") % 2
    half_groups = tiles_ref.shape[0] // 2
    live = [(live_count(metas_ref, core, owner) + GROUP - 1) // GROUP for owner in range(2)]

    def tile_copy(bank):
        return pltpu.make_async_copy(tiles_hbm.at[bank], tiles_ref.at[bank], tile_sem.at[bank])

    for owner in range(2):
        def fetch(place, carry, owner=owner):
            tile_copy(owner * half_groups + place).start()
            return carry

        lax.fori_loop(0, live[owner], fetch, 0)
    total[...] = jnp.zeros_like(total)
    for owner in range(2):
        def apply_group(place, carry, owner=owner):
            base = place * GROUP * 2 + 8 * core
            tile_copy(owner * half_groups + place).wait()
            for start in range(0, GROUP, BATCH):
                slots = [base + i // 8 * 16 + i % 8 for i in range(start, start + BATCH)]
                products = [
                    jnp.dot(
                        x_ref[owner * 64 + metas_ref[owner, 8 + slot // 128, slot % 128]],
                        tiles_ref[owner * half_groups + place, start + j],
                        preferred_element_type=jnp.float32,
                    )
                    for j, slot in enumerate(slots)
                ]
                for slot, product in zip(slots, products):
                    total[metas_ref[owner, slot // 128, slot % 128]] += product
            return carry

        lax.fori_loop(0, live[owner], apply_group, 0)


def apply_tiles(metas, tiles, x):
    return pl.pallas_call(
        apply_kernel,
        in_specs=[SMEM, HBM, VMEM],
        out_specs=VMEM,
        scratch_shapes=[pltpu.VMEM(tiles.shape, tiles.dtype), pltpu.SemaphoreType.DMA((tiles.shape[0],))],
        out_shape=jax.ShapeDtypeStruct((TILE, TILE, TILE), jnp.float32),
        compiler_params=pltpu.CompilerParams(vmem_limit_bytes=APPLY_LIMIT),
        name="apply_tiles",
    )(metas, tiles, x)


def sum_parts(part, root, spreads):
    hop = jax.ShapeDtypeStruct((8, TILE, TILE), jnp.bfloat16)
    gathered = jax.ShapeDtypeStruct(GATHERED, jnp.bfloat16)
    return pl.pallas_call(
        functools.partial(sum_kernel, spreads),
        out_shape=[hop, gathered] if spreads else [hop],
        in_specs=[VMEM, VMEM],
        out_specs=[VMEM, VMEM] if spreads else [VMEM],
        scratch_shapes=sum_scratch() + (spread_scratch(SUM_CHUNK) if spreads else []),
        compiler_params=comm_params(1 if spreads else 2, SUM_LIMIT),
        name="sum_spread" if spreads else "sum_last",
    )(part.reshape(2, 4, 2, 8, TILE, TILE), root)


def local(features, tile_rows, tile_cols, edge_lists, tile_counts):
    edges = edge_lists.reshape(2, *edge_lists.shape[3:])
    tiles, metas, root, gathered = start(tile_counts, features, tile_rows, tile_cols, edges)
    part = apply_tiles(metas, tiles, gathered.reshape(128, TILE, TILE))
    hop_one, gathered = sum_parts(part, root, True)
    part = apply_tiles(metas, tiles, gathered.reshape(128, TILE, TILE))
    (hop_two,) = sum_parts(part, root, False)
    return (hop_one.reshape(features.shape), hop_two.reshape(features.shape))


def solution(mesh):
    placed = (
        P(("row", "col"), None),
        P("row", "col", None),
        P("row", "col", None),
        P(None, "row", "col", None, None),
        P("row", "col"),
    )
    return jax.shard_map(
        local,
        mesh=mesh,
        in_specs=placed,
        out_specs=(P(("row", "col"), None), P(("row", "col"), None)),
        check_vma=False,
    )
```

```python
import functools

import jax
import jax.numpy as jnp
from jax import lax
from jax.experimental import pallas as pl
from jax.experimental.pallas import tpu as pltpu
from jax.sharding import PartitionSpec as P

TILE = 128
GROUP = 64
BATCH = 8
SUM_CHUNK = 8
RAW_CHUNK = 2
START_LIMIT = 42 * 2**20
APPLY_LIMIT = 34 * 2**20
SUM_LIMIT = 12 * 2**20
SUM_LAGS = (0, 2, 4, 6, 6, 8, 10, 10, 12)


MESH = pl.DeviceIdType.MESH


class Place:
    def __init__(self):
        self.row, self.col = lax.axis_index("row"), lax.axis_index("col")
        self.y, self.x_lo = self.row // 2, self.row % 2
        self.x_hi, self.z, self.core = self.col // 8, (self.col // 2) % 4, self.col % 2

    def at(self, y=None, x_lo=None, x_hi=None, z=None, core=None):
        pick = lambda new, old: old if new is None else new
        row = pick(y, self.y) * 2 + pick(x_lo, self.x_lo)
        col = (pick(x_hi, self.x_hi) * 4 + pick(z, self.z)) * 2 + pick(core, self.core)
        return (row, col)


def greet(devices):
    barrier = pltpu.get_barrier_semaphore()
    for device in devices:
        pl.semaphore_signal(barrier, inc=1, device_id=device, device_id_type=MESH)
    pl.semaphore_wait(barrier, len(devices))


def sum_devices(me):
    return [
        me.at(core=1 - me.core),
        me.at(z=(me.z + 1) % 4),
        me.at(z=(me.z + 3) % 4),
        me.at(x_hi=1 - me.x_hi),
    ]


def spread_devices(me):
    return [me.at(x_lo=1 - me.x_lo), me.at(y=(me.y + 1) % 4), me.at(y=(me.y + 3) % 4)]


def run_stages(stages, lags, chunks):
    for tick in range(max(lags) + chunks):
        for stage, lag in zip(stages, lags):
            if 0 <= tick - lag < chunks:
                stage(tick - lag)


def each_tile(q, chunks, body):
    size = 8 // chunks

    def step(i, carry):
        body(q * size + i)
        return carry

    lax.fori_loop(0, size, step, 0)


def span(q, chunks):
    return pl.ds(q * (8 // chunks), 8 // chunks)


def wide(x):
    return x.astype(jnp.float32)


def sum_stages(me, part, bufs, sems, finish):
    given, running, arrived, kept, across, crossed = bufs
    pair_send, pair_recv, ring_send, ring_recv, far_send, far_recv = sems
    chunks = SUM_CHUNK

    def pair_copy(q):
        return pltpu.make_async_remote_copy(
            part.at[:, :, 1 - me.core, span(q, chunks)], given.at[:, :, span(q, chunks)],
            pair_send.at[q], pair_recv.at[q],
            device_id=me.at(core=1 - me.core), device_id_type=MESH,
        )

    def ring_copy(half, step, q):
        up = (half == 0) == (step < 2)
        return pltpu.make_async_remote_copy(
            running.at[half, step, span(q, chunks)], arrived.at[half, step, span(q, chunks)],
            ring_send.at[half, step, q], ring_recv.at[half, step, q],
            device_id=me.at(z=(me.z + (1 if up else 3)) % 4), device_id_type=MESH,
        )

    def far_copy(q):
        return pltpu.make_async_remote_copy(
            across.at[span(q, chunks)], crossed.at[span(q, chunks)], far_send.at[q], far_recv.at[q],
            device_id=me.at(x_hi=1 - me.x_hi), device_id_type=MESH,
        )

    def begin():
        for q in range(chunks):
            pair_copy(q).start()

    def local_sum(half, offset, k):
        x_hi = me.x_hi if half == 0 else 1 - me.x_hi
        z = (me.z + (offset if half == 0 else 4 - offset)) % 4
        return part[x_hi, z, me.core, k] + given[x_hi, z, k]

    def first(q):
        pair_copy(q).wait_recv()
        for step, offset in ((0, 2), (2, 3)):
            for half in (1, 0):
                def body(k, half=half, step=step, offset=offset):
                    running[half, step, k] = local_sum(half, offset, k).astype(jnp.bfloat16)

                each_tile(q, chunks, body)
                ring_copy(half, step, q).start()

    def middle(q):
        for half in (1, 0):
            ring_copy(half, 0, q).wait_recv()

            def body(k, half=half):
                running[half, 1, k] = (local_sum(half, 1, k) + wide(arrived[half, 0, k])).astype(jnp.bfloat16)

            each_tile(q, chunks, body)
            ring_copy(half, 1, q).start()

    def last(q):
        for half in (1, 0):
            ring_copy(half, 2, q).wait_recv()
            ring_copy(half, 1, q).wait_recv()

            def body(k, half=half):
                total = local_sum(half, 0, k) + (wide(arrived[half, 1, k]) + wide(arrived[half, 2, k]))
                if half == 1:
                    across[k] = total.astype(jnp.bfloat16)
                else:
                    kept[k] = total

            each_tile(q, chunks, body)
            if half == 1:
                far_copy(q).start()

    def done(q):
        far_copy(q).wait_recv()
        each_tile(q, chunks, lambda k: finish(k, kept[k] + wide(crossed[k])))

    def drain():
        for q in range(chunks):
            pair_copy(q).wait_send()
            far_copy(q).wait_send()
            for half in (0, 1):
                for step in range(3):
                    ring_copy(half, step, q).wait_send()

    return begin, [first, middle, last, done], drain


def sum_scratch():
    block = lambda *lead, dtype=jnp.bfloat16: pltpu.VMEM((*lead, 8, TILE, TILE), dtype)
    dma = pltpu.SemaphoreType.DMA
    bufs = [block(2, 4, dtype=jnp.float32), block(2, 3), block(2, 3), block(dtype=jnp.float32), block(), block()]
    sems = [dma((SUM_CHUNK,))] * 2 + [dma((2, 3, SUM_CHUNK))] * 2 + [dma((SUM_CHUNK,))] * 2
    return bufs + sems


N_SUM = 12


def spread_stages(me, gathered, sems, chunks):
    side_send, side_recv, near_send, near_recv, relay_send, relay_recv, pass_send, pass_recv = sems

    def copy(block, send, recv, device):
        return pltpu.make_async_remote_copy(block, block, send, recv, device_id=device, device_id_type=MESH)

    def block(y, x_lo, q):
        return gathered.at[me.core, (me.y + y) % 4, me.x_lo if x_lo == 0 else 1 - me.x_lo, span(q, chunks)]

    def side_copy(q):
        return copy(block(0, 0, q), side_send.at[q], side_recv.at[q], me.at(x_lo=1 - me.x_lo))

    def near_copy(kind, way, q):
        device = me.at(y=(me.y + (1 if way == 0 else 3)) % 4)
        return copy(block(0, kind, q), near_send.at[kind, way, q], near_recv.at[kind, way, q], device)

    def relay_copy(way, q):
        device = me.at(y=(me.y + (1 if way == 0 else 3)) % 4)
        return copy(block(3 if way == 0 else 1, way, q), relay_send.at[way, q], relay_recv.at[way, q], device)

    def pass_copy(y, x_lo, q):
        return copy(block(y, x_lo, q), pass_send.at[y, x_lo, q], pass_recv.at[y, x_lo, q], me.at(core=1 - me.core))

    def own(q):
        side_copy(q).start()
        near_copy(0, 0, q).start()
        near_copy(0, 1, q).start()
        pass_copy(0, 0, q).start()

    def beside(q):
        side_copy(q).wait_recv()
        near_copy(1, 0, q).start()
        near_copy(1, 1, q).start()
        pass_copy(0, 1, q).start()

    def relay_own(q):
        near_copy(0, 0, q).wait_recv()
        relay_copy(0, q).start()
        pass_copy(3, 0, q).start()

    def relay_beside(q):
        near_copy(1, 1, q).wait_recv()
        relay_copy(1, q).start()
        pass_copy(1, 1, q).start()

    def opposite(q):
        near_copy(0, 1, q).wait_recv()
        pass_copy(1, 0, q).start()
        near_copy(1, 0, q).wait_recv()
        pass_copy(3, 1, q).start()
        for way in (0, 1):
            relay_copy(way, q).wait_recv()
            pass_copy(2, way, q).start()

    def drain():
        for q in range(chunks):
            for y in range(4):
                for x_lo in range(2):
                    pass_copy(y, x_lo, q).wait_recv()
        for q in range(chunks):
            side_copy(q).wait_send()
            for way in (0, 1):
                near_copy(0, way, q).wait_send()
                near_copy(1, way, q).wait_send()
                relay_copy(way, q).wait_send()
            for y in range(4):
                for x_lo in range(2):
                    pass_copy(y, x_lo, q).wait_send()

    return [own, beside, relay_own, relay_beside, opposite], drain


def spread_scratch(chunks):
    dma = pltpu.SemaphoreType.DMA
    return [dma((chunks,))] * 2 + [dma((2, 2, chunks))] * 2 + [dma((2, chunks))] * 2 + [dma((4, 2, chunks))] * 2


def hot(ids, cell):
    return jnp.where(jnp.broadcast_to(ids, (TILE, TILE)) == cell, jnp.bfloat16(1), jnp.bfloat16(0))


def narrow(x):
    return x.astype(jnp.float32).astype(jnp.bfloat16)


def start_kernel(
    count_ref, features_hbm, rows_hbm, cols_hbm, edges_ref, tiles_hbm, metas_ref, root_ref, gathered_ref,
    tiles_ref, features_ref, meta, lists, raw, slot_degree, degree, shares, roots,
    tile_sem, load_sem, list_sem, list_send, list_recv, meta_send, meta_recv, share_send, share_recv, root_send, root_recv, *sems,
):
    me = Place()
    peers = [lax.rem(me.col + i, 16) for i in range(1, 16)]
    across = me.col + 1 - 2 * me.core
    friends = [(lax.rem(me.row + i % 8, 8), me.col if i < 8 else across) for i in range(1, 16)]
    loads = [
        pltpu.make_async_copy(rows_hbm, meta.at[pl.ds(0, 8)], load_sem.at[0]),
        pltpu.make_async_copy(cols_hbm, meta.at[pl.ds(8, 8)], load_sem.at[1]),
        pltpu.make_async_copy(features_hbm, features_ref, load_sem.at[2]),
    ]
    own_lists = pltpu.make_async_copy(edges_ref.at[:, :, me.core], lists.at[me.core], list_sem)
    for load in loads:
        load.start()
    own_lists.start()
    meta[16:24, :] = jnp.full((8, TILE), count_ref[0, 0], jnp.int32)
    greet([(me.row, peer) for peer in peers] + [friend for i, friend in enumerate(friends) if i != 7])
    partner = me.at(core=1 - me.core)

    give_lists = pltpu.make_async_remote_copy(
        edges_ref.at[:, :, 1 - me.core], lists.at[me.core], list_send, list_recv, device_id=partner, device_id_type=MESH
    )
    give_meta = pltpu.make_async_remote_copy(
        meta, metas_ref.at[me.core], meta_send, meta_recv, device_id=partner, device_id_type=MESH
    )

    def tile_copy(bank):
        return pltpu.make_async_copy(tiles_ref.at[bank], tiles_hbm.at[bank], tile_sem.at[bank])

    def share_copy(i):
        return pltpu.make_async_remote_copy(
            degree.at[peers[i]], shares.at[i], share_send.at[i], share_recv.at[i],
            device_id=(me.row, peers[i]), device_id_type=MESH,
        )

    def root_copy(i):
        block = roots.at[me.core, me.y, me.x_lo]
        return pltpu.make_async_remote_copy(
            block, block, root_send.at[i], root_recv.at[i], device_id=friends[i], device_id_type=MESH
        )

    give_lists.start()
    for load in loads:
        load.wait()
    give_meta.start()
    metas_ref[me.core] = meta[...]

    def turn(k, carry):
        raw[me.core, me.y, me.x_lo, k] = wide(features_ref[k]).T.astype(jnp.bfloat16)
        return carry

    lax.fori_loop(0, 8, turn, 0)
    slot_degree[...] = jnp.zeros_like(slot_degree)
    stages, drain = spread_stages(me, raw, sems, RAW_CHUNK)
    groups = 2 * lists.shape[2] * 8 // GROUP
    blocks = GROUP // 8
    own_lists.wait()

    def build(group, carry):
        for when, moves in RAW_MOVES:
            @pl.when(group == when)
            def _(moves=moves):
                for stage, q in moves:
                    stages[stage](q)

        @pl.when(group == groups // 2)
        def _():
            give_lists.wait_recv()
            give_meta.wait_recv()

        half = group // (groups // 2)
        place = group % (groups // 2)
        owner = me.core + half * (1 - 2 * me.core)
        bank = owner * (groups // 2) + place
        base = place * blocks

        shape = (blocks, 8, TILE)
        slot = (lax.broadcasted_iota(jnp.int32, shape, 0) + base) * 16 + 8 * me.core + lax.broadcasted_iota(jnp.int32, shape, 1)
        live = slot < jnp.broadcast_to(metas_ref[owner, 16:17, :].reshape(1, 1, TILE), shape)
        dst = jnp.where(live, lists[owner, 0, pl.ds(base, blocks)], -1).reshape(GROUP, TILE)
        src = lists[owner, 1, pl.ds(base, blocks)].reshape(GROUP, TILE)
        dst, src = narrow(dst), narrow(src)
        cell = narrow(lax.broadcasted_iota(jnp.int32, (TILE, TILE), 0))
        for block in range(blocks):
            totals = []
            for i in range(8 * block, 8 * block + 8):
                counts = lax.dot_general(
                    hot(src[i : i + 1, :], cell), hot(dst[i : i + 1, :], cell).astype(jnp.float8_e4m3fn), (((1,), (1,)), ((), ())),
                    preferred_element_type=jnp.float32,
                )
                tiles_ref[bank, i] = counts.astype(jnp.bfloat16)
                totals.append(jnp.sum(counts, axis=0, keepdims=True))
            slot_degree[owner, (base + block) * 2 + me.core] = jnp.concatenate(totals, axis=0)
        tile_copy(bank).start()
        return carry

    lax.fori_loop(0, groups, build, 0)

    cell = lax.broadcasted_iota(jnp.int32, (TILE, TILE), 0)
    counted = jnp.zeros((TILE, TILE), jnp.float32)
    for owner in range(2):
        for j in range(8):
            row_hot = (jnp.broadcast_to(metas_ref[owner, j : j + 1, :], (TILE, TILE)) == cell).astype(jnp.float32)
            slots = slot_degree[owner, 16 * j : 16 * j + 16].reshape(TILE, TILE)
            counted += jnp.dot(
                row_hot.astype(jnp.bfloat16), slots.astype(jnp.bfloat16), preferred_element_type=jnp.float32
            )
    degree[...] = counted.reshape(16, 8, TILE)
    for i in range(15):
        share_copy(i).start()
    for stage, q in RAW_LATE:
        stages[stage](q)
    total = degree[me.col]
    for i in range(15):
        share_copy(i).wait_recv()
        total = total + shares[i]
    root = lax.rsqrt(1.0 + total)
    root_ref[...] = root
    roots[me.core, me.y, me.x_lo] = root
    for i in range(15):
        root_copy(i).start()
    for q in range(RAW_CHUNK):
        stages[4](q)
    drain()
    for i in range(15):
        root_copy(i).wait_recv()

    def scale(i, carry):
        c, y, x, k = i // 64, (i // 16) % 4, (i // 8) % 2, i % 8
        gathered_ref[c, y, x, k] = (wide(raw[c, y, x, k]) * roots[c, y, x, pl.ds(k, 1), :]).astype(jnp.bfloat16)
        return carry

    lax.fori_loop(0, 128, scale, 0, unroll=4)
    for i in range(15):
        share_copy(i).wait_send()
        root_copy(i).wait_send()
    give_lists.wait_send()
    give_meta.wait_send()
    for bank in range(groups):
        tile_copy(bank).wait()


RAW_MOVES = (
    (0, ((0, 0), (0, 1))),
    (6, ((1, 0), (2, 0))),
    (10, ((1, 1), (2, 1))),
    (14, ((3, 0),)),
)
RAW_LATE = ((3, 1),)


def sum_kernel(spreads, part_ref, root_ref, hop_ref, *refs):
    me = Place()
    gathered_ref = refs[0] if spreads else None
    scratch = refs[1:] if spreads else refs
    greet(sum_devices(me) + (spread_devices(me) if spreads else []))

    def finish(k, total):
        root = root_ref[pl.ds(k, 1), :]
        hop_ref[k] = (total * root).T.astype(jnp.bfloat16)
        if spreads:
            gathered_ref[me.core, me.y, me.x_lo, k] = (total * (root * root)).astype(jnp.bfloat16)

    begin, stages, drain = sum_stages(me, part_ref, scratch[:6], scratch[6:N_SUM], finish)
    begin()
    if spreads:
        more, drain_spread = spread_stages(me, gathered_ref, scratch[N_SUM:], SUM_CHUNK)
        run_stages(stages + more, SUM_LAGS, SUM_CHUNK)
        drain_spread()
    else:
        run_stages(stages, SUM_LAGS[:4], SUM_CHUNK)
    drain()


VMEM = pl.BlockSpec(memory_space=pltpu.VMEM)
SMEM = pl.BlockSpec(memory_space=pltpu.SMEM)
HBM = pl.BlockSpec(memory_space=pltpu.HBM)
GATHERED = (2, 4, 2, 8, TILE, TILE)


def comm_params(number, limit):
    return pltpu.CompilerParams(collective_id=number, has_side_effects=True, vmem_limit_bytes=limit)


def start(counts, features, rows, cols, edges):
    dma = pltpu.SemaphoreType.DMA
    slots = edges.shape[1]
    shape = jax.ShapeDtypeStruct
    f32, bf16, i32 = jnp.float32, jnp.bfloat16, jnp.int32
    return pl.pallas_call(
        start_kernel,
        out_shape=[
            shape((slots // GROUP, GROUP, TILE, TILE), bf16), shape((2, 24, TILE), i32), shape((8, TILE), f32), shape(GATHERED, bf16)
        ],
        in_specs=[SMEM, HBM, HBM, HBM, HBM],
        out_specs=[HBM, VMEM, VMEM, VMEM],
        scratch_shapes=[
            pltpu.VMEM((slots // GROUP, GROUP, TILE, TILE), bf16),
            pltpu.VMEM((8, TILE, TILE), bf16),
            pltpu.VMEM((24, TILE), i32),
            pltpu.VMEM((2, 2, slots // 16, 8, TILE), i32),
            pltpu.VMEM(GATHERED, bf16),
            pltpu.VMEM((2, slots // 8, 8, TILE), f32),
            pltpu.VMEM((16, 8, TILE), f32),
            pltpu.VMEM((15, 8, TILE), f32),
            pltpu.VMEM((2, 4, 2, 8, TILE), f32),
            dma((slots // GROUP,)), dma((3,)), *[dma] * 5, *[dma((15,))] * 4,
            *spread_scratch(RAW_CHUNK),
        ],
        compiler_params=comm_params(0, START_LIMIT),
        name="start_build",
    )(
        counts, features.reshape(8, TILE, TILE), rows.reshape(8, TILE), cols.reshape(8, TILE),
        edges.reshape(2, slots // 16, 2, 8, TILE),
    )


def live_count(metas_ref, core, owner):
    count = metas_ref[owner, 16, 0]
    return count // 16 * 8 + jnp.clip(count % 16 - 8 * core, 0, 8)


def apply_kernel(metas_ref, tiles_hbm, x_ref, total, tiles_ref, tile_sem):
    core = lax.axis_index("col") % 2
    half_groups = tiles_ref.shape[0] // 2
    live = [(live_count(metas_ref, core, owner) + GROUP - 1) // GROUP for owner in range(2)]

    def tile_copy(bank):
        return pltpu.make_async_copy(tiles_hbm.at[bank], tiles_ref.at[bank], tile_sem.at[bank])

    for owner in range(2):
        def fetch(place, carry, owner=owner):
            tile_copy(owner * half_groups + place).start()
            return carry

        lax.fori_loop(0, live[owner], fetch, 0)
    total[...] = jnp.zeros_like(total)
    for owner in range(2):
        def apply_group(place, carry, owner=owner):
            base = place * GROUP * 2 + 8 * core
            tile_copy(owner * half_groups + place).wait()
            for start in range(0, GROUP, BATCH):
                slots = [base + i // 8 * 16 + i % 8 for i in range(start, start + BATCH)]
                products = [
                    jnp.dot(
                        x_ref[owner * 64 + metas_ref[owner, 8 + slot // 128, slot % 128]],
                        tiles_ref[owner * half_groups + place, start + j],
                        preferred_element_type=jnp.float32,
                    )
                    for j, slot in enumerate(slots)
                ]
                for slot, product in zip(slots, products):
                    total[metas_ref[owner, slot // 128, slot % 128]] += product
            return carry

        lax.fori_loop(0, live[owner], apply_group, 0)


def apply_tiles(metas, tiles, x):
    return pl.pallas_call(
        apply_kernel,
        in_specs=[SMEM, HBM, VMEM],
        out_specs=VMEM,
        scratch_shapes=[pltpu.VMEM(tiles.shape, tiles.dtype), pltpu.SemaphoreType.DMA((tiles.shape[0],))],
        out_shape=jax.ShapeDtypeStruct((TILE, TILE, TILE), jnp.float32),
        compiler_params=pltpu.CompilerParams(vmem_limit_bytes=APPLY_LIMIT),
        name="apply_tiles",
    )(metas, tiles, x)


def sum_parts(part, root, spreads):
    hop = jax.ShapeDtypeStruct((8, TILE, TILE), jnp.bfloat16)
    gathered = jax.ShapeDtypeStruct(GATHERED, jnp.bfloat16)
    return pl.pallas_call(
        functools.partial(sum_kernel, spreads),
        out_shape=[hop, gathered] if spreads else [hop],
        in_specs=[VMEM, VMEM],
        out_specs=[VMEM, VMEM] if spreads else [VMEM],
        scratch_shapes=sum_scratch() + (spread_scratch(SUM_CHUNK) if spreads else []),
        compiler_params=comm_params(1 if spreads else 2, SUM_LIMIT),
        name="sum_spread" if spreads else "sum_last",
    )(part.reshape(2, 4, 2, 8, TILE, TILE), root)


def local(features, tile_rows, tile_cols, edge_lists, tile_counts):
    edges = edge_lists.reshape(2, *edge_lists.shape[3:])
    tiles, metas, root, gathered = start(tile_counts, features, tile_rows, tile_cols, edges)
    part = apply_tiles(metas, tiles, gathered.reshape(128, TILE, TILE))
    hop_one, gathered = sum_parts(part, root, True)
    part = apply_tiles(metas, tiles, gathered.reshape(128, TILE, TILE))
    (hop_two,) = sum_parts(part, root, False)
    return (hop_one.reshape(features.shape), hop_two.reshape(features.shape))


def solution(mesh):
    placed = (
        P(("row", "col"), None),
        P("row", "col", None),
        P("row", "col", None),
        P(None, "row", "col", None, None),
        P("row", "col"),
    )
    return jax.shard_map(
        local,
        mesh=mesh,
        in_specs=placed,
        out_specs=(P(("row", "col"), None), P(("row", "col"), None)),
        check_vma=False,
    )
```

```python
import functools

import jax
import jax.numpy as jnp
from jax import lax
from jax.experimental import pallas as pl
from jax.experimental.pallas import tpu as pltpu
from jax.sharding import PartitionSpec as P

TILE = 128
GROUP = 64
BATCH = 8
SUM_CHUNK = 8
RAW_CHUNK = 2
START_LIMIT = 42 * 2**20
APPLY_LIMIT = 34 * 2**20
SUM_LIMIT = 12 * 2**20
SUM_LAGS = (0, 2, 4, 6, 6, 8, 10, 10, 12)


MESH = pl.DeviceIdType.MESH


class Place:
    def __init__(self):
        self.row, self.col = lax.axis_index("row"), lax.axis_index("col")
        self.y, self.x_lo = self.row // 2, self.row % 2
        self.x_hi, self.z, self.core = self.col // 8, (self.col // 2) % 4, self.col % 2

    def at(self, y=None, x_lo=None, x_hi=None, z=None, core=None):
        pick = lambda new, old: old if new is None else new
        row = pick(y, self.y) * 2 + pick(x_lo, self.x_lo)
        col = (pick(x_hi, self.x_hi) * 4 + pick(z, self.z)) * 2 + pick(core, self.core)
        return (row, col)


def greet(devices):
    barrier = pltpu.get_barrier_semaphore()
    for device in devices:
        pl.semaphore_signal(barrier, inc=1, device_id=device, device_id_type=MESH)
    pl.semaphore_wait(barrier, len(devices))


def sum_devices(me):
    return [
        me.at(core=1 - me.core),
        me.at(z=(me.z + 1) % 4),
        me.at(z=(me.z + 3) % 4),
        me.at(x_hi=1 - me.x_hi),
    ]


def spread_devices(me):
    return [me.at(x_lo=1 - me.x_lo), me.at(y=(me.y + 1) % 4), me.at(y=(me.y + 3) % 4)]


def run_stages(stages, lags, chunks):
    for tick in range(max(lags) + chunks):
        for stage, lag in zip(stages, lags):
            if 0 <= tick - lag < chunks:
                stage(tick - lag)


def each_tile(q, chunks, body):
    size = 8 // chunks

    def step(i, carry):
        body(q * size + i)
        return carry

    lax.fori_loop(0, size, step, 0)


def span(q, chunks):
    return pl.ds(q * (8 // chunks), 8 // chunks)


def wide(x):
    return x.astype(jnp.float32)


def sum_stages(me, part, bufs, sems, finish):
    given, running, arrived, kept, across, crossed = bufs
    pair_send, pair_recv, ring_send, ring_recv, far_send, far_recv = sems
    chunks = SUM_CHUNK

    def pair_copy(q):
        return pltpu.make_async_remote_copy(
            part.at[:, :, 1 - me.core, span(q, chunks)], given.at[:, :, span(q, chunks)],
            pair_send.at[q], pair_recv.at[q],
            device_id=me.at(core=1 - me.core), device_id_type=MESH,
        )

    def ring_copy(half, step, q):
        up = (half == 0) == (step < 2)
        return pltpu.make_async_remote_copy(
            running.at[half, step, span(q, chunks)], arrived.at[half, step, span(q, chunks)],
            ring_send.at[half, step, q], ring_recv.at[half, step, q],
            device_id=me.at(z=(me.z + (1 if up else 3)) % 4), device_id_type=MESH,
        )

    def far_copy(q):
        return pltpu.make_async_remote_copy(
            across.at[span(q, chunks)], crossed.at[span(q, chunks)], far_send.at[q], far_recv.at[q],
            device_id=me.at(x_hi=1 - me.x_hi), device_id_type=MESH,
        )

    def begin():
        for q in range(chunks):
            pair_copy(q).start()

    def local_sum(half, offset, k):
        x_hi = me.x_hi if half == 0 else 1 - me.x_hi
        z = (me.z + (offset if half == 0 else 4 - offset)) % 4
        return part[x_hi, z, me.core, k] + given[x_hi, z, k]

    def first(q):
        pair_copy(q).wait_recv()
        for step, offset in ((0, 2), (2, 3)):
            for half in (1, 0):
                def body(k, half=half, step=step, offset=offset):
                    running[half, step, k] = local_sum(half, offset, k).astype(jnp.bfloat16)

                each_tile(q, chunks, body)
                ring_copy(half, step, q).start()

    def middle(q):
        for half in (1, 0):
            ring_copy(half, 0, q).wait_recv()

            def body(k, half=half):
                running[half, 1, k] = (local_sum(half, 1, k) + wide(arrived[half, 0, k])).astype(jnp.bfloat16)

            each_tile(q, chunks, body)
            ring_copy(half, 1, q).start()

    def last(q):
        for half in (1, 0):
            ring_copy(half, 2, q).wait_recv()
            ring_copy(half, 1, q).wait_recv()

            def body(k, half=half):
                total = local_sum(half, 0, k) + (wide(arrived[half, 1, k]) + wide(arrived[half, 2, k]))
                if half == 1:
                    across[k] = total.astype(jnp.bfloat16)
                else:
                    kept[k] = total

            each_tile(q, chunks, body)
            if half == 1:
                far_copy(q).start()

    def done(q):
        far_copy(q).wait_recv()
        each_tile(q, chunks, lambda k: finish(k, kept[k] + wide(crossed[k])))

    def drain():
        for q in range(chunks):
            pair_copy(q).wait_send()
            far_copy(q).wait_send()
            for half in (0, 1):
                for step in range(3):
                    ring_copy(half, step, q).wait_send()

    return begin, [first, middle, last, done], drain


def sum_scratch():
    block = lambda *lead, dtype=jnp.bfloat16: pltpu.VMEM((*lead, 8, TILE, TILE), dtype)
    dma = pltpu.SemaphoreType.DMA
    bufs = [block(2, 4, dtype=jnp.float32), block(2, 3), block(2, 3), block(dtype=jnp.float32), block(), block()]
    sems = [dma((SUM_CHUNK,))] * 2 + [dma((2, 3, SUM_CHUNK))] * 2 + [dma((SUM_CHUNK,))] * 2
    return bufs + sems


N_SUM = 12


def spread_stages(me, gathered, sems, chunks):
    side_send, side_recv, near_send, near_recv, relay_send, relay_recv, pass_send, pass_recv = sems

    def copy(block, send, recv, device):
        return pltpu.make_async_remote_copy(block, block, send, recv, device_id=device, device_id_type=MESH)

    def block(y, x_lo, q):
        return gathered.at[me.core, (me.y + y) % 4, me.x_lo if x_lo == 0 else 1 - me.x_lo, span(q, chunks)]

    def side_copy(q):
        return copy(block(0, 0, q), side_send.at[q], side_recv.at[q], me.at(x_lo=1 - me.x_lo))

    def near_copy(kind, way, q):
        device = me.at(y=(me.y + (1 if way == 0 else 3)) % 4)
        return copy(block(0, kind, q), near_send.at[kind, way, q], near_recv.at[kind, way, q], device)

    def relay_copy(way, q):
        device = me.at(y=(me.y + (1 if way == 0 else 3)) % 4)
        return copy(block(3 if way == 0 else 1, way, q), relay_send.at[way, q], relay_recv.at[way, q], device)

    def pass_copy(y, x_lo, q):
        return copy(block(y, x_lo, q), pass_send.at[y, x_lo, q], pass_recv.at[y, x_lo, q], me.at(core=1 - me.core))

    def own(q):
        side_copy(q).start()
        near_copy(0, 0, q).start()
        near_copy(0, 1, q).start()
        pass_copy(0, 0, q).start()

    def beside(q):
        side_copy(q).wait_recv()
        near_copy(1, 0, q).start()
        near_copy(1, 1, q).start()
        pass_copy(0, 1, q).start()

    def relay_own(q):
        near_copy(0, 0, q).wait_recv()
        relay_copy(0, q).start()
        pass_copy(3, 0, q).start()

    def relay_beside(q):
        near_copy(1, 1, q).wait_recv()
        relay_copy(1, q).start()
        pass_copy(1, 1, q).start()

    def opposite(q):
        near_copy(0, 1, q).wait_recv()
        pass_copy(1, 0, q).start()
        near_copy(1, 0, q).wait_recv()
        pass_copy(3, 1, q).start()
        for way in (0, 1):
            relay_copy(way, q).wait_recv()
            pass_copy(2, way, q).start()

    def drain():
        for q in range(chunks):
            for y in range(4):
                for x_lo in range(2):
                    pass_copy(y, x_lo, q).wait_recv()
        for q in range(chunks):
            side_copy(q).wait_send()
            for way in (0, 1):
                near_copy(0, way, q).wait_send()
                near_copy(1, way, q).wait_send()
                relay_copy(way, q).wait_send()
            for y in range(4):
                for x_lo in range(2):
                    pass_copy(y, x_lo, q).wait_send()

    return [own, beside, relay_own, relay_beside, opposite], drain


def spread_scratch(chunks):
    dma = pltpu.SemaphoreType.DMA
    return [dma((chunks,))] * 2 + [dma((2, 2, chunks))] * 2 + [dma((2, chunks))] * 2 + [dma((4, 2, chunks))] * 2


def hot(ids, cell):
    return jnp.where(jnp.broadcast_to(ids, (TILE, TILE)) == cell, jnp.bfloat16(1), jnp.bfloat16(0))


def narrow(x):
    return x.astype(jnp.float32).astype(jnp.bfloat16)


def start_kernel(
    count_ref, features_hbm, rows_hbm, cols_hbm, edges_ref, tiles_hbm, metas_ref, root_ref, gathered_ref,
    tiles_ref, features_ref, meta, lists, raw, slot_degree, degree, shares, roots,
    tile_sem, load_sem, list_sem, list_send, list_recv, meta_send, meta_recv, share_send, share_recv, root_send, root_recv, *sems,
):
    me = Place()
    peers = [lax.rem(me.col + i, 16) for i in range(1, 16)]
    across = me.col + 1 - 2 * me.core
    friends = [(lax.rem(me.row + i % 8, 8), me.col if i < 8 else across) for i in range(1, 16)]
    loads = [
        pltpu.make_async_copy(rows_hbm, meta.at[pl.ds(0, 8)], load_sem.at[0]),
        pltpu.make_async_copy(cols_hbm, meta.at[pl.ds(8, 8)], load_sem.at[1]),
        pltpu.make_async_copy(features_hbm, features_ref, load_sem.at[2]),
    ]
    own_lists = pltpu.make_async_copy(edges_ref.at[:, :, me.core], lists.at[me.core], list_sem)
    for load in loads:
        load.start()
    own_lists.start()
    meta[16:24, :] = jnp.full((8, TILE), count_ref[0, 0], jnp.int32)
    greet([(me.row, peer) for peer in peers] + [friend for i, friend in enumerate(friends) if i != 7])
    partner = me.at(core=1 - me.core)

    give_lists = pltpu.make_async_remote_copy(
        edges_ref.at[:, :, 1 - me.core], lists.at[me.core], list_send, list_recv, device_id=partner, device_id_type=MESH
    )
    give_meta = pltpu.make_async_remote_copy(
        meta, metas_ref.at[me.core], meta_send, meta_recv, device_id=partner, device_id_type=MESH
    )

    def tile_copy(bank):
        return pltpu.make_async_copy(tiles_ref.at[bank], tiles_hbm.at[bank], tile_sem.at[bank])

    def share_copy(i):
        return pltpu.make_async_remote_copy(
            degree.at[peers[i]], shares.at[i], share_send.at[i], share_recv.at[i],
            device_id=(me.row, peers[i]), device_id_type=MESH,
        )

    def root_copy(i):
        block = roots.at[me.core, me.y, me.x_lo]
        return pltpu.make_async_remote_copy(
            block, block, root_send.at[i], root_recv.at[i], device_id=friends[i], device_id_type=MESH
        )

    give_lists.start()
    for load in loads:
        load.wait()
    give_meta.start()
    metas_ref[me.core] = meta[...]

    def turn(k, carry):
        raw[me.core, me.y, me.x_lo, k] = wide(features_ref[k]).T.astype(jnp.bfloat16)
        return carry

    lax.fori_loop(0, 8, turn, 0)
    slot_degree[...] = jnp.zeros_like(slot_degree)
    stages, drain = spread_stages(me, raw, sems, RAW_CHUNK)
    groups = 2 * lists.shape[2] * 8 // GROUP
    blocks = GROUP // 8
    own_lists.wait()

    def build(group, carry):
        for when, moves in RAW_MOVES:
            @pl.when(group == when)
            def _(moves=moves):
                for stage, q in moves:
                    stages[stage](q)

        @pl.when(group == groups // 2)
        def _():
            give_lists.wait_recv()
            give_meta.wait_recv()

        half = group // (groups // 2)
        place = group % (groups // 2)
        owner = me.core + half * (1 - 2 * me.core)
        bank = owner * (groups // 2) + place
        base = place * blocks

        shape = (blocks, 8, TILE)
        slot = (lax.broadcasted_iota(jnp.int32, shape, 0) + base) * 16 + 8 * me.core + lax.broadcasted_iota(jnp.int32, shape, 1)
        live = slot < jnp.broadcast_to(metas_ref[owner, 16:17, :].reshape(1, 1, TILE), shape)
        dst = jnp.where(live, lists[owner, 0, pl.ds(base, blocks)], -1).reshape(GROUP, TILE)
        src = lists[owner, 1, pl.ds(base, blocks)].reshape(GROUP, TILE)
        dst, src = narrow(dst), narrow(src)
        cell = narrow(lax.broadcasted_iota(jnp.int32, (TILE, TILE), 0))
        for block in range(blocks):
            totals = []
            for i in range(8 * block, 8 * block + 8):
                counts = lax.dot_general(
                    hot(src[i : i + 1, :], cell), hot(dst[i : i + 1, :], cell).astype(jnp.float8_e4m3fn), (((1,), (1,)), ((), ())),
                    preferred_element_type=jnp.float32,
                )
                tiles_ref[bank, i] = counts.astype(jnp.bfloat16)
                totals.append(jnp.sum(counts, axis=0, keepdims=True))
            slot_degree[owner, (base + block) * 2 + me.core] = jnp.concatenate(totals, axis=0)
        tile_copy(bank).start()
        return carry

    lax.fori_loop(0, groups, build, 0)

    cell = lax.broadcasted_iota(jnp.int32, (TILE, TILE), 0)
    counted = jnp.zeros((TILE, TILE), jnp.float32)
    for owner in range(2):
        for j in range(8):
            row_hot = (jnp.broadcast_to(metas_ref[owner, j : j + 1, :], (TILE, TILE)) == cell).astype(jnp.float32)
            slots = slot_degree[owner, 16 * j : 16 * j + 16].reshape(TILE, TILE)
            counted += jnp.dot(
                row_hot.astype(jnp.bfloat16), slots.astype(jnp.bfloat16), preferred_element_type=jnp.float32
            )
    degree[...] = counted.reshape(16, 8, TILE)
    for i in range(15):
        share_copy(i).start()
    for stage, q in RAW_LATE:
        stages[stage](q)
    total = degree[me.col]
    for i in range(15):
        share_copy(i).wait_recv()
        total = total + shares[i]
    root = lax.rsqrt(1.0 + total)
    root_ref[...] = root
    roots[me.core, me.y, me.x_lo] = root
    for i in range(15):
        root_copy(i).start()
    for q in range(RAW_CHUNK):
        stages[4](q)
    drain()

    def scale_block(c, row):
        y, x = row // 2, row % 2

        def scale(k, carry):
            gathered_ref[c, y, x, k] = (wide(raw[c, y, x, k]) * roots[c, y, x, pl.ds(k, 1), :]).astype(jnp.bfloat16)
            return carry

        lax.fori_loop(0, 8, scale, 0, unroll=4)

    scale_block(me.core, me.row)
    for i in (8, 2, 6, 10, 14, 1, 7, 9, 15, 3, 5, 11, 13, 4, 12):
        root_copy(i - 1).wait_recv()
        scale_block(me.core if i < 8 else 1 - me.core, lax.rem(me.row + 8 - i % 8, 8))
    for i in range(15):
        share_copy(i).wait_send()
        root_copy(i).wait_send()
    give_lists.wait_send()
    give_meta.wait_send()
    for bank in range(groups):
        tile_copy(bank).wait()


RAW_MOVES = (
    (0, ((0, 0), (0, 1))),
    (6, ((1, 0), (2, 0))),
    (10, ((1, 1), (2, 1))),
    (14, ((3, 0),)),
)
RAW_LATE = ((3, 1),)


def sum_kernel(spreads, part_ref, root_ref, hop_ref, *refs):
    me = Place()
    gathered_ref = refs[0] if spreads else None
    scratch = refs[1:] if spreads else refs
    greet(sum_devices(me) + (spread_devices(me) if spreads else []))

    def finish(k, total):
        root = root_ref[pl.ds(k, 1), :]
        hop_ref[k] = (total * root).T.astype(jnp.bfloat16)
        if spreads:
            gathered_ref[me.core, me.y, me.x_lo, k] = (total * (root * root)).astype(jnp.bfloat16)

    begin, stages, drain = sum_stages(me, part_ref, scratch[:6], scratch[6:N_SUM], finish)
    begin()
    if spreads:
        more, drain_spread = spread_stages(me, gathered_ref, scratch[N_SUM:], SUM_CHUNK)
        run_stages(stages + more, SUM_LAGS, SUM_CHUNK)
        drain_spread()
    else:
        run_stages(stages, SUM_LAGS[:4], SUM_CHUNK)
    drain()


VMEM = pl.BlockSpec(memory_space=pltpu.VMEM)
SMEM = pl.BlockSpec(memory_space=pltpu.SMEM)
HBM = pl.BlockSpec(memory_space=pltpu.HBM)
GATHERED = (2, 4, 2, 8, TILE, TILE)


def comm_params(number, limit):
    return pltpu.CompilerParams(collective_id=number, has_side_effects=True, vmem_limit_bytes=limit)


def start(counts, features, rows, cols, edges):
    dma = pltpu.SemaphoreType.DMA
    slots = edges.shape[1]
    shape = jax.ShapeDtypeStruct
    f32, bf16, i32 = jnp.float32, jnp.bfloat16, jnp.int32
    return pl.pallas_call(
        start_kernel,
        out_shape=[
            shape((slots // GROUP, GROUP, TILE, TILE), bf16), shape((2, 24, TILE), i32), shape((8, TILE), f32), shape(GATHERED, bf16)
        ],
        in_specs=[SMEM, HBM, HBM, HBM, HBM],
        out_specs=[HBM, VMEM, VMEM, VMEM],
        scratch_shapes=[
            pltpu.VMEM((slots // GROUP, GROUP, TILE, TILE), bf16),
            pltpu.VMEM((8, TILE, TILE), bf16),
            pltpu.VMEM((24, TILE), i32),
            pltpu.VMEM((2, 2, slots // 16, 8, TILE), i32),
            pltpu.VMEM(GATHERED, bf16),
            pltpu.VMEM((2, slots // 8, 8, TILE), f32),
            pltpu.VMEM((16, 8, TILE), f32),
            pltpu.VMEM((15, 8, TILE), f32),
            pltpu.VMEM((2, 4, 2, 8, TILE), f32),
            dma((slots // GROUP,)), dma((3,)), *[dma] * 5, *[dma((15,))] * 4,
            *spread_scratch(RAW_CHUNK),
        ],
        compiler_params=comm_params(0, START_LIMIT),
        name="start_build",
    )(
        counts, features.reshape(8, TILE, TILE), rows.reshape(8, TILE), cols.reshape(8, TILE),
        edges.reshape(2, slots // 16, 2, 8, TILE),
    )


def live_count(metas_ref, core, owner):
    count = metas_ref[owner, 16, 0]
    return count // 16 * 8 + jnp.clip(count % 16 - 8 * core, 0, 8)


def apply_kernel(carries, metas_ref, tiles_hbm, x_ref, *refs):
    if carries:
        carried, total, carried_out, tiles_ref, tile_sem, carry_sem = refs
        carry_copy = pltpu.make_async_copy(carried, carried_out, carry_sem)
        carry_copy.start()
    else:
        total, tiles_ref, tile_sem = refs
    core = lax.axis_index("col") % 2
    half_groups = tiles_ref.shape[0] // 2
    live = [(live_count(metas_ref, core, owner) + GROUP - 1) // GROUP for owner in range(2)]

    def tile_copy(bank):
        return pltpu.make_async_copy(tiles_hbm.at[bank], tiles_ref.at[bank], tile_sem.at[bank])

    for owner in range(2):
        def fetch(place, carry, owner=owner):
            tile_copy(owner * half_groups + place).start()
            return carry

        lax.fori_loop(0, live[owner], fetch, 0)
    total[...] = jnp.zeros_like(total)
    for owner in range(2):
        def apply_group(place, carry, owner=owner):
            bank = owner * half_groups + place
            tile_copy(bank).wait()
            for start in range(0, GROUP, BATCH):
                lanes = [8 * core + (i // 8 * 16 + i % 8) for i in range(start, start + BATCH)]
                products = [
                    jnp.dot(
                        x_ref[owner * 64 + metas_ref[owner, 8 + place, lane]],
                        tiles_ref[bank, start + j],
                        preferred_element_type=jnp.float32,
                    )
                    for j, lane in enumerate(lanes)
                ]
                for lane, product in zip(lanes, products):
                    total[metas_ref[owner, place, lane]] += product
            return carry

        lax.fori_loop(0, live[owner], apply_group, 0)
    if carries:
        carry_copy.wait()


def apply_tiles(metas, tiles, x, *carried):
    total = jax.ShapeDtypeStruct((TILE, TILE, TILE), jnp.float32)
    dma = pltpu.SemaphoreType.DMA
    return pl.pallas_call(
        functools.partial(apply_kernel, len(carried)),
        in_specs=[SMEM, HBM, VMEM] + [VMEM] * len(carried),
        out_specs=[VMEM] + [HBM] * len(carried),
        scratch_shapes=[pltpu.VMEM(tiles.shape, tiles.dtype), dma((tiles.shape[0],))] + [dma] * len(carried),
        out_shape=[total] + [jax.ShapeDtypeStruct(c.shape, c.dtype) for c in carried],
        compiler_params=pltpu.CompilerParams(vmem_limit_bytes=APPLY_LIMIT),
        name="apply_tiles",
    )(metas, tiles, x, *carried)


def sum_parts(part, root, spreads):
    hop = jax.ShapeDtypeStruct((8, TILE, TILE), jnp.bfloat16)
    gathered = jax.ShapeDtypeStruct(GATHERED, jnp.bfloat16)
    return pl.pallas_call(
        functools.partial(sum_kernel, spreads),
        out_shape=[hop, gathered] if spreads else [hop],
        in_specs=[VMEM, VMEM],
        out_specs=[VMEM, VMEM] if spreads else [VMEM],
        scratch_shapes=sum_scratch() + (spread_scratch(SUM_CHUNK) if spreads else []),
        compiler_params=comm_params(1 if spreads else 2, SUM_LIMIT),
        name="sum_spread" if spreads else "sum_last",
    )(part.reshape(2, 4, 2, 8, TILE, TILE), root)


def local(features, tile_rows, tile_cols, edge_lists, tile_counts):
    edges = edge_lists.reshape(2, *edge_lists.shape[3:])
    tiles, metas, root, gathered = start(tile_counts, features, tile_rows, tile_cols, edges)
    (part,) = apply_tiles(metas, tiles, gathered.reshape(128, TILE, TILE))
    hop_one, gathered = sum_parts(part, root, True)
    part, hop_one = apply_tiles(metas, tiles, gathered.reshape(128, TILE, TILE), hop_one)
    (hop_two,) = sum_parts(part, root, False)
    return (hop_one.reshape(features.shape), hop_two.reshape(features.shape))


def solution(mesh):
    placed = (
        P(("row", "col"), None),
        P("row", "col", None),
        P("row", "col", None),
        P(None, "row", "col", None, None),
        P("row", "col"),
    )
    return jax.shard_map(
        local,
        mesh=mesh,
        in_specs=placed,
        out_specs=(P(("row", "col"), None), P(("row", "col"), None)),
        check_vma=False,
    )
```

```python
import functools

import jax
import jax.numpy as jnp
from jax import lax
from jax.experimental import pallas as pl
from jax.experimental.pallas import tpu as pltpu
from jax.sharding import PartitionSpec as P

TILE = 128
GROUP = 64
BATCH = 8
SUM_CHUNK = 8
RAW_CHUNK = 2
START_LIMIT = 42 * 2**20
APPLY_LIMIT = 34 * 2**20
SUM_LIMIT = 12 * 2**20
SUM_LAGS = (0, 2, 4, 6, 6, 8, 10, 10, 12)


MESH = pl.DeviceIdType.MESH


class Place:
    def __init__(self):
        self.row, self.col = lax.axis_index("row"), lax.axis_index("col")
        self.y, self.x_lo = self.row // 2, self.row % 2
        self.x_hi, self.z, self.core = self.col // 8, (self.col // 2) % 4, self.col % 2

    def at(self, y=None, x_lo=None, x_hi=None, z=None, core=None):
        pick = lambda new, old: old if new is None else new
        row = pick(y, self.y) * 2 + pick(x_lo, self.x_lo)
        col = (pick(x_hi, self.x_hi) * 4 + pick(z, self.z)) * 2 + pick(core, self.core)
        return (row, col)


def greet(devices):
    barrier = pltpu.get_barrier_semaphore()
    for device in devices:
        pl.semaphore_signal(barrier, inc=1, device_id=device, device_id_type=MESH)
    pl.semaphore_wait(barrier, len(devices))


def sum_devices(me):
    return [
        me.at(core=1 - me.core),
        me.at(z=(me.z + 1) % 4),
        me.at(z=(me.z + 3) % 4),
        me.at(x_hi=1 - me.x_hi),
    ]


def spread_devices(me):
    return [me.at(x_lo=1 - me.x_lo), me.at(y=(me.y + 1) % 4), me.at(y=(me.y + 3) % 4)]


def run_stages(stages, lags, chunks):
    for tick in range(max(lags) + chunks):
        for stage, lag in zip(stages, lags):
            if 0 <= tick - lag < chunks:
                stage(tick - lag)


def each_tile(q, chunks, body):
    size = 8 // chunks

    def step(i, carry):
        body(q * size + i)
        return carry

    lax.fori_loop(0, size, step, 0)


def span(q, chunks):
    return pl.ds(q * (8 // chunks), 8 // chunks)


def wide(x):
    return x.astype(jnp.float32)


ALL, BOTH = slice(None), pl.ds(1, 2)


def sum_stages(me, part, bufs, sems, finish):
    given, running, arrived, kept, across, crossed = bufs
    pair_send, pair_recv, ring_send, head_recv, tail_recv, far_send, far_recv = sems
    chunks = SUM_CHUNK
    size = 8 // chunks
    whole = pl.ds(0, 8)

    def cut(q):
        return span(q, chunks)

    def pair_copy(where):
        return pltpu.make_async_remote_copy(
            part.at[:, :, 1 - me.core, where], given.at[:, :, where], pair_send, pair_recv.at[where.start // size],
            device_id=me.at(core=1 - me.core), device_id_type=MESH,
        )

    def ring_copy(half, step, where):
        q = where.start // size
        up = True if half == ALL else (half == 0) == (step != 2)
        return pltpu.make_async_remote_copy(
            running.at[half, step, where], arrived.at[half, step, where],
            ring_send, head_recv.at[q] if step == 0 else tail_recv.at[0 if half == ALL else half, q],
            device_id=me.at(z=(me.z + (1 if up else 3)) % 4), device_id_type=MESH,
        )

    def far_copy(where):
        return pltpu.make_async_remote_copy(
            across.at[where], crossed.at[where], far_send, far_recv.at[where.start // size],
            device_id=me.at(x_hi=1 - me.x_hi), device_id_type=MESH,
        )

    def begin():
        for q in range(chunks):
            pair_copy(cut(q)).start()

    def local_sum(half, offset, k):
        x_hi = me.x_hi if half == 0 else 1 - me.x_hi
        z = (me.z + (offset if half == 0 else 4 - offset)) % 4
        return part[x_hi, z, me.core, k] + given[x_hi, z, k]

    def first(q):
        pair_copy(cut(q)).wait_recv()
        for step, offset in ((0, 2), (2, 3)):
            for half in (1, 0):
                def body(k, half=half, step=step, offset=offset):
                    running[half, step, k] = local_sum(half, offset, k).astype(jnp.bfloat16)

                each_tile(q, chunks, body)
                ring_copy(half, step, cut(q)).start()

    def middle(q):
        ring_copy(ALL, 0, cut(q)).wait_recv()
        for half in (1, 0):

            def body(k, half=half):
                running[half, 1, k] = (local_sum(half, 1, k) + wide(arrived[half, 0, k])).astype(jnp.bfloat16)

            each_tile(q, chunks, body)
            ring_copy(half, 1, cut(q)).start()

    def last(q):
        for half in (1, 0):
            ring_copy(half, BOTH, cut(q)).wait_recv()

            def body(k, half=half):
                total = local_sum(half, 0, k) + (wide(arrived[half, 1, k]) + wide(arrived[half, 2, k]))
                if half == 1:
                    across[k] = total.astype(jnp.bfloat16)
                else:
                    kept[k] = total

            each_tile(q, chunks, body)
            if half == 1:
                far_copy(cut(q)).start()

    def done(q):
        far_copy(cut(q)).wait_recv()
        each_tile(q, chunks, lambda k: finish(k, kept[k] + wide(crossed[k])))

    def drain():
        pair_copy(whole).wait_send()
        far_copy(whole).wait_send()
        ring_copy(ALL, ALL, whole).wait_send()

    return begin, [first, middle, last, done], drain


def sum_scratch():
    block = lambda *lead, dtype=jnp.bfloat16: pltpu.VMEM((*lead, 8, TILE, TILE), dtype)
    dma = pltpu.SemaphoreType.DMA
    bufs = [block(2, 4, dtype=jnp.float32), block(2, 3), block(2, 3), block(dtype=jnp.float32), block(), block()]
    each = dma((SUM_CHUNK,))
    sems = [dma, each, dma, each, dma((2, SUM_CHUNK)), dma, each]
    return bufs + sems


N_SUM = 13


def spread_stages(me, gathered, sems, chunks):
    side_send, near_send, relay_send, pass_send, side_recv, own_recv, beside_recv, rest_recv, pass_recv = sems

    def copy(block, send, recv, device):
        return pltpu.make_async_remote_copy(block, block, send, recv, device_id=device, device_id_type=MESH)

    def block(y, x_lo, q):
        return gathered.at[me.core, (me.y + y) % 4, me.x_lo if x_lo == 0 else 1 - me.x_lo, span(q, chunks)]

    def along(way):
        return me.at(y=(me.y + (1 if way == 0 else 3)) % 4)

    beside_device, other_core = me.at(x_lo=1 - me.x_lo), me.at(core=1 - me.core)

    def side_copy(q):
        return copy(block(0, 0, q), side_send, side_recv.at[q], beside_device)

    def near_copy(kind, way, q):
        recv = rest_recv if kind != way else own_recv if kind == 0 else beside_recv
        return copy(block(0, kind, q), near_send, recv.at[q], along(way))

    def relay_copy(way, q):
        return copy(block(3 if way == 0 else 1, way, q), relay_send, rest_recv.at[q], along(way))

    def pass_copy(y, x_lo, q):
        return copy(block(y, x_lo, q), pass_send, pass_recv, other_core)

    def own(q):
        side_copy(q).start()
        near_copy(0, 0, q).start()
        near_copy(0, 1, q).start()
        pass_copy(0, 0, q).start()

    def beside(q):
        side_copy(q).wait_recv()
        near_copy(1, 0, q).start()
        near_copy(1, 1, q).start()
        pass_copy(0, 1, q).start()

    def relay_own(q):
        near_copy(0, 0, q).wait_recv()
        relay_copy(0, q).start()
        pass_copy(3, 0, q).start()

    def relay_beside(q):
        near_copy(1, 1, q).wait_recv()
        relay_copy(1, q).start()
        pass_copy(1, 1, q).start()

    def opposite(q):
        copy(gathered.at[me.core, :, 0, span(q, chunks)], relay_send, rest_recv.at[q], beside_device).wait_recv()
        pass_copy(1, 0, q).start()
        pass_copy(3, 1, q).start()
        pass_copy(2, 0, q).start()
        pass_copy(2, 1, q).start()

    def drain():
        copy(gathered.at[1 - me.core], pass_send, pass_recv, other_core).wait_recv()
        copy(gathered.at[me.core], pass_send, pass_recv, other_core).wait_send()
        copy(gathered.at[me.core, :, 0], near_send, pass_recv, other_core).wait_send()
        copy(gathered.at[me.core, 0], relay_send, pass_recv, other_core).wait_send()
        copy(gathered.at[me.core, 0, 0], side_send, pass_recv, other_core).wait_send()

    return [own, beside, relay_own, relay_beside, opposite], drain


def spread_scratch(chunks):
    dma = pltpu.SemaphoreType.DMA
    return [dma] * 4 + [dma((chunks,))] * 4 + [dma]


def hot(ids, cell):
    return jnp.where(jnp.broadcast_to(ids, (TILE, TILE)) == cell, jnp.bfloat16(1), jnp.bfloat16(0))


def narrow(x):
    return x.astype(jnp.float32).astype(jnp.bfloat16)


def start_kernel(
    count_ref, features_hbm, rows_hbm, cols_hbm, edges_ref, tiles_hbm, metas_ref, root_ref, gathered_ref,
    tiles_ref, features_ref, meta, lists, raw, slot_degree, degree, shares, roots,
    tile_sem, load_sem, list_sem, list_send, list_recv, meta_send, meta_recv, share_send, share_recv, root_send, root_recv, *sems,
):
    me = Place()
    peers = [lax.rem(me.col + i, 16) for i in range(1, 16)]
    across = me.col + 1 - 2 * me.core
    friends = [(lax.rem(me.row + i % 8, 8), me.col if i < 8 else across) for i in range(1, 16)]
    loads = [
        pltpu.make_async_copy(rows_hbm, meta.at[pl.ds(0, 8)], load_sem.at[0]),
        pltpu.make_async_copy(cols_hbm, meta.at[pl.ds(8, 8)], load_sem.at[1]),
        pltpu.make_async_copy(features_hbm, features_ref, load_sem.at[2]),
    ]
    own_lists = pltpu.make_async_copy(edges_ref.at[:, :, me.core], lists.at[me.core], list_sem)
    for load in loads:
        load.start()
    own_lists.start()
    meta[16:24, :] = jnp.full((8, TILE), count_ref[0, 0], jnp.int32)
    greet([(me.row, peer) for peer in peers] + [friend for i, friend in enumerate(friends) if i != 7])
    partner = me.at(core=1 - me.core)

    give_lists = pltpu.make_async_remote_copy(
        edges_ref.at[:, :, 1 - me.core], lists.at[me.core], list_send, list_recv, device_id=partner, device_id_type=MESH
    )
    give_meta = pltpu.make_async_remote_copy(
        meta, metas_ref.at[me.core], meta_send, meta_recv, device_id=partner, device_id_type=MESH
    )

    def tile_copy(bank):
        return pltpu.make_async_copy(tiles_ref.at[bank], tiles_hbm.at[bank], tile_sem)

    def share_copy(i):
        return pltpu.make_async_remote_copy(
            degree.at[peers[i]], shares.at[i], share_send, share_recv,
            device_id=(me.row, peers[i]), device_id_type=MESH,
        )

    def all_shares(send):
        return pltpu.make_async_remote_copy(
            shares, shares, send, share_recv, device_id=partner, device_id_type=MESH
        )

    def root_copy(i):
        block = roots.at[me.core, me.y, me.x_lo]
        return pltpu.make_async_remote_copy(
            block, block, root_send, root_recv.at[i], device_id=friends[i], device_id_type=MESH
        )

    give_lists.start()
    for load in loads:
        load.wait()
    give_meta.start()
    metas_ref[me.core] = meta[...]

    def turn(k, carry):
        raw[me.core, me.y, me.x_lo, k] = wide(features_ref[k]).T.astype(jnp.bfloat16)
        return carry

    lax.fori_loop(0, 8, turn, 0)
    slot_degree[...] = jnp.zeros_like(slot_degree)
    stages, drain = spread_stages(me, raw, sems, RAW_CHUNK)
    groups = 2 * lists.shape[2] * 8 // GROUP
    blocks = GROUP // 8
    own_lists.wait()

    def build(group, carry):
        for when, moves in RAW_MOVES:
            @pl.when(group == when)
            def _(moves=moves):
                for stage, q in moves:
                    stages[stage](q)

        @pl.when(group == groups // 2)
        def _():
            give_lists.wait_recv()
            give_meta.wait_recv()

        half = group // (groups // 2)
        place = group % (groups // 2)
        owner = me.core + half * (1 - 2 * me.core)
        bank = owner * (groups // 2) + place
        base = place * blocks

        shape = (blocks, 8, TILE)
        slot = (lax.broadcasted_iota(jnp.int32, shape, 0) + base) * 16 + 8 * me.core + lax.broadcasted_iota(jnp.int32, shape, 1)
        live = slot < jnp.broadcast_to(metas_ref[owner, 16:17, :].reshape(1, 1, TILE), shape)
        dst = jnp.where(live, lists[owner, 0, pl.ds(base, blocks)], -1).reshape(GROUP, TILE)
        src = lists[owner, 1, pl.ds(base, blocks)].reshape(GROUP, TILE)
        dst, src = narrow(dst), narrow(src)
        cell = narrow(lax.broadcasted_iota(jnp.int32, (TILE, TILE), 0))
        for block in range(blocks):
            totals = []
            for i in range(8 * block, 8 * block + 8):
                counts = lax.dot_general(
                    hot(src[i : i + 1, :], cell), hot(dst[i : i + 1, :], cell).astype(jnp.float8_e4m3fn), (((1,), (1,)), ((), ())),
                    preferred_element_type=jnp.float32,
                )
                tiles_ref[bank, i] = counts.astype(jnp.bfloat16)
                totals.append(jnp.sum(counts, axis=0, keepdims=True))
            slot_degree[owner, (base + block) * 2 + me.core] = jnp.concatenate(totals, axis=0)
        tile_copy(bank).start()
        return carry

    lax.fori_loop(0, groups, build, 0)

    cell = lax.broadcasted_iota(jnp.int32, (TILE, TILE), 0)
    counted = jnp.zeros((TILE, TILE), jnp.float32)
    for owner in range(2):
        for j in range(8):
            row_hot = (jnp.broadcast_to(metas_ref[owner, j : j + 1, :], (TILE, TILE)) == cell).astype(jnp.float32)
            slots = slot_degree[owner, 16 * j : 16 * j + 16].reshape(TILE, TILE)
            counted += jnp.dot(
                row_hot.astype(jnp.bfloat16), slots.astype(jnp.bfloat16), preferred_element_type=jnp.float32
            )
    degree[...] = counted.reshape(16, 8, TILE)
    for i in range(15):
        share_copy(i).start()
    for stage, q in RAW_LATE:
        stages[stage](q)
    total = degree[me.col]
    all_shares(share_send).wait_recv()
    for i in range(15):
        total = total + shares[i]
    root = lax.rsqrt(1.0 + total)
    root_ref[...] = root
    roots[me.core, me.y, me.x_lo] = root
    for i in range(15):
        root_copy(i).start()
    for q in range(RAW_CHUNK):
        stages[4](q)
    drain()

    def scale_block(c, row):
        y, x = row // 2, row % 2

        def scale(k, carry):
            gathered_ref[c, y, x, k] = (wide(raw[c, y, x, k]) * roots[c, y, x, pl.ds(k, 1), :]).astype(jnp.bfloat16)
            return carry

        lax.fori_loop(0, 8, scale, 0, unroll=4)

    scale_block(me.core, me.row)
    for i in (8, 2, 6, 10, 14, 1, 7, 9, 15, 3, 5, 11, 13, 4, 12):
        root_copy(i - 1).wait_recv()
        scale_block(me.core if i < 8 else 1 - me.core, lax.rem(me.row + 8 - i % 8, 8))
    all_shares(share_send).wait_send()
    all_shares(root_send).wait_send()
    give_lists.wait_send()
    give_meta.wait_send()
    pltpu.make_async_copy(tiles_ref, tiles_hbm, tile_sem).wait()


RAW_MOVES = (
    (0, ((0, 0), (0, 1))),
    (6, ((1, 0), (2, 0))),
    (10, ((1, 1), (2, 1))),
    (14, ((3, 0),)),
)
RAW_LATE = ((3, 1),)


def sum_kernel(spreads, part_ref, root_ref, hop_ref, *refs):
    me = Place()
    gathered_ref = refs[0] if spreads else None
    scratch = refs[1:] if spreads else refs
    greet(sum_devices(me) + (spread_devices(me) if spreads else []))

    def finish(k, total):
        root = root_ref[pl.ds(k, 1), :]
        hop_ref[k] = (total * root).T.astype(jnp.bfloat16)
        if spreads:
            gathered_ref[me.core, me.y, me.x_lo, k] = (total * (root * root)).astype(jnp.bfloat16)

    begin, stages, drain = sum_stages(me, part_ref, scratch[:6], scratch[6:N_SUM], finish)
    begin()
    if spreads:
        more, drain_spread = spread_stages(me, gathered_ref, scratch[N_SUM:], SUM_CHUNK)
        run_stages(stages + more, SUM_LAGS, SUM_CHUNK)
        drain_spread()
    else:
        run_stages(stages, SUM_LAGS[:4], SUM_CHUNK)
    drain()


VMEM = pl.BlockSpec(memory_space=pltpu.VMEM)
SMEM = pl.BlockSpec(memory_space=pltpu.SMEM)
HBM = pl.BlockSpec(memory_space=pltpu.HBM)
GATHERED = (2, 4, 2, 8, TILE, TILE)


def comm_params(number, limit):
    return pltpu.CompilerParams(collective_id=number, has_side_effects=True, vmem_limit_bytes=limit)


def start(counts, features, rows, cols, edges):
    dma = pltpu.SemaphoreType.DMA
    slots = edges.shape[1]
    shape = jax.ShapeDtypeStruct
    f32, bf16, i32 = jnp.float32, jnp.bfloat16, jnp.int32
    return pl.pallas_call(
        start_kernel,
        out_shape=[
            shape((slots // GROUP, GROUP, TILE, TILE), bf16), shape((2, 24, TILE), i32), shape((8, TILE), f32), shape(GATHERED, bf16)
        ],
        in_specs=[SMEM, HBM, HBM, HBM, HBM],
        out_specs=[HBM, VMEM, VMEM, VMEM],
        scratch_shapes=[
            pltpu.VMEM((slots // GROUP, GROUP, TILE, TILE), bf16),
            pltpu.VMEM((8, TILE, TILE), bf16),
            pltpu.VMEM((24, TILE), i32),
            pltpu.VMEM((2, 2, slots // 16, 8, TILE), i32),
            pltpu.VMEM(GATHERED, bf16),
            pltpu.VMEM((2, slots // 8, 8, TILE), f32),
            pltpu.VMEM((16, 8, TILE), f32),
            pltpu.VMEM((15, 8, TILE), f32),
            pltpu.VMEM((2, 4, 2, 8, TILE), f32),
            dma, dma((3,)), *[dma] * 8, dma((15,)),
            *spread_scratch(RAW_CHUNK),
        ],
        compiler_params=comm_params(0, START_LIMIT),
        name="start_build",
    )(
        counts, features.reshape(8, TILE, TILE), rows.reshape(8, TILE), cols.reshape(8, TILE),
        edges.reshape(2, slots // 16, 2, 8, TILE),
    )


def live_count(metas_ref, core, owner):
    count = metas_ref[owner, 16, 0]
    return count // 16 * 8 + jnp.clip(count % 16 - 8 * core, 0, 8)


def apply_kernel(carries, metas_ref, tiles_hbm, x_ref, *refs):
    if carries:
        carried, total, carried_out, tiles_ref, tile_sem, carry_sem = refs
        carry_copy = pltpu.make_async_copy(carried, carried_out, carry_sem)
        carry_copy.start()
    else:
        total, tiles_ref, tile_sem = refs
    core = lax.axis_index("col") % 2
    half_groups = tiles_ref.shape[0] // 2
    live = [(live_count(metas_ref, core, owner) + GROUP - 1) // GROUP for owner in range(2)]

    def tile_copy(bank):
        return pltpu.make_async_copy(tiles_hbm.at[bank], tiles_ref.at[bank], tile_sem.at[bank])

    for owner in range(2):
        def fetch(place, carry, owner=owner):
            tile_copy(owner * half_groups + place).start()
            return carry

        lax.fori_loop(0, live[owner], fetch, 0)
    total[...] = jnp.zeros_like(total)
    for owner in range(2):
        def apply_group(place, carry, owner=owner):
            bank = owner * half_groups + place
            tile_copy(bank).wait()
            for start in range(0, GROUP, BATCH):
                lanes = [8 * core + (i // 8 * 16 + i % 8) for i in range(start, start + BATCH)]
                products = [
                    jnp.dot(
                        x_ref[owner * 64 + metas_ref[owner, 8 + place, lane]],
                        tiles_ref[bank, start + j],
                        preferred_element_type=jnp.float32,
                    )
                    for j, lane in enumerate(lanes)
                ]
                for lane, product in zip(lanes, products):
                    total[metas_ref[owner, place, lane]] += product
            return carry

        lax.fori_loop(0, live[owner], apply_group, 0)
    if carries:
        carry_copy.wait()


def apply_tiles(metas, tiles, x, *carried):
    total = jax.ShapeDtypeStruct((TILE, TILE, TILE), jnp.float32)
    dma = pltpu.SemaphoreType.DMA
    return pl.pallas_call(
        functools.partial(apply_kernel, len(carried)),
        in_specs=[SMEM, HBM, VMEM] + [VMEM] * len(carried),
        out_specs=[VMEM] + [HBM] * len(carried),
        scratch_shapes=[pltpu.VMEM(tiles.shape, tiles.dtype), dma((tiles.shape[0],))] + [dma] * len(carried),
        out_shape=[total] + [jax.ShapeDtypeStruct(c.shape, c.dtype) for c in carried],
        compiler_params=pltpu.CompilerParams(vmem_limit_bytes=APPLY_LIMIT),
        name="apply_tiles",
    )(metas, tiles, x, *carried)


def sum_parts(part, root, spreads):
    hop = jax.ShapeDtypeStruct((8, TILE, TILE), jnp.bfloat16)
    gathered = jax.ShapeDtypeStruct(GATHERED, jnp.bfloat16)
    return pl.pallas_call(
        functools.partial(sum_kernel, spreads),
        out_shape=[hop, gathered] if spreads else [hop],
        in_specs=[VMEM, VMEM],
        out_specs=[VMEM, VMEM] if spreads else [VMEM],
        scratch_shapes=sum_scratch() + (spread_scratch(SUM_CHUNK) if spreads else []),
        compiler_params=comm_params(1 if spreads else 2, SUM_LIMIT),
        name="sum_spread" if spreads else "sum_last",
    )(part.reshape(2, 4, 2, 8, TILE, TILE), root)


def local(features, tile_rows, tile_cols, edge_lists, tile_counts):
    edges = edge_lists.reshape(2, *edge_lists.shape[3:])
    tiles, metas, root, gathered = start(tile_counts, features, tile_rows, tile_cols, edges)
    (part,) = apply_tiles(metas, tiles, gathered.reshape(128, TILE, TILE))
    hop_one, gathered = sum_parts(part, root, True)
    part, hop_one = apply_tiles(metas, tiles, gathered.reshape(128, TILE, TILE), hop_one)
    (hop_two,) = sum_parts(part, root, False)
    return (hop_one.reshape(features.shape), hop_two.reshape(features.shape))


def solution(mesh):
    placed = (
        P(("row", "col"), None),
        P("row", "col", None),
        P("row", "col", None),
        P(None, "row", "col", None, None),
        P("row", "col"),
    )
    return jax.shard_map(
        local,
        mesh=mesh,
        in_specs=placed,
        out_specs=(P(("row", "col"), None), P(("row", "col"), None)),
        check_vma=False,
    )
```

```python
import functools

import jax
import jax.numpy as jnp
from jax import lax
from jax.experimental import pallas as pl
from jax.experimental.pallas import tpu as pltpu
from jax.sharding import PartitionSpec as P

TILE = 128
GROUP = 64
BATCH = 8
SUM_CHUNK = 8
RAW_CHUNK = 2
START_LIMIT = 42 * 2**20
APPLY_LIMIT = 34 * 2**20
SUM_LIMIT = 12 * 2**20
SUM_LAGS = (0, 2, 4, 6, 6, 8, 10, 10, 12)


MESH = pl.DeviceIdType.MESH


class Place:
    def __init__(self):
        self.row, self.col = lax.axis_index("row"), lax.axis_index("col")
        self.y, self.x_lo = self.row // 2, self.row % 2
        self.x_hi, self.z, self.core = self.col // 8, (self.col // 2) % 4, self.col % 2

    def at(self, y=None, x_lo=None, x_hi=None, z=None, core=None):
        pick = lambda new, old: old if new is None else new
        row = pick(y, self.y) * 2 + pick(x_lo, self.x_lo)
        col = (pick(x_hi, self.x_hi) * 4 + pick(z, self.z)) * 2 + pick(core, self.core)
        return (row, col)


def greet(devices):
    barrier = pltpu.get_barrier_semaphore()
    for device in devices:
        pl.semaphore_signal(barrier, inc=1, device_id=device, device_id_type=MESH)
    pl.semaphore_wait(barrier, len(devices))


def sum_devices(me):
    return [
        me.at(core=1 - me.core),
        me.at(z=(me.z + 1) % 4),
        me.at(z=(me.z + 3) % 4),
        me.at(x_hi=1 - me.x_hi),
    ]


def spread_devices(me):
    return [me.at(x_lo=1 - me.x_lo), me.at(y=(me.y + 1) % 4), me.at(y=(me.y + 3) % 4)]


def run_stages(stages, lags, chunks):
    for tick in range(max(lags) + chunks):
        for stage, lag in zip(stages, lags):
            if 0 <= tick - lag < chunks:
                stage(tick - lag)


def each_tile(q, chunks, body):
    size = 8 // chunks

    def step(i, carry):
        body(q * size + i)
        return carry

    lax.fori_loop(0, size, step, 0)


def span(q, chunks):
    return pl.ds(q * (8 // chunks), 8 // chunks)


def wide(x):
    return x.astype(jnp.float32)


ALL, BOTH = slice(None), pl.ds(1, 2)


def sum_stages(me, part, bufs, sems, finish):
    given, running, arrived, kept, across, crossed = bufs
    pair_send, pair_recv, ring_send, head_recv, tail_recv, far_send, far_recv = sems
    chunks = SUM_CHUNK
    size = 8 // chunks
    whole = pl.ds(0, 8)

    def cut(q):
        return span(q, chunks)

    def pair_copy(where):
        return pltpu.make_async_remote_copy(
            part.at[:, :, 1 - me.core, where], given.at[:, :, where], pair_send, pair_recv.at[where.start // size],
            device_id=me.at(core=1 - me.core), device_id_type=MESH,
        )

    def ring_copy(half, step, where):
        q = where.start // size
        up = True if half == ALL else (half == 0) == (step != 2)
        return pltpu.make_async_remote_copy(
            running.at[half, step, where], arrived.at[half, step, where],
            ring_send, head_recv.at[q] if step == 0 else tail_recv.at[0 if half == ALL else half, q],
            device_id=me.at(z=(me.z + (1 if up else 3)) % 4), device_id_type=MESH,
        )

    def far_copy(where):
        return pltpu.make_async_remote_copy(
            across.at[where], crossed.at[where], far_send, far_recv.at[where.start // size],
            device_id=me.at(x_hi=1 - me.x_hi), device_id_type=MESH,
        )

    def begin():
        for q in range(chunks):
            pair_copy(cut(q)).start()

    def local_sum(half, offset, k):
        x_hi = me.x_hi if half == 0 else 1 - me.x_hi
        z = (me.z + (offset if half == 0 else 4 - offset)) % 4
        return part[x_hi, z, me.core, k] + given[x_hi, z, k]

    def first(q):
        pair_copy(cut(q)).wait_recv()
        for step, offset in ((0, 2), (2, 3)):
            for half in (1, 0):
                def body(k, half=half, step=step, offset=offset):
                    running[half, step, k] = local_sum(half, offset, k).astype(jnp.bfloat16)

                each_tile(q, chunks, body)
                ring_copy(half, step, cut(q)).start()

    def middle(q):
        ring_copy(ALL, 0, cut(q)).wait_recv()
        for half in (1, 0):

            def body(k, half=half):
                running[half, 1, k] = (local_sum(half, 1, k) + wide(arrived[half, 0, k])).astype(jnp.bfloat16)

            each_tile(q, chunks, body)
            ring_copy(half, 1, cut(q)).start()

    def last(q):
        for half in (1, 0):
            ring_copy(half, BOTH, cut(q)).wait_recv()

            def body(k, half=half):
                total = local_sum(half, 0, k) + (wide(arrived[half, 1, k]) + wide(arrived[half, 2, k]))
                if half == 1:
                    across[k] = total.astype(jnp.bfloat16)
                else:
                    kept[k] = total

            each_tile(q, chunks, body)
            if half == 1:
                far_copy(cut(q)).start()

    def done(q):
        far_copy(cut(q)).wait_recv()
        each_tile(q, chunks, lambda k: finish(k, kept[k] + wide(crossed[k])))

    def drain():
        pair_copy(whole).wait_send()
        far_copy(whole).wait_send()
        ring_copy(ALL, ALL, whole).wait_send()

    return begin, [first, middle, last, done], drain


def sum_scratch():
    block = lambda *lead, dtype=jnp.bfloat16: pltpu.VMEM((*lead, 8, TILE, TILE), dtype)
    dma = pltpu.SemaphoreType.DMA
    bufs = [block(2, 4, dtype=jnp.float32), block(2, 3), block(2, 3), block(dtype=jnp.float32), block(), block()]
    each = dma((SUM_CHUNK,))
    sems = [dma, each, dma, each, dma((2, SUM_CHUNK)), dma, each]
    return bufs + sems


N_SUM = 13


def spread_stages(me, gathered, sems, chunks):
    side_send, near_send, relay_send, pass_send, side_recv, own_recv, beside_recv, rest_recv, pass_recv = sems

    def copy(block, send, recv, device):
        return pltpu.make_async_remote_copy(block, block, send, recv, device_id=device, device_id_type=MESH)

    def block(y, x_lo, q):
        return gathered.at[me.core, (me.y + y) % 4, me.x_lo if x_lo == 0 else 1 - me.x_lo, span(q, chunks)]

    def along(way):
        return me.at(y=(me.y + (1 if way == 0 else 3)) % 4)

    beside_device, other_core = me.at(x_lo=1 - me.x_lo), me.at(core=1 - me.core)

    def side_copy(q):
        return copy(block(0, 0, q), side_send, side_recv.at[q], beside_device)

    def near_copy(kind, way, q):
        recv = rest_recv if kind != way else own_recv if kind == 0 else beside_recv
        return copy(block(0, kind, q), near_send, recv.at[q], along(way))

    def relay_copy(way, q):
        return copy(block(3 if way == 0 else 1, way, q), relay_send, rest_recv.at[q], along(way))

    def pass_copy(y, x_lo, q):
        return copy(block(y, x_lo, q), pass_send, pass_recv, other_core)

    def own(q):
        side_copy(q).start()
        near_copy(0, 0, q).start()
        near_copy(0, 1, q).start()
        pass_copy(0, 0, q).start()

    def beside(q):
        side_copy(q).wait_recv()
        near_copy(1, 0, q).start()
        near_copy(1, 1, q).start()
        pass_copy(0, 1, q).start()

    def relay_own(q):
        near_copy(0, 0, q).wait_recv()
        relay_copy(0, q).start()
        pass_copy(3, 0, q).start()

    def relay_beside(q):
        near_copy(1, 1, q).wait_recv()
        relay_copy(1, q).start()
        pass_copy(1, 1, q).start()

    def opposite(q):
        copy(gathered.at[me.core, :, 0, span(q, chunks)], relay_send, rest_recv.at[q], beside_device).wait_recv()
        pass_copy(1, 0, q).start()
        pass_copy(3, 1, q).start()
        pass_copy(2, 0, q).start()
        pass_copy(2, 1, q).start()

    def drain():
        copy(gathered.at[1 - me.core], pass_send, pass_recv, other_core).wait_recv()
        copy(gathered.at[me.core], pass_send, pass_recv, other_core).wait_send()
        copy(gathered.at[me.core, :, 0], near_send, pass_recv, other_core).wait_send()
        copy(gathered.at[me.core, 0], relay_send, pass_recv, other_core).wait_send()
        copy(gathered.at[me.core, 0, 0], side_send, pass_recv, other_core).wait_send()

    return [own, beside, relay_own, relay_beside, opposite], drain


def spread_scratch(chunks):
    dma = pltpu.SemaphoreType.DMA
    return [dma] * 4 + [dma((chunks,))] * 4 + [dma]


def hot(ids, cell):
    return jnp.where(jnp.broadcast_to(ids, (TILE, TILE)) == cell, jnp.bfloat16(1), jnp.bfloat16(0))


def narrow(x):
    return x.astype(jnp.float32).astype(jnp.bfloat16)


def start_kernel(
    features_ref, meta_ref, edges_ref, tiles_hbm, metas_ref, root_ref, gathered_ref,
    tiles_ref, lists, raw, slot_degree, degree, shares, roots,
    tile_sem, list_sem, list_send, list_recv, meta_send, meta_recv, share_send, share_recv, root_send, root_recv, *sems,
):
    me = Place()
    peers = [lax.rem(me.col + i, 16) for i in range(1, 16)]
    across = me.col + 1 - 2 * me.core
    friends = [(lax.rem(me.row + i % 8, 8), me.col if i < 8 else across) for i in range(1, 16)]
    own_lists = pltpu.make_async_copy(edges_ref.at[:, :, me.core], lists.at[me.core], list_sem)
    own_lists.start()
    everyone = [(me.row, peer) for peer in peers] + [friend for i, friend in enumerate(friends) if i != 7]
    barrier = pltpu.get_barrier_semaphore()
    for device in everyone:
        pl.semaphore_signal(barrier, inc=1, device_id=device, device_id_type=MESH)
    partner = me.at(core=1 - me.core)

    give_lists = pltpu.make_async_remote_copy(
        edges_ref.at[:, :, 1 - me.core], lists.at[me.core], list_send, list_recv, device_id=partner, device_id_type=MESH
    )
    give_meta = pltpu.make_async_remote_copy(
        meta_ref, metas_ref.at[me.core], meta_send, meta_recv, device_id=partner, device_id_type=MESH
    )

    def tile_copy(bank):
        return pltpu.make_async_copy(tiles_ref.at[bank], tiles_hbm.at[bank], tile_sem)

    def share_copy(i):
        return pltpu.make_async_remote_copy(
            degree.at[peers[i]], shares.at[i], share_send, share_recv,
            device_id=(me.row, peers[i]), device_id_type=MESH,
        )

    def all_shares(send):
        return pltpu.make_async_remote_copy(
            shares, shares, send, share_recv, device_id=partner, device_id_type=MESH
        )

    def root_copy(i):
        block = roots.at[me.core, me.y, me.x_lo]
        return pltpu.make_async_remote_copy(
            block, block, root_send, root_recv.at[i], device_id=friends[i], device_id_type=MESH
        )

    metas_ref[me.core] = meta_ref[...]

    def turn(k, carry):
        raw[me.core, me.y, me.x_lo, k] = wide(features_ref[k]).T.astype(jnp.bfloat16)
        return carry

    lax.fori_loop(0, 8, turn, 0, unroll=4)
    slot_degree[...] = jnp.zeros_like(slot_degree)
    stages, drain = spread_stages(me, raw, sems, RAW_CHUNK)
    groups = 2 * lists.shape[2] * 8 // GROUP
    blocks = GROUP // 8
    own_lists.wait()

    def build(group, carry):
        @pl.when(group == RAW_MOVES[0][0])
        def _():
            pl.semaphore_wait(barrier, len(everyone))
            give_lists.start()
            give_meta.start()

        for when, moves in RAW_MOVES:
            @pl.when(group == when)
            def _(moves=moves):
                for stage, q in moves:
                    stages[stage](q)

        @pl.when(group == groups // 2)
        def _():
            give_lists.wait_recv()
            give_meta.wait_recv()

        half = group // (groups // 2)
        place = group % (groups // 2)
        owner = me.core + half * (1 - 2 * me.core)
        bank = owner * (groups // 2) + place
        base = place * blocks

        shape = (blocks, 8, TILE)
        slot = (lax.broadcasted_iota(jnp.int32, shape, 0) + base) * 16 + 8 * me.core + lax.broadcasted_iota(jnp.int32, shape, 1)
        live = slot < jnp.broadcast_to(metas_ref[owner, 16:17, :].reshape(1, 1, TILE), shape)
        dst = jnp.where(live, lists[owner, 0, pl.ds(base, blocks)], -1).reshape(GROUP, TILE)
        src = lists[owner, 1, pl.ds(base, blocks)].reshape(GROUP, TILE)
        dst, src = narrow(dst), narrow(src)
        cell = narrow(lax.broadcasted_iota(jnp.int32, (TILE, TILE), 0))
        for block in range(blocks):
            totals = []
            for i in range(8 * block, 8 * block + 8):
                counts = lax.dot_general(
                    hot(src[i : i + 1, :], cell), hot(dst[i : i + 1, :], cell).astype(jnp.float8_e4m3fn), (((1,), (1,)), ((), ())),
                    preferred_element_type=jnp.float32,
                )
                tiles_ref[bank, i] = counts.astype(jnp.bfloat16)
                totals.append(jnp.sum(counts, axis=0, keepdims=True))
            slot_degree[owner, (base + block) * 2 + me.core] = jnp.concatenate(totals, axis=0)
        tile_copy(bank).start()
        return carry

    lax.fori_loop(0, groups, build, 0)

    cell = lax.broadcasted_iota(jnp.int32, (TILE, TILE), 0)
    counted = jnp.zeros((TILE, TILE), jnp.float32)
    for owner in range(2):
        for j in range(8):
            row_hot = (jnp.broadcast_to(metas_ref[owner, j : j + 1, :], (TILE, TILE)) == cell).astype(jnp.float32)
            slots = slot_degree[owner, 16 * j : 16 * j + 16].reshape(TILE, TILE)
            counted += jnp.dot(
                row_hot.astype(jnp.bfloat16), slots.astype(jnp.bfloat16), preferred_element_type=jnp.float32
            )
    degree[...] = counted.reshape(16, 8, TILE)
    for i in range(15):
        share_copy(i).start()
    for stage, q in RAW_LATE:
        stages[stage](q)
    total = degree[me.col]
    all_shares(share_send).wait_recv()
    for i in range(15):
        total = total + shares[i]
    root = lax.rsqrt(1.0 + total)
    root_ref[...] = root
    roots[me.core, me.y, me.x_lo] = root
    for i in range(15):
        root_copy(i).start()
    for q in range(RAW_CHUNK):
        stages[4](q)
    drain()

    def scale_block(c, row):
        y, x = row // 2, row % 2

        def scale(k, carry):
            gathered_ref[c, y, x, k] = (wide(raw[c, y, x, k]) * roots[c, y, x, pl.ds(k, 1), :]).astype(jnp.bfloat16)
            return carry

        lax.fori_loop(0, 8, scale, 0, unroll=4)

    scale_block(me.core, me.row)
    for i in (8, 2, 6, 10, 14, 1, 7, 9, 15, 3, 5, 11, 13, 4, 12):
        root_copy(i - 1).wait_recv()
        scale_block(me.core if i < 8 else 1 - me.core, lax.rem(me.row + 8 - i % 8, 8))
    all_shares(share_send).wait_send()
    all_shares(root_send).wait_send()
    give_lists.wait_send()
    give_meta.wait_send()
    pltpu.make_async_copy(tiles_ref, tiles_hbm, tile_sem).wait()


RAW_MOVES = (
    (3, ((0, 0), (0, 1))),
    (9, ((1, 0), (2, 0))),
    (13, ((1, 1), (2, 1))),
)
RAW_LATE = ((3, 0), (3, 1))


def sum_kernel(spreads, part_ref, root_ref, hop_ref, *refs):
    me = Place()
    gathered_ref = refs[0] if spreads else None
    scratch = refs[1:] if spreads else refs
    greet(sum_devices(me) + (spread_devices(me) if spreads else []))

    def finish(k, total):
        root = root_ref[pl.ds(k, 1), :]
        hop_ref[k] = (total * root).T.astype(jnp.bfloat16)
        if spreads:
            gathered_ref[me.core, me.y, me.x_lo, k] = (total * (root * root)).astype(jnp.bfloat16)

    begin, stages, drain = sum_stages(me, part_ref, scratch[:6], scratch[6:N_SUM], finish)
    begin()
    if spreads:
        more, drain_spread = spread_stages(me, gathered_ref, scratch[N_SUM:], SUM_CHUNK)
        run_stages(stages + more, SUM_LAGS, SUM_CHUNK)
        drain_spread()
    else:
        run_stages(stages, SUM_LAGS[:4], SUM_CHUNK)
    drain()


VMEM = pl.BlockSpec(memory_space=pltpu.VMEM)
SMEM = pl.BlockSpec(memory_space=pltpu.SMEM)
HBM = pl.BlockSpec(memory_space=pltpu.HBM)
GATHERED = (2, 4, 2, 8, TILE, TILE)


def comm_params(number, limit):
    return pltpu.CompilerParams(collective_id=number, has_side_effects=True, vmem_limit_bytes=limit)


def start(features, meta, edges):
    dma = pltpu.SemaphoreType.DMA
    slots = edges.shape[1]
    shape = jax.ShapeDtypeStruct
    f32, bf16, i32 = jnp.float32, jnp.bfloat16, jnp.int32
    return pl.pallas_call(
        start_kernel,
        out_shape=[
            shape((slots // GROUP, GROUP, TILE, TILE), bf16), shape((2, 24, TILE), i32), shape((8, TILE), f32), shape(GATHERED, bf16)
        ],
        in_specs=[VMEM, VMEM, HBM],
        out_specs=[HBM, VMEM, VMEM, VMEM],
        scratch_shapes=[
            pltpu.VMEM((slots // GROUP, GROUP, TILE, TILE), bf16),
            pltpu.VMEM((2, 2, slots // 16, 8, TILE), i32),
            pltpu.VMEM(GATHERED, bf16),
            pltpu.VMEM((2, slots // 8, 8, TILE), f32),
            pltpu.VMEM((16, 8, TILE), f32),
            pltpu.VMEM((15, 8, TILE), f32),
            pltpu.VMEM((2, 4, 2, 8, TILE), f32),
            *[dma] * 9, dma((15,)),
            *spread_scratch(RAW_CHUNK),
        ],
        compiler_params=comm_params(0, START_LIMIT),
        name="start_build",
    )(features.reshape(8, TILE, TILE), meta, edges.reshape(2, slots // 16, 2, 8, TILE))


def live_count(metas_ref, core, owner):
    count = metas_ref[owner, 16, 0]
    return count // 16 * 8 + jnp.clip(count % 16 - 8 * core, 0, 8)


def apply_kernel(carries, metas_ref, tiles_hbm, x_ref, *refs):
    if carries:
        carried, total, carried_out, tiles_ref, tile_sem, carry_sem = refs
        carry_copy = pltpu.make_async_copy(carried, carried_out, carry_sem)
        carry_copy.start()
    else:
        total, tiles_ref, tile_sem = refs
    core = lax.axis_index("col") % 2
    half_groups = tiles_ref.shape[0] // 2
    live = [(live_count(metas_ref, core, owner) + GROUP - 1) // GROUP for owner in range(2)]

    def tile_copy(bank):
        return pltpu.make_async_copy(tiles_hbm.at[bank], tiles_ref.at[bank], tile_sem.at[bank])

    for owner in range(2):
        def fetch(place, carry, owner=owner):
            tile_copy(owner * half_groups + place).start()
            return carry

        lax.fori_loop(0, live[owner], fetch, 0)
    total[...] = jnp.zeros_like(total)
    for owner in range(2):
        def apply_group(place, carry, owner=owner):
            bank = owner * half_groups + place
            tile_copy(bank).wait()
            for start in range(0, GROUP, BATCH):
                lanes = [8 * core + (i // 8 * 16 + i % 8) for i in range(start, start + BATCH)]
                products = [
                    jnp.dot(
                        x_ref[owner * 64 + metas_ref[owner, 8 + place, lane]],
                        tiles_ref[bank, start + j],
                        preferred_element_type=jnp.float32,
                    )
                    for j, lane in enumerate(lanes)
                ]
                for lane, product in zip(lanes, products):
                    total[metas_ref[owner, place, lane]] += product
            return carry

        lax.fori_loop(0, live[owner], apply_group, 0)
    if carries:
        carry_copy.wait()


def apply_tiles(metas, tiles, x, *carried):
    total = jax.ShapeDtypeStruct((TILE, TILE, TILE), jnp.float32)
    dma = pltpu.SemaphoreType.DMA
    return pl.pallas_call(
        functools.partial(apply_kernel, len(carried)),
        in_specs=[SMEM, HBM, VMEM] + [VMEM] * len(carried),
        out_specs=[VMEM] + [HBM] * len(carried),
        scratch_shapes=[pltpu.VMEM(tiles.shape, tiles.dtype), dma((tiles.shape[0],))] + [dma] * len(carried),
        out_shape=[total] + [jax.ShapeDtypeStruct(c.shape, c.dtype) for c in carried],
        compiler_params=pltpu.CompilerParams(vmem_limit_bytes=APPLY_LIMIT),
        name="apply_tiles",
    )(metas, tiles, x, *carried)


def sum_parts(part, root, spreads):
    hop = jax.ShapeDtypeStruct((8, TILE, TILE), jnp.bfloat16)
    gathered = jax.ShapeDtypeStruct(GATHERED, jnp.bfloat16)
    return pl.pallas_call(
        functools.partial(sum_kernel, spreads),
        out_shape=[hop, gathered] if spreads else [hop],
        in_specs=[VMEM, VMEM],
        out_specs=[VMEM, VMEM] if spreads else [VMEM],
        scratch_shapes=sum_scratch() + (spread_scratch(SUM_CHUNK) if spreads else []),
        compiler_params=comm_params(1 if spreads else 2, SUM_LIMIT),
        name="sum_spread" if spreads else "sum_last",
    )(part.reshape(2, 4, 2, 8, TILE, TILE), root)


def local(features, tile_rows, tile_cols, edge_lists, tile_counts):
    edges = edge_lists.reshape(2, *edge_lists.shape[3:])
    meta = jnp.concatenate(
        [tile_rows.reshape(8, TILE), tile_cols.reshape(8, TILE), jnp.broadcast_to(tile_counts, (8, TILE))], axis=0
    )
    tiles, metas, root, gathered = start(features, meta, edges)
    (part,) = apply_tiles(metas, tiles, gathered.reshape(128, TILE, TILE))
    hop_one, gathered = sum_parts(part, root, True)
    part, hop_one = apply_tiles(metas, tiles, gathered.reshape(128, TILE, TILE), hop_one)
    (hop_two,) = sum_parts(part, root, False)
    return (hop_one.reshape(features.shape), hop_two.reshape(features.shape))


def solution(mesh):
    placed = (
        P(("row", "col"), None),
        P("row", "col", None),
        P("row", "col", None),
        P(None, "row", "col", None, None),
        P("row", "col"),
    )
    return jax.shard_map(
        local,
        mesh=mesh,
        in_specs=placed,
        out_specs=(P(("row", "col"), None), P(("row", "col"), None)),
        check_vma=False,
    )
```

```python
import functools

import jax
import jax.numpy as jnp
from jax import lax
from jax.experimental import pallas as pl
from jax.experimental.pallas import tpu as pltpu
from jax.sharding import PartitionSpec as P

TILE = 128
GROUP = 64
BATCH = 8
SUM_CHUNK = 8
RAW_CHUNK = 2
START_LIMIT = 42 * 2**20
APPLY_LIMIT = 34 * 2**20
SUM_LIMIT = 12 * 2**20
SUM_LAGS = (0, 2, 4, 6, 6, 8, 10, 10, 12)


MESH = pl.DeviceIdType.MESH


class Place:
    def __init__(self):
        self.row, self.col = lax.axis_index("row"), lax.axis_index("col")
        self.y, self.x_lo = self.row // 2, self.row % 2
        self.x_hi, self.z, self.core = self.col // 8, (self.col // 2) % 4, self.col % 2

    def at(self, y=None, x_lo=None, x_hi=None, z=None, core=None):
        pick = lambda new, old: old if new is None else new
        row = pick(y, self.y) * 2 + pick(x_lo, self.x_lo)
        col = (pick(x_hi, self.x_hi) * 4 + pick(z, self.z)) * 2 + pick(core, self.core)
        return (row, col)


def greet(devices):
    barrier = pltpu.get_barrier_semaphore()
    for device in devices:
        pl.semaphore_signal(barrier, inc=1, device_id=device, device_id_type=MESH)
    pl.semaphore_wait(barrier, len(devices))


def sum_devices(me):
    return [
        me.at(core=1 - me.core),
        me.at(z=(me.z + 1) % 4),
        me.at(z=(me.z + 3) % 4),
        me.at(x_hi=1 - me.x_hi),
    ]


def spread_devices(me):
    return [me.at(x_lo=1 - me.x_lo), me.at(y=(me.y + 1) % 4), me.at(y=(me.y + 3) % 4)]


def run_stages(stages, lags, chunks):
    for tick in range(max(lags) + chunks):
        for stage, lag in zip(stages, lags):
            if 0 <= tick - lag < chunks:
                stage(tick - lag)


def each_tile(q, chunks, body):
    size = 8 // chunks

    def step(i, carry):
        body(q * size + i)
        return carry

    lax.fori_loop(0, size, step, 0)


def span(q, chunks):
    return pl.ds(q * (8 // chunks), 8 // chunks)


def wide(x):
    return x.astype(jnp.float32)


ALL, BOTH = slice(None), pl.ds(1, 2)


def sum_stages(me, part, bufs, sems, finish):
    given, running, arrived, kept, across, crossed = bufs
    pair_send, pair_recv, ring_send, head_recv, tail_recv, far_send, far_recv = sems
    chunks = SUM_CHUNK
    size = 8 // chunks
    whole = pl.ds(0, 8)

    def cut(q):
        return span(q, chunks)

    def pair_copy(where):
        return pltpu.make_async_remote_copy(
            part.at[:, :, 1 - me.core, where], given.at[:, :, where], pair_send, pair_recv.at[where.start // size],
            device_id=me.at(core=1 - me.core), device_id_type=MESH,
        )

    def ring_copy(half, step, where):
        q = where.start // size
        up = True if half == ALL else (half == 0) == (step != 2)
        return pltpu.make_async_remote_copy(
            running.at[half, step, where], arrived.at[half, step, where],
            ring_send, head_recv.at[q] if step == 0 else tail_recv.at[0 if half == ALL else half, q],
            device_id=me.at(z=(me.z + (1 if up else 3)) % 4), device_id_type=MESH,
        )

    def far_copy(where):
        return pltpu.make_async_remote_copy(
            across.at[where], crossed.at[where], far_send, far_recv.at[where.start // size],
            device_id=me.at(x_hi=1 - me.x_hi), device_id_type=MESH,
        )

    def begin():
        for q in range(chunks):
            pair_copy(cut(q)).start()

    def local_sum(half, offset, k):
        x_hi = me.x_hi if half == 0 else 1 - me.x_hi
        z = (me.z + (offset if half == 0 else 4 - offset)) % 4
        return part[x_hi, z, me.core, k] + given[x_hi, z, k]

    def first(q):
        pair_copy(cut(q)).wait_recv()
        for step, offset in ((0, 2), (2, 3)):
            for half in (1, 0):
                def body(k, half=half, step=step, offset=offset):
                    running[half, step, k] = local_sum(half, offset, k).astype(jnp.bfloat16)

                each_tile(q, chunks, body)
                ring_copy(half, step, cut(q)).start()

    def middle(q):
        ring_copy(ALL, 0, cut(q)).wait_recv()
        for half in (1, 0):

            def body(k, half=half):
                running[half, 1, k] = (local_sum(half, 1, k) + wide(arrived[half, 0, k])).astype(jnp.bfloat16)

            each_tile(q, chunks, body)
            ring_copy(half, 1, cut(q)).start()

    def last(q):
        for half in (1, 0):
            ring_copy(half, BOTH, cut(q)).wait_recv()

            def body(k, half=half):
                total = local_sum(half, 0, k) + (wide(arrived[half, 1, k]) + wide(arrived[half, 2, k]))
                if half == 1:
                    across[k] = total.astype(jnp.bfloat16)
                else:
                    kept[k] = total

            each_tile(q, chunks, body)
            if half == 1:
                far_copy(cut(q)).start()

    def done(q):
        far_copy(cut(q)).wait_recv()
        each_tile(q, chunks, lambda k: finish(k, kept[k] + wide(crossed[k])))

    def drain():
        pair_copy(whole).wait_send()
        far_copy(whole).wait_send()
        ring_copy(ALL, ALL, whole).wait_send()

    return begin, [first, middle, last, done], drain


def sum_scratch():
    block = lambda *lead, dtype=jnp.bfloat16: pltpu.VMEM((*lead, 8, TILE, TILE), dtype)
    dma = pltpu.SemaphoreType.DMA
    bufs = [block(2, 4, dtype=jnp.float32), block(2, 3), block(2, 3), block(dtype=jnp.float32), block(), block()]
    each = dma((SUM_CHUNK,))
    sems = [dma, each, dma, each, dma((2, SUM_CHUNK)), dma, each]
    return bufs + sems


N_SUM = 13


def spread_stages(me, gathered, sems, chunks):
    side_send, near_send, relay_send, pass_send, side_recv, own_recv, beside_recv, rest_recv, pass_recv = sems

    def copy(block, send, recv, device):
        return pltpu.make_async_remote_copy(block, block, send, recv, device_id=device, device_id_type=MESH)

    def block(y, x_lo, q):
        return gathered.at[me.core, (me.y + y) % 4, me.x_lo if x_lo == 0 else 1 - me.x_lo, span(q, chunks)]

    def along(way):
        return me.at(y=(me.y + (1 if way == 0 else 3)) % 4)

    beside_device, other_core = me.at(x_lo=1 - me.x_lo), me.at(core=1 - me.core)

    def side_copy(q):
        return copy(block(0, 0, q), side_send, side_recv.at[q], beside_device)

    def near_copy(kind, way, q):
        recv = rest_recv if kind != way else own_recv if kind == 0 else beside_recv
        return copy(block(0, kind, q), near_send, recv.at[q], along(way))

    def relay_copy(way, q):
        return copy(block(3 if way == 0 else 1, way, q), relay_send, rest_recv.at[q], along(way))

    def pass_copy(y, x_lo, q):
        return copy(block(y, x_lo, q), pass_send, pass_recv, other_core)

    def own(q):
        side_copy(q).start()
        near_copy(0, 0, q).start()
        near_copy(0, 1, q).start()
        pass_copy(0, 0, q).start()

    def beside(q):
        side_copy(q).wait_recv()
        near_copy(1, 0, q).start()
        near_copy(1, 1, q).start()
        pass_copy(0, 1, q).start()

    def relay_own(q):
        near_copy(0, 0, q).wait_recv()
        relay_copy(0, q).start()
        pass_copy(3, 0, q).start()

    def relay_beside(q):
        near_copy(1, 1, q).wait_recv()
        relay_copy(1, q).start()
        pass_copy(1, 1, q).start()

    def opposite(q):
        copy(gathered.at[me.core, :, 0, span(q, chunks)], relay_send, rest_recv.at[q], beside_device).wait_recv()
        pass_copy(1, 0, q).start()
        pass_copy(3, 1, q).start()
        pass_copy(2, 0, q).start()
        pass_copy(2, 1, q).start()

    def drain():
        copy(gathered.at[1 - me.core], pass_send, pass_recv, other_core).wait_recv()
        copy(gathered.at[me.core], pass_send, pass_recv, other_core).wait_send()
        copy(gathered.at[me.core, :, 0], near_send, pass_recv, other_core).wait_send()
        copy(gathered.at[me.core, 0], relay_send, pass_recv, other_core).wait_send()
        copy(gathered.at[me.core, 0, 0], side_send, pass_recv, other_core).wait_send()

    return [own, beside, relay_own, relay_beside, opposite], drain


def spread_scratch(chunks):
    dma = pltpu.SemaphoreType.DMA
    return [dma] * 4 + [dma((chunks,))] * 4 + [dma]


def hot(ids, cell):
    return jnp.where(jnp.broadcast_to(ids, (TILE, TILE)) == cell, jnp.bfloat16(1), jnp.bfloat16(0))


def narrow(x):
    return x.astype(jnp.float32).astype(jnp.bfloat16)


def start_kernel(
    features_ref, meta_ref, edges_ref, tiles_hbm, metas_ref, root_ref, gathered_ref,
    tiles_ref, lists, raw, slot_degree, degree, shares, roots,
    tile_sem, list_sem, list_send, list_recv, meta_send, meta_recv, share_send, share_recv, root_send, root_recv, *sems,
):
    me = Place()
    peers = [lax.rem(me.col + i, 16) for i in range(1, 16)]
    across = me.col + 1 - 2 * me.core
    friends = [(lax.rem(me.row + i % 8, 8), me.col if i < 8 else across) for i in range(1, 16)]
    own_lists = pltpu.make_async_copy(edges_ref.at[:, :, me.core], lists.at[me.core], list_sem)
    own_lists.start()
    everyone = [(me.row, peer) for peer in peers] + [friend for i, friend in enumerate(friends) if i != 7]
    barrier = pltpu.get_barrier_semaphore()
    for device in everyone:
        pl.semaphore_signal(barrier, inc=1, device_id=device, device_id_type=MESH)
    partner = me.at(core=1 - me.core)

    give_lists = pltpu.make_async_remote_copy(
        edges_ref.at[:, :, 1 - me.core], lists.at[me.core], list_send, list_recv, device_id=partner, device_id_type=MESH
    )
    give_meta = pltpu.make_async_remote_copy(
        meta_ref, metas_ref.at[me.core], meta_send, meta_recv, device_id=partner, device_id_type=MESH
    )

    def tile_copy(bank):
        return pltpu.make_async_copy(tiles_ref.at[bank], tiles_hbm.at[bank], tile_sem)

    def share_copy(i):
        return pltpu.make_async_remote_copy(
            degree.at[peers[i]], shares.at[i], share_send, share_recv,
            device_id=(me.row, peers[i]), device_id_type=MESH,
        )

    def all_shares(send):
        return pltpu.make_async_remote_copy(
            shares, shares, send, share_recv, device_id=partner, device_id_type=MESH
        )

    def root_copy(i):
        block = roots.at[me.core, me.y, me.x_lo]
        return pltpu.make_async_remote_copy(
            block, block, root_send, root_recv.at[i], device_id=friends[i], device_id_type=MESH
        )

    metas_ref[me.core] = meta_ref[...]

    def turn(k, carry):
        raw[me.core, me.y, me.x_lo, k] = wide(features_ref[k]).T.astype(jnp.bfloat16)
        return carry

    lax.fori_loop(0, 8, turn, 0, unroll=4)
    slot_degree[...] = jnp.zeros_like(slot_degree)
    stages, drain = spread_stages(me, raw, sems, RAW_CHUNK)
    groups = 2 * lists.shape[2] * 8 // GROUP
    blocks = GROUP // 8
    own_lists.wait()

    def build(group, carry):
        @pl.when(group == RAW_MOVES[0][0])
        def _():
            pl.semaphore_wait(barrier, len(everyone))
            give_lists.start()
            give_meta.start()

        for when, moves in RAW_MOVES:
            @pl.when(group == when)
            def _(moves=moves):
                for stage, q in moves:
                    stages[stage](q)

        @pl.when(group == groups // 2)
        def _():
            give_lists.wait_recv()
            give_meta.wait_recv()

        half = group // (groups // 2)
        place = group % (groups // 2)
        owner = me.core + half * (1 - 2 * me.core)
        bank = owner * (groups // 2) + place
        base = place * blocks

        shape = (blocks, 8, TILE)
        slot = (lax.broadcasted_iota(jnp.int32, shape, 0) + base) * 16 + 8 * me.core + lax.broadcasted_iota(jnp.int32, shape, 1)
        live = slot < jnp.broadcast_to(metas_ref[owner, 16:17, :].reshape(1, 1, TILE), shape)
        dst = jnp.where(live, lists[owner, 0, pl.ds(base, blocks)], -1).reshape(GROUP, TILE)
        src = lists[owner, 1, pl.ds(base, blocks)].reshape(GROUP, TILE)
        dst, src = narrow(dst), narrow(src)
        cell = narrow(lax.broadcasted_iota(jnp.int32, (TILE, TILE), 0))
        for block in range(blocks):
            totals = []
            for i in range(8 * block, 8 * block + 8):
                counts = lax.dot_general(
                    hot(src[i : i + 1, :], cell), hot(dst[i : i + 1, :], cell).astype(jnp.float8_e4m3fn), (((1,), (1,)), ((), ())),
                    preferred_element_type=jnp.float32,
                )
                tiles_ref[bank, i] = counts.astype(jnp.bfloat16)
                totals.append(jnp.sum(counts, axis=0, keepdims=True))
            slot_degree[owner, (base + block) * 2 + me.core] = jnp.concatenate(totals, axis=0)
        tile_copy(bank).start()
        return carry

    lax.fori_loop(0, groups, build, 0)

    cell = lax.broadcasted_iota(jnp.int32, (TILE, TILE), 0)
    counted = jnp.zeros((TILE, TILE), jnp.float32)
    for owner in range(2):
        for j in range(8):
            row_hot = (jnp.broadcast_to(metas_ref[owner, j : j + 1, :], (TILE, TILE)) == cell).astype(jnp.float32)
            slots = slot_degree[owner, 16 * j : 16 * j + 16].reshape(TILE, TILE)
            counted += jnp.dot(
                row_hot.astype(jnp.bfloat16), slots.astype(jnp.bfloat16), preferred_element_type=jnp.float32
            )
    degree[...] = counted.reshape(16, 8, TILE)
    for i in range(15):
        share_copy(i).start()
    for stage, q in RAW_LATE:
        stages[stage](q)
    total = degree[me.col]
    all_shares(share_send).wait_recv()
    for i in range(15):
        total = total + shares[i]
    root = lax.rsqrt(1.0 + total)
    root_ref[...] = root
    roots[me.core, me.y, me.x_lo] = root
    for i in range(15):
        root_copy(i).start()
    for q in range(RAW_CHUNK):
        stages[4](q)
    drain()

    def scale_block(c, row):
        y, x = row // 2, row % 2

        def scale(k, carry):
            gathered_ref[c, y, x, k] = (wide(raw[c, y, x, k]) * roots[c, y, x, pl.ds(k, 1), :]).astype(jnp.bfloat16)
            return carry

        lax.fori_loop(0, 8, scale, 0, unroll=4)

    scale_block(me.core, me.row)
    for i in (8, 2, 6, 10, 14, 1, 7, 9, 15, 3, 5, 11, 13, 4, 12):
        root_copy(i - 1).wait_recv()
        scale_block(me.core if i < 8 else 1 - me.core, lax.rem(me.row + 8 - i % 8, 8))
    all_shares(share_send).wait_send()
    all_shares(root_send).wait_send()
    give_lists.wait_send()
    give_meta.wait_send()
    pltpu.make_async_copy(tiles_ref, tiles_hbm, tile_sem).wait()


RAW_MOVES = (
    (3, ((0, 0), (0, 1))),
    (9, ((1, 0), (2, 0))),
    (13, ((1, 1), (2, 1))),
)
RAW_LATE = ((3, 0), (3, 1))


def sum_kernel(spreads, part_ref, root_ref, hop_ref, *refs):
    me = Place()
    gathered_ref = refs[0] if spreads else None
    scratch = refs[1:] if spreads else refs
    greet(sum_devices(me) + (spread_devices(me) if spreads else []))

    def finish(k, total):
        root = root_ref[pl.ds(k, 1), :]
        hop_ref[k] = (total * root).T.astype(jnp.bfloat16)
        if spreads:
            gathered_ref[me.core, me.y, me.x_lo, k] = (total * (root * root)).astype(jnp.bfloat16)

    begin, stages, drain = sum_stages(me, part_ref, scratch[:6], scratch[6:N_SUM], finish)
    begin()
    if spreads:
        more, drain_spread = spread_stages(me, gathered_ref, scratch[N_SUM:], SUM_CHUNK)
        run_stages(stages + more, SUM_LAGS, SUM_CHUNK)
        drain_spread()
    else:
        run_stages(stages, SUM_LAGS[:4], SUM_CHUNK)
    drain()


VMEM = pl.BlockSpec(memory_space=pltpu.VMEM)
SMEM = pl.BlockSpec(memory_space=pltpu.SMEM)
HBM = pl.BlockSpec(memory_space=pltpu.HBM)
GATHERED = (2, 4, 2, 8, TILE, TILE)


def comm_params(number, limit):
    return pltpu.CompilerParams(collective_id=number, has_side_effects=True, vmem_limit_bytes=limit)


def start(features, meta, edges):
    dma = pltpu.SemaphoreType.DMA
    slots = edges.shape[1]
    shape = jax.ShapeDtypeStruct
    f32, bf16, i32 = jnp.float32, jnp.bfloat16, jnp.int32
    return pl.pallas_call(
        start_kernel,
        out_shape=[
            shape((slots // GROUP, GROUP, TILE, TILE), bf16), shape((2, 24, TILE), i32), shape((8, TILE), f32), shape(GATHERED, bf16)
        ],
        in_specs=[VMEM, VMEM, HBM],
        out_specs=[HBM, VMEM, VMEM, VMEM],
        scratch_shapes=[
            pltpu.VMEM((slots // GROUP, GROUP, TILE, TILE), bf16),
            pltpu.VMEM((2, 2, slots // 16, 8, TILE), i32),
            pltpu.VMEM(GATHERED, bf16),
            pltpu.VMEM((2, slots // 8, 8, TILE), f32),
            pltpu.VMEM((16, 8, TILE), f32),
            pltpu.VMEM((15, 8, TILE), f32),
            pltpu.VMEM((2, 4, 2, 8, TILE), f32),
            *[dma] * 9, dma((15,)),
            *spread_scratch(RAW_CHUNK),
        ],
        compiler_params=comm_params(0, START_LIMIT),
        name="start_build",
    )(features.reshape(8, TILE, TILE), meta, edges.reshape(2, slots // 16, 2, 8, TILE))


def live_count(metas_ref, core, owner):
    count = metas_ref[owner, 16, 0]
    return count // 16 * 8 + jnp.clip(count % 16 - 8 * core, 0, 8)


def apply_kernel(carries, metas_ref, tiles_hbm, x_ref, *refs):
    if carries:
        carried, total, carried_out, tiles_ref, tile_sem, carry_sem = refs
        carry_copy = pltpu.make_async_copy(carried, carried_out, carry_sem)
        carry_copy.start()
    else:
        total, tiles_ref, tile_sem = refs
    core = lax.axis_index("col") % 2
    half_groups = tiles_ref.shape[0] // 2
    live = [(live_count(metas_ref, core, owner) + GROUP - 1) // GROUP for owner in range(2)]

    def tile_copy(bank):
        return pltpu.make_async_copy(tiles_hbm.at[bank], tiles_ref.at[bank], tile_sem.at[bank])

    for owner in range(2):
        def fetch(place, carry, owner=owner):
            tile_copy(owner * half_groups + place).start()
            return carry

        lax.fori_loop(0, live[owner], fetch, 0)
    total[...] = jnp.zeros_like(total)
    for owner in range(2):
        def apply_group(place, carry, owner=owner):
            bank = owner * half_groups + place
            tile_copy(bank).wait()
            for start in range(0, GROUP, BATCH):
                lanes = [8 * core + (i // 8 * 16 + i % 8) for i in range(start, start + BATCH)]
                products = [
                    jnp.dot(
                        x_ref[owner * 64 + metas_ref[owner, 8 + place, lane]],
                        tiles_ref[bank, start + j],
                        preferred_element_type=jnp.float32,
                    )
                    for j, lane in enumerate(lanes)
                ]
                for lane, product in zip(lanes, products):
                    total[metas_ref[owner, place, lane]] += product
            return carry

        lax.fori_loop(0, live[owner], apply_group, 0)
    if carries:
        carry_copy.wait()


def apply_tiles(metas, tiles, x, *carried):
    total = jax.ShapeDtypeStruct((TILE, TILE, TILE), jnp.float32)
    dma = pltpu.SemaphoreType.DMA
    return pl.pallas_call(
        functools.partial(apply_kernel, len(carried)),
        in_specs=[SMEM, HBM, VMEM] + [VMEM] * len(carried),
        out_specs=[VMEM] + [HBM] * len(carried),
        scratch_shapes=[pltpu.VMEM(tiles.shape, tiles.dtype), dma((tiles.shape[0],))] + [dma] * len(carried),
        out_shape=[total] + [jax.ShapeDtypeStruct(c.shape, c.dtype) for c in carried],
        compiler_params=pltpu.CompilerParams(vmem_limit_bytes=APPLY_LIMIT),
        name="apply_tiles",
    )(metas, tiles, x, *carried)


def sum_parts(part, root, spreads):
    hop = jax.ShapeDtypeStruct((8, TILE, TILE), jnp.bfloat16)
    gathered = jax.ShapeDtypeStruct(GATHERED, jnp.bfloat16)
    return pl.pallas_call(
        functools.partial(sum_kernel, spreads),
        out_shape=[hop, gathered] if spreads else [hop],
        in_specs=[VMEM, VMEM],
        out_specs=[VMEM, VMEM] if spreads else [VMEM],
        scratch_shapes=sum_scratch() + (spread_scratch(SUM_CHUNK) if spreads else []),
        compiler_params=comm_params(1 if spreads else 2, SUM_LIMIT),
        name="sum_spread" if spreads else "sum_last",
    )(part.reshape(2, 4, 2, 8, TILE, TILE), root)


def local(features, tile_rows, tile_cols, edge_lists, tile_counts):
    edges = edge_lists.reshape(2, *edge_lists.shape[3:])
    meta = jnp.concatenate(
        [tile_rows.reshape(8, TILE) & 127, tile_cols.reshape(8, TILE) & 63, jnp.broadcast_to(tile_counts, (8, TILE))],
        axis=0,
    )
    tiles, metas, root, gathered = start(features, meta, edges)
    (part,) = apply_tiles(metas, tiles, gathered.reshape(128, TILE, TILE))
    hop_one, gathered = sum_parts(part, root, True)
    part, hop_one = apply_tiles(metas, tiles, gathered.reshape(128, TILE, TILE), hop_one)
    (hop_two,) = sum_parts(part, root, False)
    return (hop_one.reshape(features.shape), hop_two.reshape(features.shape))


def solution(mesh):
    placed = (
        P(("row", "col"), None),
        P("row", "col", None),
        P("row", "col", None),
        P(None, "row", "col", None, None),
        P("row", "col"),
    )
    return jax.shard_map(
        local,
        mesh=mesh,
        in_specs=placed,
        out_specs=(P(("row", "col"), None), P(("row", "col"), None)),
        check_vma=False,
    )
```
